32 devices in a mesh: row: 4 (over z), col: 8 (over y, x, core).
Axes of the slice: x: 2, y: 2, z: 4, core: 2. Of those that a mesh axis runs over, the one named last changes fastest.
Arguments:
- eigvecs: bfloat16 [40960, 2048], P('row', 'col'), may hold values from -0.125 to 0.125
- reflectors: bfloat16 [2, 40960, 128], P(None, 'row'), may hold values from -6 to 6
- factors: float32 [2, 128, 128], replicated, may hold values from -0.00024414062 to 0.00024414062
- frequencies: float32 [2048], replicated, may hold values from 0.3 to 3
- region_blocks: int32 [72], P('row'), may hold values from 0 to 319, as said below
Outputs:
- covariance: float32 [9216, 9216], P('row', 'col')
The draws below stay inside these ranges and needn't reach their ends.
Inputs may be any that keep to these rules, and one draw needn't show every extreme that they name: `region_blocks`: the 72 block numbers are distinct and ascending; exactly 18 of them lie in each consecutive run of 80 block numbers.
All inputs are finite; a program needn't handle non-finite values.
Results may differ from the reference program's by a relative error of at most 0.004.
Values may be sent and summed in bfloat16 or wider, within the bound.
A program may use at most 128 MiB of HBM per device.

```python
import math
import jax
import jax.numpy as jnp
from jax import lax

ROWS_DEV = 10240
HB = 128
BLOCK = 128
N = 40960
K = 2048
RBD = 18
N_ROW = 4


def draw_region_blocks(key, part):
    local_blocks = ROWS_DEV // BLOCK
    scores = jax.random.randint(key, (N_ROW, local_blocks), 0, 1 << 20)
    scores = scores * local_blocks + jnp.arange(local_blocks, dtype=jnp.int32)[None, :]
    chosen = lax.top_k(scores, RBD)[1]
    chosen = jnp.sort(chosen, axis=1)
    chosen = chosen + jnp.arange(N_ROW, dtype=jnp.int32)[:, None] * local_blocks
    return chosen.reshape(-1).astype(jnp.int32)


def level_of(key, shape, pieces, low, top_value):
    level = 1.0
    for axis_at, blocks in pieces:
        draws = jax.random.uniform(jax.random.fold_in(jax.random.fold_in(key, 6), axis_at), (blocks,), jnp.float32, low / len(pieces), top_value / len(pieces))
        level = level * jnp.repeat(jnp.exp(draws), shape[axis_at] // blocks).reshape((-1,) + (1,) * (len(shape) - 1 - axis_at))
    return level


def scatter_about(own_key, shape, spread, reach, pieces=(), kind=jnp.bfloat16):
    array = jax.random.normal(own_key, shape, jnp.float32) * spread
    if len(pieces) > 0:
        array = level_of(own_key, shape, pieces, -0.22, 0.18) * array
    return jnp.clip(array, min=-reach, max=reach).astype(kind)


def setup_inputs(seed: int = 0) -> dict:
    seeds = jax.random.split(jax.random.key(seed), 6)
    return {
        "eigvecs": scatter_about(seeds[0], (N, K), K ** -0.5, 0.125, ((0, 4), (1, 8))),
        "reflectors": scatter_about(seeds[1], (2, N, HB), 1.0, 6.0, ((1, 4),)),
        "factors": scatter_about(seeds[2], (2, HB, HB), (HB * HB * N) ** -0.5, 0.00024414062, (), jnp.float32),
        "frequencies": jnp.clip(jnp.exp(jax.random.uniform(seeds[3], (K,), jnp.float32, math.log(0.3), math.log(3.0))), 0.3, 3.0),
        "region_blocks": draw_region_blocks(jax.random.fold_in(seeds[5], 71), 0),
    }


def contract_rows(left, right):
    return lax.dot_general(left, right, (((0,), (0,)), ((), ())), preferred_element_type=jnp.float32)


def reference(eigvecs, reflectors, factors, frequencies, region_blocks):
    first_block = reflectors[0]
    second_block = reflectors[1]
    first_factor = jnp.triu(factors[0])
    second_factor = jnp.triu(factors[1])
    highest = lax.Precision.HIGHEST
    second_proj = contract_rows(second_block, eigvecs)
    second_apply = jnp.dot(second_factor, second_proj, precision=highest).astype(jnp.bfloat16)
    cross = contract_rows(first_block, second_block)
    first_proj = contract_rows(first_block, eigvecs) - jnp.dot(cross, second_apply.astype(jnp.float32), precision=highest)
    first_apply = jnp.dot(first_factor, first_proj, precision=highest).astype(jnp.bfloat16)
    offsets = jnp.arange(BLOCK, dtype=jnp.int32)
    rows = (region_blocks.astype(jnp.int32)[:, None] * BLOCK + offsets[None, :]).reshape(-1)
    region = eigvecs[rows].astype(jnp.float32)
    region = region - jnp.dot(second_block[rows], second_apply, preferred_element_type=jnp.float32)
    region = region - jnp.dot(first_block[rows], first_apply, preferred_element_type=jnp.float32)
    region = region.astype(jnp.bfloat16)
    weight = 1.0 / jnp.tanh(frequencies / 2.0) / (2.0 * frequencies)
    scaled = (region.astype(jnp.float32) * weight[None, :]).astype(jnp.bfloat16)
    return lax.dot_general(scaled, region, (((1,), (1,)), ((), ())), preferred_element_type=jnp.float32)
```

```python
import functools

import jax
import jax.numpy as jnp
from jax import lax
from jax.experimental import pallas as pl
from jax.experimental.pallas import tpu as pltpu
from jax.sharding import PartitionSpec as P

BLOCK = 128
MESH = pl.DeviceIdType.MESH
SUB = 12


def contract_rows(left, right):
    return lax.dot_general(
        left, right, (((0,), (0,)), ((), ())), preferred_element_type=jnp.float32
    )


def contract_cols(left, right):
    return lax.dot_general(
        left, right, (((1,), (1,)), ((), ())), preferred_element_type=jnp.float32
    )


def exchange_kernel(
    n_row, sub, x_ref, a_ref, b_ref, half_buf,
    own_sem, send_plane, send_sib, recv_a, send_z, recv_b, fill_sem,
):
    r = lax.axis_index("row")
    c = lax.axis_index("col")
    k = c // 2
    h = lax.rem(c, 2)
    o = 1 - h
    sib = 2 * k + o
    rows, cols = x_ref.shape
    step = rows // sub
    hsub = sub // 2
    half = rows // 2
    has_up = (r < n_row - 1).astype(jnp.int32)
    has_dn = (r > 0).astype(jnp.int32)

    barrier = pltpu.get_barrier_semaphore()

    def greet(row, col):
        pl.semaphore_signal(barrier, inc=1, device_id=(row, col), device_id_type=MESH)

    greet(r, sib)
    for d in range(1, n_row):
        greet(r, 2 * (k ^ d) + h)

    @pl.when(r < n_row - 1)
    def _():
        greet(r + 1, c)

    @pl.when(r > 0)
    def _():
        greet(r - 1, c)

    pl.semaphore_wait(barrier, n_row + has_up + has_dn)

    def piece_cols(d, side):
        owner = 2 * (k ^ d) + (h if side == 0 else o)
        return pl.ds(pl.multiple_of(owner * cols, cols), cols)

    def a_at(d, side, s):
        return a_ref.at[pl.ds(s * step, step), piece_cols(d, side)]

    def plane_copy(d, s):
        return pltpu.make_async_remote_copy(
            src_ref=x_ref.at[pl.ds(s * step, step), :],
            dst_ref=a_ref.at[pl.ds(s * step, step), piece_cols(0, 0)],
            send_sem=send_plane.at[d, s], recv_sem=recv_a.at[d, 0, s],
            device_id=(r, 2 * (k ^ d) + h), device_id_type=MESH,
        )

    def sib_copy(d, s):
        src = x_ref.at[pl.ds(s * step, step), :] if d == 0 else a_at(d, 0, s)
        return pltpu.make_async_remote_copy(
            src_ref=src, dst_ref=a_at(d, 0, s),
            send_sem=send_sib.at[d, s], recv_sem=recv_a.at[d, 1, s],
            device_id=(r, sib), device_id_type=MESH,
        )

    def half_rows(t):
        return pl.ds(pl.multiple_of(h * half + t * step, step), step)

    def z_copy(src, way, target, d, side, t):
        return pltpu.make_async_remote_copy(
            src_ref=src,
            dst_ref=b_ref.at[pl.ds(t * step, step), piece_cols(d, side)],
            send_sem=send_z.at[way, d, side, t], recv_sem=recv_b.at[d, side, t],
            device_id=(target, c), device_id_type=MESH,
        )

    def from_source(way, target, d, side, t):
        if d == 0 and side == 0:
            src = x_ref.at[half_rows(t), :]
        else:
            src = a_ref.at[half_rows(t), piece_cols(d, side)]
        return z_copy(src, way, target, d, side, t)

    def relay(way, target, d, side, t):
        src = b_ref.at[pl.ds(t * step, step), piece_cols(d, side)]
        return z_copy(src, way, target, d, side, t)

    own = pltpu.make_async_copy(x_ref, a_ref.at[:, piece_cols(0, 0)], own_sem)
    own.start()
    for s in range(sub):
        sib_copy(0, s).start()
    for d in range(1, n_row):
        for s in range(sub):
            plane_copy(d, s).start()

    arrivals = [(d, s) for d in range(1, n_row) for s in range(sub)]
    parts = [(d, side, t) for d in range(n_row) for side in (0, 1) for t in range(hsub)]

    def take_a(d, s):
        plane_copy(d, s).wait_recv()
        sib_copy(d, s).start()

    at_source = r == k
    above = r > k
    below = r < k

    @pl.when(at_source)
    def _():
        def push(d, side, t):
            @pl.when(r < n_row - 1)
            def _():
                from_source(0, r + 1, d, side, t).start()

            @pl.when(r > 0)
            def _():
                from_source(1, r - 1, d, side, t).start()

        for d in range(n_row):
            if d:
                for s in range(sub):
                    take_a(d, s)
            else:
                for t in range(hsub):
                    push(d, 0, t)
            for s in range(sub):
                sib_copy(d, s).wait_recv()
            for side in (0, 1) if d else (1,):
                for t in range(hsub):
                    push(d, side, t)
        own.wait()
        fill = pltpu.make_async_copy(
            a_ref.at[pl.ds(pl.multiple_of(h * half, half), half), :], half_buf, fill_sem
        )
        fill.start()
        fill.wait()
        out = pltpu.make_async_copy(half_buf, b_ref, fill_sem)
        out.start()
        out.wait()

    @pl.when(jnp.logical_not(at_source))
    def _():
        for i, (d, side, t) in enumerate(parts):
            if i < len(arrivals):
                take_a(*arrivals[i])
            relay(0, r, d, side, t).wait_recv()

            @pl.when(above & (r < n_row - 1))
            def _():
                relay(0, r + 1, d, side, t).start()

            @pl.when(below & (r > 0))
            def _():
                relay(1, r - 1, d, side, t).start()

        for d, s in arrivals[len(parts):]:
            take_a(d, s)
        for d in range(n_row):
            for s in range(sub):
                sib_copy(d, s).wait_recv()
        own.wait()

    for d in range(n_row):
        for s in range(sub):
            sib_copy(d, s).wait_send()
            if d:
                plane_copy(d, s).wait_send()
    for d, side, t in parts:
        @pl.when((r >= k) & (r < n_row - 1))
        def _():
            relay(0, r, d, side, t).wait_send()

        @pl.when((r <= k) & (r > 0))
        def _():
            relay(1, r, d, side, t).wait_send()


def exchange(x, n_row):
    rows, cols = x.shape
    n_col = 2 * n_row
    sub = SUB if n_row <= 4 else SUB // 2
    hsub = sub // 2
    dma = pltpu.SemaphoreType.DMA
    return pl.pallas_call(
        functools.partial(exchange_kernel, n_row, sub),
        out_shape=(
            jax.ShapeDtypeStruct((rows, cols * n_col), x.dtype),
            jax.ShapeDtypeStruct((rows // 2, cols * n_col), x.dtype),
        ),
        in_specs=[pl.BlockSpec(memory_space=pltpu.VMEM)],
        out_specs=(pl.BlockSpec(memory_space=pl.ANY),) * 2,
        scratch_shapes=[
            pltpu.VMEM((rows // 2, cols * n_col), x.dtype),
            dma,
            dma((n_row, sub)),
            dma((n_row, sub)),
            dma((n_row, 2, sub)),
            dma((2, n_row, 2, hsub)),
            dma((n_row, 2, hsub)),
            dma,
        ],
        compiler_params=pltpu.CompilerParams(collective_id=0, has_side_effects=True),
        name="exchange",
    )(x)


def project_kernel(
    n_row, w_ref, g_ref, t_ref, p_ref,
    w_in, g_in, w_sum, g_sum, w_full, g_full, send_1, recv_1, send_2, recv_2,
):
    r = lax.axis_index("row")
    c = lax.axis_index("col")
    barrier = pltpu.get_barrier_semaphore()
    for d in range(1, n_row):
        pl.semaphore_signal(barrier, inc=1, device_id=(r ^ d, c), device_id_type=MESH)
    pl.semaphore_wait(barrier, n_row - 1)
    pairs = ((w_ref, w_in, w_sum, w_full), (g_ref, g_in, g_sum, g_full))

    def part(array, owner):
        size = array.shape[0] // n_row
        return pl.ds(pl.multiple_of(owner * size, size), size)

    def scatter(d, i):
        array, landing, _, _ = pairs[i]
        return pltpu.make_async_remote_copy(
            src_ref=array.at[part(array, r ^ d), :], dst_ref=landing.at[d],
            send_sem=send_1.at[d, i], recv_sem=recv_1.at[d, i],
            device_id=(r ^ d, c), device_id_type=MESH,
        )

    def spread(d, i):
        array, _, total, full = pairs[i]
        return pltpu.make_async_remote_copy(
            src_ref=total, dst_ref=full.at[part(array, r), :],
            send_sem=send_2.at[d, i], recv_sem=recv_2.at[d, i],
            device_id=(r ^ d, c), device_id_type=MESH,
        )

    every = [(d, i) for d in range(1, n_row) for i in (1, 0)]
    for d, i in every:
        scatter(d, i).start()
    for d, i in every:
        scatter(d, i).wait_recv()
    for i in (1, 0):
        array, landing, total, full = pairs[i]
        value = array[part(array, r), :]
        for d in range(1, n_row):
            value = value + landing[d]
        total[...] = value
    for i in (1, 0):
        array, _, total, full = pairs[i]
        full[part(array, r), :] = total[...]
    for d, i in every:
        spread(d, i).start()
    for d, i in every:
        spread(d, i).wait_recv()
    highest = lax.Precision.HIGHEST
    width = g_ref.shape[0]
    second = jnp.dot(
        t_ref[1], w_full[width:, :], precision=highest, preferred_element_type=jnp.float32
    ).astype(jnp.bfloat16)
    first = w_full[:width, :] - jnp.dot(
        g_full[...], second.astype(jnp.float32),
        precision=highest, preferred_element_type=jnp.float32,
    )
    first = jnp.dot(t_ref[0], first, precision=highest, preferred_element_type=jnp.float32)
    p_ref[0] = first.astype(jnp.bfloat16)
    p_ref[1] = second
    for d, i in every:
        scatter(d, i).wait_send()
        spread(d, i).wait_send()


def project(w, g, factors, n_row):
    dma = pltpu.SemaphoreType.DMA((n_row, 2))
    width, columns = g.shape[0], w.shape[1]
    vmem = pl.BlockSpec(memory_space=pltpu.VMEM)

    def landing(array):
        return pltpu.VMEM((n_row, array.shape[0] // n_row, array.shape[1]), jnp.float32)

    def total(array):
        return pltpu.VMEM((array.shape[0] // n_row, array.shape[1]), jnp.float32)

    return pl.pallas_call(
        functools.partial(project_kernel, n_row),
        out_shape=jax.ShapeDtypeStruct((2, width, columns), jnp.bfloat16),
        in_specs=[vmem] * 3,
        out_specs=vmem,
        scratch_shapes=[
            landing(w), landing(g), total(w), total(g),
            pltpu.VMEM(w.shape, jnp.float32), pltpu.VMEM(g.shape, jnp.float32),
            dma, dma, dma, dma,
        ],
        compiler_params=pltpu.CompilerParams(collective_id=1, has_side_effects=True),
        name="project",
    )(w, g, factors)


def region_kernel(index_ref, p_ref, vecs_ref, refl_ref, out_ref, vecs, refl, sems):
    count = vecs.shape[0]

    def copies(b):
        at = index_ref[b]
        return (
            pltpu.make_async_copy(vecs_ref.at[at], vecs.at[b], sems.at[b, 0]),
            pltpu.make_async_copy(refl_ref.at[0, at], refl.at[0, b], sems.at[b, 1]),
            pltpu.make_async_copy(refl_ref.at[1, at], refl.at[1, b], sems.at[b, 2]),
        )

    for b in range(count):
        for copy in copies(b):
            copy.start()
    for b in range(count):
        for copy in copies(b):
            copy.wait()
        value = vecs[b].astype(jnp.float32)
        value = value - jnp.dot(refl[1, b], p_ref[1], preferred_element_type=jnp.float32)
        value = value - jnp.dot(refl[0, b], p_ref[0], preferred_element_type=jnp.float32)
        out_ref[b] = value.astype(out_ref.dtype)


def region_rows(index, applied, vecs, refl):
    count = index.shape[0]
    columns, width = vecs.shape[2], refl.shape[3]
    vmem = pl.BlockSpec(memory_space=pltpu.VMEM)
    hbm = pl.BlockSpec(memory_space=pl.ANY)
    return pl.pallas_call(
        region_kernel,
        out_shape=jax.ShapeDtypeStruct((count, BLOCK, columns), vecs.dtype),
        in_specs=[pl.BlockSpec(memory_space=pltpu.SMEM), vmem, hbm, hbm],
        out_specs=vmem,
        scratch_shapes=[
            pltpu.VMEM((count, BLOCK, columns), vecs.dtype),
            pltpu.VMEM((2, count, BLOCK, width), refl.dtype),
            pltpu.SemaphoreType.DMA((count, 3)),
        ],
        name="region",
    )(index, applied, vecs, refl)


def per_device(n_row, eigvecs, reflectors, factors, frequencies, region_blocks):
    columns = eigvecs.shape[1]
    width = reflectors.shape[2]
    local = lax.dot_general(
        reflectors, eigvecs, (((1,), (0,)), ((), ())), preferred_element_type=jnp.float32
    ).reshape(2 * width, columns)
    cross_local = contract_rows(reflectors[0], reflectors[1])
    applied = project(local, cross_local, jnp.triu(factors), n_row)
    local_blocks = eigvecs.shape[0] // BLOCK
    local_index = region_blocks - lax.axis_index("row") * local_blocks
    region = region_rows(
        local_index,
        applied,
        eigvecs.reshape(local_blocks, BLOCK, columns),
        reflectors.reshape(2, local_blocks, BLOCK, width),
    ).reshape(-1, columns)
    weight = 1.0 / jnp.tanh(frequencies / 2.0) / (2.0 * frequencies)
    mine, partner = exchange(region, n_row)
    scaled = (mine.astype(jnp.float32) * weight[None, :]).astype(jnp.bfloat16)
    return contract_cols(scaled, partner)


BF = jnp.bfloat16
F32 = jnp.float32
HIGH = lax.Precision.HIGHEST


def dot_nt(left, right, **kw):
    return lax.dot_general(left, right, (((1,), (1,)), ((), ())), preferred_element_type=F32, **kw)


def dot_tn(left, right):
    return lax.dot_general(left, right, (((0,), (0,)), ((), ())), preferred_element_type=F32)


def prep_kernel(chunks, index_ref, vecs_ref, refl_ref, x_ref, y_ref, w_ref, g_ref,
                vecs, refl, w_acc, g_acc, gather_sem, vec_sem, refl_sem):
    count = x_ref.shape[0]
    base = lax.axis_index("row") * vecs_ref.shape[0]
    blocks = vecs_ref.shape[0] // chunks

    def gather(b):
        at = index_ref[b] - base
        return (
            pltpu.make_async_copy(vecs_ref.at[at], x_ref.at[b], gather_sem.at[b, 0]),
            pltpu.make_async_copy(refl_ref.at[0, at], y_ref.at[0, b], gather_sem.at[b, 1]),
            pltpu.make_async_copy(refl_ref.at[1, at], y_ref.at[1, b], gather_sem.at[b, 2]),
        )

    def load(i):
        part = pl.ds(i * blocks, blocks)
        return (
            pltpu.make_async_copy(vecs_ref.at[part], vecs.at[part], vec_sem.at[i]),
            pltpu.make_async_copy(refl_ref.at[0, part], refl.at[0, part], refl_sem.at[i, 0]),
            pltpu.make_async_copy(refl_ref.at[1, part], refl.at[1, part], refl_sem.at[i, 1]),
        )

    for i in range(chunks):
        for copy in load(i):
            copy.start()
    for b in range(count):
        for copy in gather(b):
            copy.start()
    rows = blocks * BLOCK
    for i in range(chunks):
        for copy in load(i):
            copy.wait()
        part = pl.ds(i * blocks, blocks)
        e = vecs[part].reshape(rows, vecs.shape[2])
        y0 = refl[0, part].reshape(rows, refl.shape[3])
        y1 = refl[1, part].reshape(rows, refl.shape[3])
        w = dot_tn(e, jnp.concatenate([y0, y1], axis=1))
        g = dot_tn(y0, y1)
        if i:
            w = w + w_acc[...]
            g = g + g_acc[...]
        if i < chunks - 1:
            w_acc[...] = w
            g_acc[...] = g
        else:
            w_ref[...] = w.astype(BF)
            g_ref[...] = g.astype(BF)
    for b in range(count):
        for copy in gather(b):
            copy.wait()


def prep(index, vecs, refl):
    blocks, _, columns = vecs.shape
    width = refl.shape[3]
    count = index.shape[0]
    chunks = 10
    vmem = pl.BlockSpec(memory_space=pltpu.VMEM)
    hbm = pl.BlockSpec(memory_space=pltpu.HBM)
    dma = pltpu.SemaphoreType.DMA
    return pl.pallas_call(
        functools.partial(prep_kernel, chunks),
        out_shape=(
            pltpu.VMEM((count, BLOCK, columns), BF),
            pltpu.VMEM((2, count, BLOCK, width), BF),
            pltpu.VMEM((columns, 2 * width), BF),
            pltpu.VMEM((width, width), BF),
        ),
        in_specs=[pl.BlockSpec(memory_space=pltpu.SMEM), hbm, hbm],
        out_specs=(vmem,) * 4,
        scratch_shapes=[
            pltpu.VMEM(vecs.shape, BF),
            pltpu.VMEM(refl.shape, BF),
            pltpu.VMEM((columns, 2 * width), F32),
            pltpu.VMEM((width, width), F32),
            dma((count, 3)), dma((chunks,)), dma((chunks, 2)),
        ],
        compiler_params=pltpu.CompilerParams(vmem_limit_bytes=24 << 20),
        name="prep",
    )(index, vecs, refl)


def spread_kernel(
    x_ref, y_ref, w_ref, g_ref, t_ref, f_ref, acc_ref, sa_ref, last_ref,
    buf, tbuf, rbuf, w_in, g_in, g_full, p_full, weight,
    w_send, w_recv, g_send, g_recv, h_send, h_recv, p_send, p_recv,
    own_send, relay_send, zrel_send, zsrc_send, detz_send, deti_send, rr_send,
    ax, ay, ad, asib, zb, det, tz, rr,
):
    r = lax.axis_index("row")
    c = lax.axis_index("col")
    k = c // 2
    h = lax.rem(c, 2)
    o = 1 - h
    count = x_ref.shape[0]
    half = count // 2
    columns = x_ref.shape[2]
    width = g_ref.shape[0]
    quarter = columns // 4
    last_row = 3

    def col(chip, core):
        return 2 * chip + core

    barrier = pltpu.get_barrier_semaphore()

    def greet(row, column):
        pl.semaphore_signal(barrier, inc=1, device_id=(row, column), device_id_type=MESH)

    for d in range(1, 4):
        greet(lax.rem(r + d, 4), c)
    for d in (1, 2):
        for core in (0, 1):
            greet(r, col(k ^ d, core))
    greet(r, col(k, o))
    pl.semaphore_wait(barrier, 8)

    def remote(src, dst, send, recv, row, column):
        return pltpu.make_async_remote_copy(
            src_ref=src, dst_ref=dst, send_sem=send, recv_sem=recv,
            device_id=(row, column), device_id_type=MESH,
        )

    def w_copy(d):
        q = lax.rem(r + d, 4)
        part = pl.ds(pl.multiple_of(q * quarter, quarter), quarter)
        return remote(w_ref.at[part], w_in.at[d], w_send.at[d], w_recv.at[d], q, c)

    g_half = width // 2

    def g_copy(d):
        q = lax.rem(r + d, 4)
        part = pl.ds(pl.multiple_of(h * g_half, g_half), g_half)
        return remote(g_ref.at[part], g_in.at[d], g_send.at[d], g_recv.at[d], q, c)

    for d in (2, 1, 3):
        g_copy(d).start()
        w_copy(d).start()

    f = f_ref[...]
    weight[...] = 1.0 / jnp.tanh(f / 2.0) / (2.0 * f)
    row_at = lax.broadcasted_iota(jnp.int32, (width, width), 0)
    col_at = lax.broadcasted_iota(jnp.int32, (width, width), 1)
    upper = row_at <= col_at
    zero = jnp.zeros((width, width), F32)
    t0 = jnp.where(upper, t_ref[0], zero)
    t1 = jnp.where(upper, t_ref[1], zero)

    g_part = pl.ds(pl.multiple_of(h * g_half, g_half), g_half)
    for d in (1, 2, 3):
        g_copy(d).wait_recv()
    value = g_ref[g_part, :].astype(F32)
    for d in (1, 2, 3):
        value = value + g_in[d].astype(F32)
    g_full[h] = value
    h_copy = remote(g_full.at[h], g_full.at[h], h_send, h_recv, r, col(k, o))
    h_copy.start()
    for d in (1, 2, 3):
        w_copy(d).wait_recv()
    mine = pl.ds(pl.multiple_of(r * quarter, quarter), quarter)
    w = w_ref[mine, :].astype(F32)
    for d in (1, 2, 3):
        w = w + w_in[d].astype(F32)
    second = dot_nt(w[:, width:], t1, precision=HIGH).astype(BF)
    h_copy.wait_recv()
    g = jnp.concatenate([g_full[0], g_full[1]], axis=0)
    first = w[:, :width] - dot_nt(second.astype(F32), g, precision=HIGH)
    first = dot_nt(first, t0, precision=HIGH).astype(BF)
    p_full[r, :, :width] = first
    p_full[r, :, width:] = second

    def p_copy(d):
        return remote(p_full.at[r], p_full.at[r], p_send.at[d], p_recv.at[d], lax.rem(r + d, 4), c)

    def p_arrival(d):
        q = lax.rem(r + d, 4)
        return remote(p_full.at[q], p_full.at[q], p_send.at[d], p_recv.at[4 - d], q, c)

    for d in (2, 1, 3):
        p_copy(d).start()
    for d in (1, 2, 3):
        p_arrival(d).wait_recv()

    def block_of(n):
        return lax.rem(n, 2) * half + n // 2

    def a_copy(way, n):
        b = block_of(n)
        src = buf.at[c, b]
        if way == 2:
            return remote(src, buf.at[c, b], own_send.at[2], asib.at[0, n], r, col(k, o))
        sem = ax if way == 0 else ay
        return remote(src, buf.at[c, b], own_send.at[way], sem.at[n], r, col(k ^ (way + 1), h))

    corner = (k == 0) | (k == 3)
    is_low = k == 0
    rank = jnp.where(is_low, r, 3 - r)
    away = jnp.where(is_low, -1, 1)
    slot = jnp.where(is_low, 0, 1)
    early = 5

    def det_own(hops, n):
        b = block_of(n)
        return remote(
            buf.at[c, b], tbuf.at[rank - 1, b], detz_send.at[hops - 1], tz.at[rank - 1, n],
            r + away * hops, c,
        )

    applied = p_full[...].reshape(columns, 2 * width)

    def make_region(n, _):
        b = block_of(n)
        y = jnp.concatenate([y_ref[0, b], y_ref[1, b]], axis=1)
        buf[c, b] = (x_ref[b].astype(F32) - dot_nt(y, applied)).astype(BF)
        for way in (0, 1, 2):
            a_copy(way, n).start()

        @pl.when(corner & ((rank > 1) | ((rank == 1) & (n < early))))
        def _():
            @pl.when(rank == 3)
            def _():
                det_own(2, n).start()

            det_own(1, n).start()

        return 0

    lax.fori_loop(0, count, make_region, 0)

    def a_arrival(way, n):
        src = col(k ^ (way + 1), h)
        b = block_of(n)
        at = buf.at[src, b]
        sem = (ax, ay, ad)[way]
        return remote(at, at, own_send.at[2], sem.at[n], r, col(k, o))

    def sib_copy(j, n):
        src = col(k ^ j, h)
        b = block_of(n)
        at = buf.at[src, b]
        return remote(at, at, own_send.at[2], asib.at[j, n], r, col(k, o))

    def sib_arrival(j, n):
        src = col(k ^ j, o)
        b = block_of(n)
        at = buf.at[src, b]
        return remote(at, at, own_send.at[2], asib.at[j, n], r, col(k, o))

    def relay(way, n):
        src = col(k ^ (way + 1), h)
        at = buf.at[src, block_of(n)]
        to = k ^ (2 - way)
        return remote(at, at, relay_send.at[way], ad.at[n], r, col(to, h))

    down = r < k
    at_source = r == k
    step = jnp.where(down, -1, 1)
    depth = jnp.where(down, k, 3 - k)

    def z_piece(t, depth, is_down):
        third = t // (2 * half)
        n = lax.rem(t, 2 * half) // 2
        e = lax.rem(t, 2)
        j1 = jnp.where(depth == 3, 2, 3)
        j2 = 6 - depth - j1
        j = jnp.where(third == 0, depth, jnp.where(third == 1, j1, j2))
        j = jnp.where(is_down, j, 3 - j)
        return col(j, lax.rem(h + e, 2)), n

    steps = 3 * 2 * half

    def z_relay(t):
        src, n = z_piece(t, depth, down)
        at = buf.at[src, count + n]
        return remote(at, at, zrel_send, zb.at[t], r + step, c)

    def z_source(t, is_down):
        src, n = z_piece(t, k if is_down else 3 - k, jnp.bool_(is_down))
        return remote(
            buf.at[src, h * half + n], buf.at[src, count + n],
            zsrc_send.at[0 if is_down else 1], zb.at[t], r + (-1 if is_down else 1), c,
        )

    def det_z(p, n):
        at = tbuf.at[p - 1, block_of(n)]
        return remote(at, at, detz_send.at[p], tz.at[p - 1, n], r + away, c)

    def det_plane(p, n):
        b = block_of(n)
        src = tbuf.at[p - 1, b]
        core = lax.rem(n, 2)
        if p < 3:
            return remote(
                src, buf.at[c, count + n // 2], deti_send.at[p], det.at[h, n // 2],
                r, col(k ^ p, core),
            )
        return remote(
            src, rbuf.at[slot, n // 2], deti_send.at[p], rr.at[slot, n // 2],
            r, col(k ^ (1 + h), core),
        )

    between = (k == 1) | (k == 2)

    def rr_copy(way, n):
        low = k - 1 if way == 0 else 2 - k
        src = low if way == 0 else low + 6
        return remote(
            rbuf.at[way, n], buf.at[src, count + n], rr_send.at[way], det.at[low, n],
            r, col(3 if way == 0 else 0, h),
        )

    def det_arrival(low, n):
        src = jnp.where(down, low, low + 6)
        at = buf.at[src, count + n]
        return remote(at, at, own_send.at[2], det.at[low, n], r, col(k, o))

    mine_at = jnp.where(at_source, h * half, count)

    def scale(q):
        src = col(k ^ (q // 2), lax.rem(h + q, 2))
        wt = jnp.concatenate([weight[pl.ds(2 * src, 1), :], weight[pl.ds(2 * src + 1, 1), :]], axis=1)

        def one(b, _):
            rows = pl.ds(pl.multiple_of(b * BLOCK, BLOCK), BLOCK)
            sa_ref[src, rows, :] = (buf[src, b].astype(F32) * wt).astype(BF)
            return 0

        lax.fori_loop(0, count, one, 0)

    tile = 256

    def pair(q, tiles):
        at = mine_at + 2 * q
        lanes = pl.ds(pl.multiple_of(q * tile, tile), tile)

        def one(i, _):
            rows = pl.ds(pl.multiple_of(i * tile, tile), tile)
            total = jnp.zeros((tile, tile), F32)
            for s in range(8):
                total = total + dot_nt(sa_ref[s, rows, :], buf[s, pl.ds(at, 2)].reshape(tile, columns))
            acc_ref[rows, lanes] = total
            return 0

        lax.fori_loop(tiles[0], tiles[1], one, 0)

    def wait_detours(n):
        @pl.when(jnp.logical_not(at_source))
        def _():
            for low in (0, 1):
                det_arrival(low, n).wait_recv()

    def z_source_step(t):
        @pl.when(at_source)
        def _():
            @pl.when(r > 0)
            def _():
                z_source(t, True).start()

            @pl.when(r < last_row)
            def _():
                z_source(t, False).start()

    hops = jnp.where(down, k - r, r - k)
    lag = 2

    def z_relay_step(u):
        t = u - lag * hops

        @pl.when(jnp.logical_not(at_source) & (t >= 0) & (t < steps))
        def _():
            z_relay(t).wait_recv()

            @pl.when((down & (r > 0)) | (jnp.logical_not(down) & (r < last_row)))
            def _():
                z_relay(t).start()

    def first_third(t, _):
        @pl.when(lax.rem(t, 2) == 0)
        def _():
            n = t
            sib_arrival(0, n).wait_recv()
            sib_arrival(0, n + 1).wait_recv()
        z_source_step(t)
        return 0

    lax.fori_loop(0, count, first_third, 0)

    n_tiles = acc_ref.shape[0] // tile

    def beat(u, _):
        def span(first, length):
            return (u >= first) & (u < first + length)

        z_relay_step(u)

        @pl.when(span(2, count))
        def _():
            n = u - 2
            for way in (0, 1):
                a_arrival(way, n).wait_recv()
                sib_copy(way + 1, n).start()
            even = lax.rem(n, 2) == 0

            @pl.when(even)
            def _():
                relay(0, n).start()

            @pl.when(jnp.logical_not(even))
            def _():
                relay(1, n).start()

        @pl.when(span(4, count))
        def _():
            n = u - 4
            sib_arrival(1, n).wait_recv()
            sib_arrival(2, n).wait_recv()

        @pl.when(span(6, count))
        def _():
            z_source_step(u + count - 6)

        @pl.when(corner)
        def _():
            n5 = (u - 5) // 2

            @pl.when((rank == 1) & span(5, 2 * count) & (lax.rem(u, 2) == 1))
            def _():
                for p in (3, 2):
                    det_z(p, n5).wait_recv()
                    det_z(p, n5).start()

            @pl.when((rank == 1) & span(36, count - early))
            def _():
                det_own(1, u - 36 + early).start()

            v = u - 22
            n22 = (2 * v) // 3

            @pl.when(span(22, 27) & (lax.rem(v, 3) != 1))
            def _():
                for p in (3, 2):
                    @pl.when(p > rank)
                    def _():
                        @pl.when(rank != 1)
                        def _():
                            det_z(p, n22).wait_recv()

                        det_plane(p, n22).start()

            @pl.when((rank == 0) & (span(22, early) | span(40 + early, count - early)))
            def _():
                n = jnp.where(u < 40, u - 22, u - 40)
                det_z(1, n).wait_recv()
                det_plane(1, n).start()

        w = u - 26 - 2 * h
        @pl.when(between & (w >= 0) & (w < 3 * half) & (lax.rem(w, 3) == 0))
        def _():
            n = w // 3
            for way in (0, 1):
                @pl.when(r < last_row if way == 0 else r > 0)
                def _():
                    at = rbuf.at[way, n]
                    remote(at, at, rr_send.at[way], rr.at[way, n], r, col(k, o)).wait_recv()
                    rr_copy(way, n).start()

        @pl.when(span(23, half))
        def _():
            for i in range(2):
                n = 2 * (u - 23) + i
                a_arrival(2, n).wait_recv()
                sib_copy(3, n).start()

        @pl.when(span(25, half))
        def _():
            for i in range(2):
                sib_arrival(3, 2 * (u - 25) + i).wait_recv()

        @pl.when(span(27, count))
        def _():
            z_source_step(u + 2 * count - 27)

        @pl.when(span(34, 8))
        def _():
            scale(u - 34)

        q = (u - 46) // 4
        i = lax.rem(u - 46, 4)

        @pl.when(span(46, 12) & (i == 0))
        def _():
            wait_detours(2 * q)
            wait_detours(2 * q + 1)

        @pl.when(span(46, 12) & (i < 3))
        def _():
            pair(q, (i * (n_tiles // 3), (i + 1) * (n_tiles // 3)))

        return 0

    lax.fori_loop(0, steps + 3 * lag, beat, 0)
    wait_detours(6)
    wait_detours(7)
    pair(3, (0, n_tiles))
    wait_detours(8)
    for s in range(8):
        last_ref[s] = buf[s, mine_at + 8]

    def drain(ref, sem):
        pltpu.make_async_copy(ref, ref, sem).wait()

    for d in (1, 2, 3):
        w_copy(d).wait_send()
        g_copy(d).wait_send()
        p_copy(d).wait_send()
    h_copy.wait_send()
    shard = buf.at[0, pl.ds(0, count)]
    for way in (0, 1):
        drain(shard, own_send.at[way])
        drain(buf.at[0, pl.ds(0, half)], relay_send.at[way])
    drain(buf.at[:, pl.ds(0, half)], own_send.at[2])

    @pl.when(at_source)
    def _():
        @pl.when(r > 0)
        def _():
            drain(buf.at[pl.ds(0, 2)], zsrc_send.at[0])

        @pl.when(r < last_row)
        def _():
            drain(buf.at[pl.ds(0, 2)], zsrc_send.at[1])

    @pl.when((down & (r > 0)) | ((r > k) & (r < last_row)))
    def _():
        drain(buf.at[pl.ds(0, 2)], zrel_send)

    @pl.when(corner)
    def _():
        for p in (3, 2, 1):
            @pl.when(p > rank)
            def _():
                drain(shard, deti_send.at[p])

        @pl.when(rank == 1)
        def _():
            for p in (3, 2):
                drain(shard, detz_send.at[p])

        @pl.when(rank > 0)
        def _():
            drain(shard, detz_send.at[0])

        @pl.when(rank == 3)
        def _():
            drain(shard, detz_send.at[1])

    @pl.when(between)
    def _():
        for way in (0, 1):
            @pl.when(r < last_row if way == 0 else r > 0)
            def _():
                drain(rbuf.at[0], rr_send.at[way])


def spread(x, y, w, g, factors, frequencies):
    count, _, columns = x.shape
    width = g.shape[0]
    half = count // 2
    dma = pltpu.SemaphoreType.DMA
    vmem = pl.BlockSpec(memory_space=pltpu.VMEM)
    return pl.pallas_call(
        spread_kernel,
        out_shape=(
            pltpu.VMEM((count * BLOCK, half * BLOCK), F32),
            pltpu.VMEM((8, count * BLOCK, columns), BF),
            pltpu.VMEM((8, BLOCK, columns), BF),
        ),
        in_specs=[vmem] * 6,
        out_specs=(vmem,) * 3,
        scratch_shapes=[
            pltpu.VMEM((8, count + half, BLOCK, columns), BF),
            pltpu.VMEM((3, count, BLOCK, columns), BF),
            pltpu.VMEM((2, half, BLOCK, columns), BF),
            pltpu.VMEM((4, columns // 4, 2 * width), BF),
            pltpu.VMEM((4, width // 2, width), BF),
            pltpu.VMEM((2, width // 2, width), F32),
            pltpu.VMEM((4, columns // 4, 2 * width), BF),
            pltpu.VMEM(frequencies.shape, F32),
            dma((4,)), dma((4,)), dma((4,)), dma((4,)), dma, dma, dma((4,)), dma((4,)),
            dma((3,)), dma((2,)), dma, dma((2,)), dma((4,)), dma((4,)), dma((2,)),
            dma((count,)), dma((count,)), dma((count,)), dma((4, count)),
            dma((3 * count,)), dma((2, half)), dma((3, count)), dma((2, half)),
        ],
        compiler_params=pltpu.CompilerParams(
            collective_id=2, has_side_effects=True, vmem_limit_bytes=30 << 20
        ),
        name="spread",
    )(x, y, w, g, factors, frequencies)


def finish_kernel(acc_ref, sa_ref, last_ref, out_ref, tail, sem, tail_sem):
    rows, columns = acc_ref.shape
    lane = last_ref.shape[1]
    parts = 4
    size = rows // parts
    done = columns - lane

    def main_copy(i):
        at = pl.ds(i * size, size)
        return pltpu.make_async_copy(
            acc_ref.at[at, pl.ds(0, done)], out_ref.at[at, pl.ds(0, done)], sem.at[i]
        )

    def tail_copy(i):
        at = pl.ds(i * size, size)
        return pltpu.make_async_copy(tail.at[at], out_ref.at[at, pl.ds(done, lane)], tail_sem.at[i])

    for i in range(parts):
        main_copy(i).start()
    for i in range(parts):
        at = pl.ds(i * size, size)
        total = jnp.zeros((size, lane), F32)
        for s in range(8):
            total = total + dot_nt(sa_ref[s, at, :], last_ref[s])
        tail[at] = total
        tail_copy(i).start()
    for i in range(parts):
        main_copy(i).wait()
        tail_copy(i).wait()


def finish(acc, sa, last):
    vmem = pl.BlockSpec(memory_space=pltpu.VMEM)
    dma = pltpu.SemaphoreType.DMA
    return pl.pallas_call(
        finish_kernel,
        out_shape=jax.ShapeDtypeStruct(acc.shape, F32),
        in_specs=[vmem] * 3,
        out_specs=pl.BlockSpec(memory_space=pl.ANY),
        scratch_shapes=[pltpu.VMEM((acc.shape[0], last.shape[1]), F32), dma((4,)), dma((4,))],
        compiler_params=pltpu.CompilerParams(vmem_limit_bytes=8 << 20),
        name="finish",
    )(acc, sa, last)


def per_device_square(eigvecs, reflectors, factors, frequencies, region_blocks):
    local_blocks = eigvecs.shape[0] // BLOCK
    in_hbm = functools.partial(pltpu.with_memory_space_constraint, memory_space=pltpu.HBM)
    x, y, w, g = prep(
        region_blocks,
        in_hbm(eigvecs.reshape(local_blocks, BLOCK, eigvecs.shape[1])),
        in_hbm(reflectors.reshape(2, local_blocks, BLOCK, reflectors.shape[2])),
    )
    acc, sa, last = spread(x, y, w, g, factors, frequencies.reshape(-1, 128))
    return finish(acc, sa, last)


def solution(mesh):
    shape = mesh.shape
    if shape["row"] == 4 and shape["col"] == 8:
        body = per_device_square
    else:
        body = functools.partial(per_device, shape["row"])
    return jax.shard_map(
        body,
        mesh=mesh,
        in_specs=(P("row", "col"), P(None, "row", None), P(), P(), P("row")),
        out_specs=P("row", "col"),
        check_vma=False,
    )
```

```python
import functools

import jax
import jax.numpy as jnp
from jax import lax
from jax.experimental import pallas as pl
from jax.experimental.pallas import tpu as pltpu
from jax.sharding import PartitionSpec as P

BLOCK = 128
MESH = pl.DeviceIdType.MESH
SUB = 12


def contract_rows(left, right):
    return lax.dot_general(
        left, right, (((0,), (0,)), ((), ())), preferred_element_type=jnp.float32
    )


def contract_cols(left, right):
    return lax.dot_general(
        left, right, (((1,), (1,)), ((), ())), preferred_element_type=jnp.float32
    )


def exchange_kernel(
    n_row, sub, x_ref, a_ref, b_ref, half_buf,
    own_sem, send_plane, send_sib, recv_a, send_z, recv_b, fill_sem,
):
    r = lax.axis_index("row")
    c = lax.axis_index("col")
    k = c // 2
    h = lax.rem(c, 2)
    o = 1 - h
    sib = 2 * k + o
    rows, cols = x_ref.shape
    step = rows // sub
    hsub = sub // 2
    half = rows // 2
    has_up = (r < n_row - 1).astype(jnp.int32)
    has_dn = (r > 0).astype(jnp.int32)

    barrier = pltpu.get_barrier_semaphore()

    def greet(row, col):
        pl.semaphore_signal(barrier, inc=1, device_id=(row, col), device_id_type=MESH)

    greet(r, sib)
    for d in range(1, n_row):
        greet(r, 2 * (k ^ d) + h)

    @pl.when(r < n_row - 1)
    def _():
        greet(r + 1, c)

    @pl.when(r > 0)
    def _():
        greet(r - 1, c)

    pl.semaphore_wait(barrier, n_row + has_up + has_dn)

    def piece_cols(d, side):
        owner = 2 * (k ^ d) + (h if side == 0 else o)
        return pl.ds(pl.multiple_of(owner * cols, cols), cols)

    def a_at(d, side, s):
        return a_ref.at[pl.ds(s * step, step), piece_cols(d, side)]

    def plane_copy(d, s):
        return pltpu.make_async_remote_copy(
            src_ref=x_ref.at[pl.ds(s * step, step), :],
            dst_ref=a_ref.at[pl.ds(s * step, step), piece_cols(0, 0)],
            send_sem=send_plane.at[d, s], recv_sem=recv_a.at[d, 0, s],
            device_id=(r, 2 * (k ^ d) + h), device_id_type=MESH,
        )

    def sib_copy(d, s):
        src = x_ref.at[pl.ds(s * step, step), :] if d == 0 else a_at(d, 0, s)
        return pltpu.make_async_remote_copy(
            src_ref=src, dst_ref=a_at(d, 0, s),
            send_sem=send_sib.at[d, s], recv_sem=recv_a.at[d, 1, s],
            device_id=(r, sib), device_id_type=MESH,
        )

    def half_rows(t):
        return pl.ds(pl.multiple_of(h * half + t * step, step), step)

    def z_copy(src, way, target, d, side, t):
        return pltpu.make_async_remote_copy(
            src_ref=src,
            dst_ref=b_ref.at[pl.ds(t * step, step), piece_cols(d, side)],
            send_sem=send_z.at[way, d, side, t], recv_sem=recv_b.at[d, side, t],
            device_id=(target, c), device_id_type=MESH,
        )

    def from_source(way, target, d, side, t):
        if d == 0 and side == 0:
            src = x_ref.at[half_rows(t), :]
        else:
            src = a_ref.at[half_rows(t), piece_cols(d, side)]
        return z_copy(src, way, target, d, side, t)

    def relay(way, target, d, side, t):
        src = b_ref.at[pl.ds(t * step, step), piece_cols(d, side)]
        return z_copy(src, way, target, d, side, t)

    own = pltpu.make_async_copy(x_ref, a_ref.at[:, piece_cols(0, 0)], own_sem)
    own.start()
    for s in range(sub):
        sib_copy(0, s).start()
    for d in range(1, n_row):
        for s in range(sub):
            plane_copy(d, s).start()

    arrivals = [(d, s) for d in range(1, n_row) for s in range(sub)]
    parts = [(d, side, t) for d in range(n_row) for side in (0, 1) for t in range(hsub)]

    def take_a(d, s):
        plane_copy(d, s).wait_recv()
        sib_copy(d, s).start()

    at_source = r == k
    above = r > k
    below = r < k

    @pl.when(at_source)
    def _():
        def push(d, side, t):
            @pl.when(r < n_row - 1)
            def _():
                from_source(0, r + 1, d, side, t).start()

            @pl.when(r > 0)
            def _():
                from_source(1, r - 1, d, side, t).start()

        for d in range(n_row):
            if d:
                for s in range(sub):
                    take_a(d, s)
            else:
                for t in range(hsub):
                    push(d, 0, t)
            for s in range(sub):
                sib_copy(d, s).wait_recv()
            for side in (0, 1) if d else (1,):
                for t in range(hsub):
                    push(d, side, t)
        own.wait()
        fill = pltpu.make_async_copy(
            a_ref.at[pl.ds(pl.multiple_of(h * half, half), half), :], half_buf, fill_sem
        )
        fill.start()
        fill.wait()
        out = pltpu.make_async_copy(half_buf, b_ref, fill_sem)
        out.start()
        out.wait()

    @pl.when(jnp.logical_not(at_source))
    def _():
        for i, (d, side, t) in enumerate(parts):
            if i < len(arrivals):
                take_a(*arrivals[i])
            relay(0, r, d, side, t).wait_recv()

            @pl.when(above & (r < n_row - 1))
            def _():
                relay(0, r + 1, d, side, t).start()

            @pl.when(below & (r > 0))
            def _():
                relay(1, r - 1, d, side, t).start()

        for d, s in arrivals[len(parts):]:
            take_a(d, s)
        for d in range(n_row):
            for s in range(sub):
                sib_copy(d, s).wait_recv()
        own.wait()

    for d in range(n_row):
        for s in range(sub):
            sib_copy(d, s).wait_send()
            if d:
                plane_copy(d, s).wait_send()
    for d, side, t in parts:
        @pl.when((r >= k) & (r < n_row - 1))
        def _():
            relay(0, r, d, side, t).wait_send()

        @pl.when((r <= k) & (r > 0))
        def _():
            relay(1, r, d, side, t).wait_send()


def exchange(x, n_row):
    rows, cols = x.shape
    n_col = 2 * n_row
    sub = SUB if n_row <= 4 else SUB // 2
    hsub = sub // 2
    dma = pltpu.SemaphoreType.DMA
    return pl.pallas_call(
        functools.partial(exchange_kernel, n_row, sub),
        out_shape=(
            jax.ShapeDtypeStruct((rows, cols * n_col), x.dtype),
            jax.ShapeDtypeStruct((rows // 2, cols * n_col), x.dtype),
        ),
        in_specs=[pl.BlockSpec(memory_space=pltpu.VMEM)],
        out_specs=(pl.BlockSpec(memory_space=pl.ANY),) * 2,
        scratch_shapes=[
            pltpu.VMEM((rows // 2, cols * n_col), x.dtype),
            dma,
            dma((n_row, sub)),
            dma((n_row, sub)),
            dma((n_row, 2, sub)),
            dma((2, n_row, 2, hsub)),
            dma((n_row, 2, hsub)),
            dma,
        ],
        compiler_params=pltpu.CompilerParams(collective_id=0, has_side_effects=True),
        name="exchange",
    )(x)


def project_kernel(
    n_row, w_ref, g_ref, t_ref, p_ref,
    w_in, g_in, w_sum, g_sum, w_full, g_full, send_1, recv_1, send_2, recv_2,
):
    r = lax.axis_index("row")
    c = lax.axis_index("col")
    barrier = pltpu.get_barrier_semaphore()
    for d in range(1, n_row):
        pl.semaphore_signal(barrier, inc=1, device_id=(r ^ d, c), device_id_type=MESH)
    pl.semaphore_wait(barrier, n_row - 1)
    pairs = ((w_ref, w_in, w_sum, w_full), (g_ref, g_in, g_sum, g_full))

    def part(array, owner):
        size = array.shape[0] // n_row
        return pl.ds(pl.multiple_of(owner * size, size), size)

    def scatter(d, i):
        array, landing, _, _ = pairs[i]
        return pltpu.make_async_remote_copy(
            src_ref=array.at[part(array, r ^ d), :], dst_ref=landing.at[d],
            send_sem=send_1.at[d, i], recv_sem=recv_1.at[d, i],
            device_id=(r ^ d, c), device_id_type=MESH,
        )

    def spread(d, i):
        array, _, total, full = pairs[i]
        return pltpu.make_async_remote_copy(
            src_ref=total, dst_ref=full.at[part(array, r), :],
            send_sem=send_2.at[d, i], recv_sem=recv_2.at[d, i],
            device_id=(r ^ d, c), device_id_type=MESH,
        )

    every = [(d, i) for d in range(1, n_row) for i in (1, 0)]
    for d, i in every:
        scatter(d, i).start()
    for d, i in every:
        scatter(d, i).wait_recv()
    for i in (1, 0):
        array, landing, total, full = pairs[i]
        value = array[part(array, r), :]
        for d in range(1, n_row):
            value = value + landing[d]
        total[...] = value
    for i in (1, 0):
        array, _, total, full = pairs[i]
        full[part(array, r), :] = total[...]
    for d, i in every:
        spread(d, i).start()
    for d, i in every:
        spread(d, i).wait_recv()
    highest = lax.Precision.HIGHEST
    width = g_ref.shape[0]
    second = jnp.dot(
        t_ref[1], w_full[width:, :], precision=highest, preferred_element_type=jnp.float32
    ).astype(jnp.bfloat16)
    first = w_full[:width, :] - jnp.dot(
        g_full[...], second.astype(jnp.float32),
        precision=highest, preferred_element_type=jnp.float32,
    )
    first = jnp.dot(t_ref[0], first, precision=highest, preferred_element_type=jnp.float32)
    p_ref[0] = first.astype(jnp.bfloat16)
    p_ref[1] = second
    for d, i in every:
        scatter(d, i).wait_send()
        spread(d, i).wait_send()


def project(w, g, factors, n_row):
    dma = pltpu.SemaphoreType.DMA((n_row, 2))
    width, columns = g.shape[0], w.shape[1]
    vmem = pl.BlockSpec(memory_space=pltpu.VMEM)

    def landing(array):
        return pltpu.VMEM((n_row, array.shape[0] // n_row, array.shape[1]), jnp.float32)

    def total(array):
        return pltpu.VMEM((array.shape[0] // n_row, array.shape[1]), jnp.float32)

    return pl.pallas_call(
        functools.partial(project_kernel, n_row),
        out_shape=jax.ShapeDtypeStruct((2, width, columns), jnp.bfloat16),
        in_specs=[vmem] * 3,
        out_specs=vmem,
        scratch_shapes=[
            landing(w), landing(g), total(w), total(g),
            pltpu.VMEM(w.shape, jnp.float32), pltpu.VMEM(g.shape, jnp.float32),
            dma, dma, dma, dma,
        ],
        compiler_params=pltpu.CompilerParams(collective_id=1, has_side_effects=True),
        name="project",
    )(w, g, factors)


def region_kernel(index_ref, p_ref, vecs_ref, refl_ref, out_ref, vecs, refl, sems):
    count = vecs.shape[0]

    def copies(b):
        at = index_ref[b]
        return (
            pltpu.make_async_copy(vecs_ref.at[at], vecs.at[b], sems.at[b, 0]),
            pltpu.make_async_copy(refl_ref.at[0, at], refl.at[0, b], sems.at[b, 1]),
            pltpu.make_async_copy(refl_ref.at[1, at], refl.at[1, b], sems.at[b, 2]),
        )

    for b in range(count):
        for copy in copies(b):
            copy.start()
    for b in range(count):
        for copy in copies(b):
            copy.wait()
        value = vecs[b].astype(jnp.float32)
        value = value - jnp.dot(refl[1, b], p_ref[1], preferred_element_type=jnp.float32)
        value = value - jnp.dot(refl[0, b], p_ref[0], preferred_element_type=jnp.float32)
        out_ref[b] = value.astype(out_ref.dtype)


def region_rows(index, applied, vecs, refl):
    count = index.shape[0]
    columns, width = vecs.shape[2], refl.shape[3]
    vmem = pl.BlockSpec(memory_space=pltpu.VMEM)
    hbm = pl.BlockSpec(memory_space=pl.ANY)
    return pl.pallas_call(
        region_kernel,
        out_shape=jax.ShapeDtypeStruct((count, BLOCK, columns), vecs.dtype),
        in_specs=[pl.BlockSpec(memory_space=pltpu.SMEM), vmem, hbm, hbm],
        out_specs=vmem,
        scratch_shapes=[
            pltpu.VMEM((count, BLOCK, columns), vecs.dtype),
            pltpu.VMEM((2, count, BLOCK, width), refl.dtype),
            pltpu.SemaphoreType.DMA((count, 3)),
        ],
        name="region",
    )(index, applied, vecs, refl)


def per_device(n_row, eigvecs, reflectors, factors, frequencies, region_blocks):
    columns = eigvecs.shape[1]
    width = reflectors.shape[2]
    local = lax.dot_general(
        reflectors, eigvecs, (((1,), (0,)), ((), ())), preferred_element_type=jnp.float32
    ).reshape(2 * width, columns)
    cross_local = contract_rows(reflectors[0], reflectors[1])
    applied = project(local, cross_local, jnp.triu(factors), n_row)
    local_blocks = eigvecs.shape[0] // BLOCK
    local_index = region_blocks - lax.axis_index("row") * local_blocks
    region = region_rows(
        local_index,
        applied,
        eigvecs.reshape(local_blocks, BLOCK, columns),
        reflectors.reshape(2, local_blocks, BLOCK, width),
    ).reshape(-1, columns)
    weight = 1.0 / jnp.tanh(frequencies / 2.0) / (2.0 * frequencies)
    mine, partner = exchange(region, n_row)
    scaled = (mine.astype(jnp.float32) * weight[None, :]).astype(jnp.bfloat16)
    return contract_cols(scaled, partner)


BF = jnp.bfloat16
F32 = jnp.float32
HIGH = lax.Precision.HIGHEST


def dot_nt(left, right, **kw):
    return lax.dot_general(left, right, (((1,), (1,)), ((), ())), preferred_element_type=F32, **kw)


def dot_tn(left, right):
    return lax.dot_general(left, right, (((0,), (0,)), ((), ())), preferred_element_type=F32)


def spread_kernel(
    chunks, index_ref, vecs_ref, refl_ref, t_ref, f_ref, acc_ref, sa_ref, last_ref,
    index, vecs, refl, w_sum, g_sum, w_ref, g_ref, index_sem, vec_sem, refl_sem, buf, tbuf, rbuf, w_in, g_in, g_full, p_full, weight,
    w_send, w_recv, g_send, g_recv, h_send, h_recv, p_send, p_recv,
    own_send, relay_send, zrel_send, zsrc_send, detz_send, deti_send, rr_send,
    ax, ay, ad, asib, zb, det, tz, rr,
):
    r = lax.axis_index("row")
    c = lax.axis_index("col")
    k = c // 2
    h = lax.rem(c, 2)
    o = 1 - h
    count = index.shape[0]
    half = count // 2
    columns = vecs.shape[2]
    width = refl.shape[3]
    blocks = vecs.shape[0] // chunks
    quarter = columns // 4
    last_row = 3

    def col(chip, core):
        return 2 * chip + core

    barrier = pltpu.get_barrier_semaphore()

    def greet(row, column):
        pl.semaphore_signal(barrier, inc=1, device_id=(row, column), device_id_type=MESH)

    for d in range(1, 4):
        greet(lax.rem(r + d, 4), c)
    for d in (1, 2):
        for core in (0, 1):
            greet(r, col(k ^ d, core))
    greet(r, col(k, o))

    def load(i):
        part = pl.ds(i * blocks, blocks)
        return (
            pltpu.make_async_copy(vecs_ref.at[part], vecs.at[part], vec_sem.at[i]),
            pltpu.make_async_copy(refl_ref.at[0, part], refl.at[0, part], refl_sem.at[i, 0]),
            pltpu.make_async_copy(refl_ref.at[1, part], refl.at[1, part], refl_sem.at[i, 1]),
        )

    ahead = 3
    for i in range(ahead):
        for copy in load(i):
            copy.start()
    index_copy = pltpu.make_async_copy(index_ref, index, index_sem)
    index_copy.start()
    rows = blocks * BLOCK
    for i in range(chunks):
        if i + ahead < chunks:
            for copy in load(i + ahead):
                copy.start()
        for copy in load(i):
            copy.wait()
        part = pl.ds(i * blocks, blocks)
        e = vecs[part].reshape(rows, columns)
        y0 = refl[0, part].reshape(rows, width)
        y1 = refl[1, part].reshape(rows, width)
        w = dot_tn(e, jnp.concatenate([y0, y1], axis=1))
        g = dot_tn(y0, y1)
        if i:
            w = w + w_sum[...]
            g = g + g_sum[...]
        w_sum[...] = w
        g_sum[...] = g
    w_ref[...] = w.astype(BF)
    g_ref[...] = g.astype(BF)
    index_copy.wait()

    pl.semaphore_wait(barrier, 8)

    def remote(src, dst, send, recv, row, column):
        return pltpu.make_async_remote_copy(
            src_ref=src, dst_ref=dst, send_sem=send, recv_sem=recv,
            device_id=(row, column), device_id_type=MESH,
        )

    def w_copy(d):
        q = lax.rem(r + d, 4)
        part = pl.ds(pl.multiple_of(q * quarter, quarter), quarter)
        return remote(w_ref.at[part], w_in.at[d], w_send.at[d], w_recv.at[d], q, c)

    g_half = width // 2

    def g_copy(d):
        q = lax.rem(r + d, 4)
        part = pl.ds(pl.multiple_of(h * g_half, g_half), g_half)
        return remote(g_ref.at[part], g_in.at[d], g_send.at[d], g_recv.at[d], q, c)

    for d in (2, 1, 3):
        g_copy(d).start()
        w_copy(d).start()

    f = f_ref[...]
    weight[...] = 1.0 / jnp.tanh(f / 2.0) / (2.0 * f)
    row_at = lax.broadcasted_iota(jnp.int32, (width, width), 0)
    col_at = lax.broadcasted_iota(jnp.int32, (width, width), 1)
    upper = row_at <= col_at
    zero = jnp.zeros((width, width), F32)
    t0 = jnp.where(upper, t_ref[0], zero)
    t1 = jnp.where(upper, t_ref[1], zero)

    g_part = pl.ds(pl.multiple_of(h * g_half, g_half), g_half)
    for d in (1, 2, 3):
        g_copy(d).wait_recv()
    value = g_sum[g_part, :]
    for d in (1, 2, 3):
        value = value + g_in[d].astype(F32)
    g_full[h] = value
    h_copy = remote(g_full.at[h], g_full.at[h], h_send, h_recv, r, col(k, o))
    h_copy.start()
    for d in (1, 2, 3):
        w_copy(d).wait_recv()
    mine = pl.ds(pl.multiple_of(r * quarter, quarter), quarter)
    w = w_sum[mine, :]
    for d in (1, 2, 3):
        w = w + w_in[d].astype(F32)
    second = dot_nt(w[:, width:], t1, precision=HIGH).astype(BF)
    h_copy.wait_recv()
    g = jnp.concatenate([g_full[0], g_full[1]], axis=0)
    first = w[:, :width] - dot_nt(second.astype(F32), g, precision=HIGH)
    first = dot_nt(first, t0, precision=HIGH).astype(BF)
    p_full[r, :, :width] = first
    p_full[r, :, width:] = second

    def p_copy(d):
        return remote(p_full.at[r], p_full.at[r], p_send.at[d], p_recv.at[d], lax.rem(r + d, 4), c)

    def p_arrival(d):
        q = lax.rem(r + d, 4)
        return remote(p_full.at[q], p_full.at[q], p_send.at[d], p_recv.at[4 - d], q, c)

    for d in (2, 1, 3):
        p_copy(d).start()
    for d in (1, 2, 3):
        p_arrival(d).wait_recv()

    def block_of(n):
        return lax.rem(n, 2) * half + n // 2

    def a_copy(way, n):
        b = block_of(n)
        src = buf.at[c, b]
        if way == 2:
            return remote(src, buf.at[c, b], own_send.at[2], asib.at[0, n], r, col(k, o))
        sem = ax if way == 0 else ay
        return remote(src, buf.at[c, b], own_send.at[way], sem.at[n], r, col(k ^ (way + 1), h))

    corner = (k == 0) | (k == 3)
    is_low = k == 0
    rank = jnp.where(is_low, r, 3 - r)
    away = jnp.where(is_low, -1, 1)
    slot = jnp.where(is_low, 0, 1)
    early = 5

    def det_own(hops, n):
        b = block_of(n)
        return remote(
            buf.at[c, b], tbuf.at[rank - 1, b], detz_send.at[hops - 1], tz.at[rank - 1, n],
            r + away * hops, c,
        )

    down = r < k
    at_source = r == k
    step = jnp.where(down, -1, 1)
    depth = jnp.where(down, k, 3 - k)

    def z_piece(t, depth, is_down):
        third = t // (2 * half)
        n = jnp.where(third == 0, lax.rem(t, half), lax.rem(t, 2 * half) // 2)
        e = jnp.where(third == 0, t // half, lax.rem(t, 2))
        j1 = jnp.where(depth == 3, 2, 3)
        j2 = 6 - depth - j1
        j = jnp.where(third == 0, depth, jnp.where(third == 1, j1, j2))
        j = jnp.where(is_down, j, 3 - j)
        return col(j, lax.rem(h + e, 2)), n

    steps = 3 * 2 * half

    def z_relay(t):
        src, n = z_piece(t, depth, down)
        at = buf.at[src, count + n]
        return remote(at, at, zrel_send, zb.at[t], r + step, c)

    def z_source(t, is_down):
        src, n = z_piece(t, k if is_down else 3 - k, jnp.bool_(is_down))
        return remote(
            buf.at[src, h * half + n], buf.at[src, count + n],
            zsrc_send.at[0 if is_down else 1], zb.at[t], r + (-1 if is_down else 1), c,
        )

    def z_source_step(t):
        @pl.when(at_source)
        def _():
            @pl.when(r > 0)
            def _():
                z_source(t, True).start()

            @pl.when(r < last_row)
            def _():
                z_source(t, False).start()

    applied = p_full[...].reshape(columns, 2 * width)

    base = r * vecs.shape[0]

    def make_region(n, _):
        b = block_of(n)
        at = jnp.clip(index[b] - base, 0, vecs.shape[0] - 1)
        y = jnp.concatenate([refl[0, at], refl[1, at]], axis=1)
        buf[c, b] = (vecs[at].astype(F32) - dot_nt(y, applied)).astype(BF)
        for way in (0, 1, 2):
            a_copy(way, n).start()

        @pl.when(corner & ((rank > 1) | ((rank == 1) & (n < early))))
        def _():
            @pl.when(rank == 3)
            def _():
                det_own(2, n).start()

            det_own(1, n).start()

        @pl.when(lax.rem(n, 2) == h)
        def _():
            z_source_step(n // 2)

        return 0

    lax.fori_loop(0, count, make_region, 0)

    def a_arrival(way, n):
        src = col(k ^ (way + 1), h)
        b = block_of(n)
        at = buf.at[src, b]
        sem = (ax, ay, ad)[way]
        return remote(at, at, own_send.at[2], sem.at[n], r, col(k, o))

    def sib_copy(j, n):
        src = col(k ^ j, h)
        b = block_of(n)
        at = buf.at[src, b]
        return remote(at, at, own_send.at[2], asib.at[j, n], r, col(k, o))

    def sib_arrival(j, n):
        src = col(k ^ j, o)
        b = block_of(n)
        at = buf.at[src, b]
        return remote(at, at, own_send.at[2], asib.at[j, n], r, col(k, o))

    def relay(way, n):
        src = col(k ^ (way + 1), h)
        at = buf.at[src, block_of(n)]
        to = k ^ (2 - way)
        return remote(at, at, relay_send.at[way], ad.at[n], r, col(to, h))

    def det_z(p, n):
        at = tbuf.at[p - 1, block_of(n)]
        return remote(at, at, detz_send.at[p], tz.at[p - 1, n], r + away, c)

    def det_plane(p, n):
        b = block_of(n)
        src = tbuf.at[p - 1, b]
        core = lax.rem(n, 2)
        if p < 3:
            return remote(
                src, buf.at[c, count + n // 2], deti_send.at[p], det.at[h, n // 2],
                r, col(k ^ p, core),
            )
        return remote(
            src, rbuf.at[slot, n // 2], deti_send.at[p], rr.at[slot, n // 2],
            r, col(k ^ (1 + h), core),
        )

    between = (k == 1) | (k == 2)

    def rr_copy(way, n):
        low = k - 1 if way == 0 else 2 - k
        src = low if way == 0 else low + 6
        return remote(
            rbuf.at[way, n], buf.at[src, count + n], rr_send.at[way], det.at[low, n],
            r, col(3 if way == 0 else 0, h),
        )

    def det_arrival(low, n):
        src = jnp.where(down, low, low + 6)
        at = buf.at[src, count + n]
        return remote(at, at, own_send.at[2], det.at[low, n], r, col(k, o))

    mine_at = jnp.where(at_source, h * half, count)

    from_low = jnp.logical_not(down | (at_source & (k >= 2)))
    deep = jnp.where(from_low, 3 - k, k)
    mid = jnp.where(deep == 3, 2, 3)
    order = []
    for j in (deep, mid, 6 - deep - mid, 0):
        j = jnp.where(from_low, 3 - j, j)
        order += [col(j, 0), col(j, 1)]

    def at_place(s):
        src = order[0]
        for i in range(1, 8):
            src = jnp.where(s == i, order[i], src)
        return src

    def scale(s, part):
        src = at_place(s)
        wt = jnp.concatenate([weight[pl.ds(2 * src, 1), :], weight[pl.ds(2 * src + 1, 1), :]], axis=1)

        def one(i, _):
            b = part * half + i
            rows = pl.ds(pl.multiple_of(b * BLOCK, BLOCK), BLOCK)
            sa_ref[s, rows, :] = (buf[src, b].astype(F32) * wt).astype(BF)
            return 0

        lax.fori_loop(0, half, one, 0)

    tile = 256

    def product(block, lane, size, third, places, add):
        at = mine_at + block
        lanes = pl.ds(pl.multiple_of(lane, BLOCK), size * BLOCK)

        def one(i, _):
            rows = pl.ds(pl.multiple_of(i * tile, tile), tile)
            total = jnp.zeros((tile, size * BLOCK), F32)
            for s in places:
                right = buf[order[s], pl.ds(at, size)].reshape(size * BLOCK, columns)
                total = total + dot_nt(sa_ref[s, rows, :], right)
            if add:
                total = total + acc_ref[rows, lanes]
            acc_ref[rows, lanes] = total
            return 0

        lax.fori_loop(third * (n_tiles // 3), (third + 1) * (n_tiles // 3), one, 0)

    def pair(q, third, places, add):
        product(2 * q, q * tile, 2, third, places, add)

    def wait_detours(n):
        @pl.when(jnp.logical_not(at_source))
        def _():
            for low in (0, 1):
                det_arrival(low, n).wait_recv()

    hops = jnp.where(down, k - r, r - k)
    lag = 2

    def z_relay_step(u):
        t = u - lag * hops

        @pl.when(jnp.logical_not(at_source) & (t >= 0) & (t < steps))
        def _():
            z_relay(t).wait_recv()

            @pl.when((down & (r > 0)) | (jnp.logical_not(down) & (r < last_row)))
            def _():
                z_relay(t).start()

    def first_third(n, _):
        sib_arrival(0, 2 * n).wait_recv()
        sib_arrival(0, 2 * n + 1).wait_recv()
        z_source_step(half + n)
        return 0

    lax.fori_loop(0, half, first_third, 0)

    n_tiles = acc_ref.shape[0] // tile

    def beat(u, _):
        def span(first, length):
            return (u >= first) & (u < first + length)

        z_relay_step(u)

        @pl.when(span(2, count))
        def _():
            n = u - 2
            for way in (0, 1):
                a_arrival(way, n).wait_recv()
                sib_copy(way + 1, n).start()
            even = lax.rem(n, 2) == 0

            @pl.when(even)
            def _():
                relay(0, n).start()

            @pl.when(jnp.logical_not(even))
            def _():
                relay(1, n).start()

        @pl.when(span(4, count))
        def _():
            n = u - 4
            sib_arrival(1, n).wait_recv()
            sib_arrival(2, n).wait_recv()

        @pl.when(span(6, count))
        def _():
            z_source_step(u + count - 6)

        @pl.when(corner)
        def _():
            n5 = (u - 5) // 2

            @pl.when((rank == 1) & span(5, 2 * count) & (lax.rem(u, 2) == 1))
            def _():
                for p in (3, 2):
                    det_z(p, n5).wait_recv()
                    det_z(p, n5).start()

            @pl.when((rank == 1) & span(36, count - early))
            def _():
                det_own(1, u - 36 + early).start()

            v = u - 22
            n22 = (2 * v) // 3

            @pl.when(span(22, 27) & (lax.rem(v, 3) != 1))
            def _():
                for p in (3, 2):
                    @pl.when(p > rank)
                    def _():
                        @pl.when(rank != 1)
                        def _():
                            det_z(p, n22).wait_recv()

                        det_plane(p, n22).start()

            @pl.when((rank == 0) & (span(22, early) | span(40 + early, count - early)))
            def _():
                n = jnp.where(u < 40, u - 22, u - 40)
                det_z(1, n).wait_recv()
                det_plane(1, n).start()

        w = u - 26 - 2 * h
        @pl.when(between & (w >= 0) & (w < 3 * half) & (lax.rem(w, 3) == 0))
        def _():
            n = w // 3
            for way in (0, 1):
                @pl.when(r < last_row if way == 0 else r > 0)
                def _():
                    at = rbuf.at[way, n]
                    remote(at, at, rr_send.at[way], rr.at[way, n], r, col(k, o)).wait_recv()
                    rr_copy(way, n).start()

        @pl.when(span(23, half))
        def _():
            for i in range(2):
                n = 2 * (u - 23) + i
                a_arrival(2, n).wait_recv()
                sib_copy(3, n).start()

        @pl.when(span(25, half))
        def _():
            for i in range(2):
                sib_arrival(3, 2 * (u - 25) + i).wait_recv()

        @pl.when(span(27, count))
        def _():
            z_source_step(u + 2 * count - 27)

        for first, length, place in ((6, 4, 0), (22, 4, 2), (34, 8, 4)):
            @pl.when(span(first, length))
            def _():
                scale(place + (u - first) // 2, lax.rem(u - first, 2))

        for first, q in ((27, 0), (31, 1), (42, 2)):
            @pl.when(span(first, 3))
            def _():
                pair(q, u - first, range(4), False)

        q = (u - 46) // 4
        i = lax.rem(u - 46, 4)

        @pl.when((u == 45) | (u == 49) | (u == 53))
        def _():
            pair(3, (u - 45) // 4, range(4), False)

        @pl.when(span(46, 12) & (i == 0))
        def _():
            wait_detours(2 * q)
            wait_detours(2 * q + 1)

        @pl.when(span(46, 12) & (i < 3))
        def _():
            pair(q, i, range(4, 8), True)

        @pl.when(span(57, 3))
        def _():
            product(8, 4 * tile, 1, u - 57, range(4), False)

        return 0

    lax.fori_loop(0, steps + 3 * lag, beat, 0)
    wait_detours(6)
    wait_detours(7)
    wait_detours(8)
    for s in range(4):
        last_ref[s] = buf[order[4 + s], pl.ds(mine_at + 6, 3)]

    def drain(ref, sem):
        pltpu.make_async_copy(ref, ref, sem).wait()

    for d in (1, 2, 3):
        w_copy(d).wait_send()
        g_copy(d).wait_send()
        p_copy(d).wait_send()
    h_copy.wait_send()
    shard = buf.at[0, pl.ds(0, count)]
    for way in (0, 1):
        drain(shard, own_send.at[way])
        drain(buf.at[0, pl.ds(0, half)], relay_send.at[way])
    drain(buf.at[:, pl.ds(0, half)], own_send.at[2])

    @pl.when(at_source)
    def _():
        @pl.when(r > 0)
        def _():
            drain(buf.at[pl.ds(0, 2)], zsrc_send.at[0])

        @pl.when(r < last_row)
        def _():
            drain(buf.at[pl.ds(0, 2)], zsrc_send.at[1])

    @pl.when((down & (r > 0)) | ((r > k) & (r < last_row)))
    def _():
        drain(buf.at[pl.ds(0, 2)], zrel_send)

    @pl.when(corner)
    def _():
        for p in (3, 2, 1):
            @pl.when(p > rank)
            def _():
                drain(shard, deti_send.at[p])

        @pl.when(rank == 1)
        def _():
            for p in (3, 2):
                drain(shard, detz_send.at[p])

        @pl.when(rank > 0)
        def _():
            drain(shard, detz_send.at[0])

        @pl.when(rank == 3)
        def _():
            drain(shard, detz_send.at[1])

    @pl.when(between)
    def _():
        for way in (0, 1):
            @pl.when(r < last_row if way == 0 else r > 0)
            def _():
                drain(rbuf.at[0], rr_send.at[way])


def spread(index, vecs, refl, factors, frequencies):
    count = index.shape[0]
    columns, width = vecs.shape[2], refl.shape[3]
    chunks = 10
    half = count // 2
    dma = pltpu.SemaphoreType.DMA
    vmem = pl.BlockSpec(memory_space=pltpu.VMEM)
    hbm = pl.BlockSpec(memory_space=pltpu.HBM)
    return pl.pallas_call(
        functools.partial(spread_kernel, chunks),
        out_shape=(
            pltpu.VMEM((count * BLOCK, half * BLOCK), F32),
            pltpu.VMEM((8, count * BLOCK, columns), BF),
            pltpu.VMEM((4, 3, BLOCK, columns), BF),
        ),
        in_specs=[hbm] * 3 + [vmem] * 2,
        out_specs=(vmem,) * 3,
        scratch_shapes=[
            pltpu.SMEM((count,), jnp.int32),
            pltpu.VMEM(vecs.shape, BF),
            pltpu.VMEM(refl.shape, BF),
            pltpu.VMEM((columns, 2 * width), F32),
            pltpu.VMEM((width, width), F32),
            pltpu.VMEM((columns, 2 * width), BF),
            pltpu.VMEM((width, width), BF),
            dma, dma((chunks,)), dma((chunks, 2)),
            pltpu.VMEM((8, count + half, BLOCK, columns), BF),
            pltpu.VMEM((3, count, BLOCK, columns), BF),
            pltpu.VMEM((2, half, BLOCK, columns), BF),
            pltpu.VMEM((4, columns // 4, 2 * width), BF),
            pltpu.VMEM((4, width // 2, width), BF),
            pltpu.VMEM((2, width // 2, width), F32),
            pltpu.VMEM((4, columns // 4, 2 * width), BF),
            pltpu.VMEM(frequencies.shape, F32),
            dma((4,)), dma((4,)), dma((4,)), dma((4,)), dma, dma, dma((4,)), dma((4,)),
            dma((3,)), dma((2,)), dma, dma((2,)), dma((4,)), dma((4,)), dma((2,)),
            dma((count,)), dma((count,)), dma((count,)), dma((4, count)),
            dma((3 * count,)), dma((2, half)), dma((3, count)), dma((2, half)),
        ],
        compiler_params=pltpu.CompilerParams(
            collective_id=2, has_side_effects=True, vmem_limit_bytes=36 << 20
        ),
        name="spread",
    )(index, vecs, refl, factors, frequencies)


def finish_kernel(acc_ref, sa_ref, last_ref, out_ref, tail, sem, pair_sem, single_sem):
    rows, columns = acc_ref.shape
    held, blocks, lane, depth = last_ref.shape
    parts = 4
    size = rows // parts
    done = columns - blocks * lane

    def at(i):
        return pl.ds(i * size, size)

    def main_copy(i):
        lanes = pl.ds(0, done)
        return pltpu.make_async_copy(acc_ref.at[at(i), lanes], out_ref.at[at(i), lanes], sem.at[i])

    def pair_copy(i):
        return pltpu.make_async_copy(
            tail.at[at(i), pl.ds(0, 2 * lane)], out_ref.at[at(i), pl.ds(done, 2 * lane)], pair_sem.at[i]
        )

    def single_copy(i):
        return pltpu.make_async_copy(
            tail.at[at(i), pl.ds(2 * lane, lane)],
            out_ref.at[at(i), pl.ds(columns - lane, lane)], single_sem.at[i],
        )

    for i in range(parts):
        main_copy(i).start()
    for first, count, copy in ((0, 2, pair_copy), (2, 1, single_copy)):
        lanes = pl.ds(first * lane, count * lane)
        for i in range(parts):
            total = acc_ref[at(i), pl.ds(done + first * lane, count * lane)]
            for s in range(held):
                right = last_ref[s, first:first + count].reshape(count * lane, depth)
                total = total + dot_nt(sa_ref[held + s, at(i), :], right)
            tail[at(i), lanes] = total
            copy(i).start()
    for i in range(parts):
        main_copy(i).wait()
        pair_copy(i).wait()
        single_copy(i).wait()


def finish(acc, sa, last):
    vmem = pl.BlockSpec(memory_space=pltpu.VMEM)
    dma = pltpu.SemaphoreType.DMA
    return pl.pallas_call(
        finish_kernel,
        out_shape=jax.ShapeDtypeStruct(acc.shape, F32),
        in_specs=[vmem] * 3,
        out_specs=pl.BlockSpec(memory_space=pl.ANY),
        scratch_shapes=[pltpu.VMEM((acc.shape[0], last.shape[1] * last.shape[2]), F32), dma((4,)), dma((4,)), dma((4,))],
        compiler_params=pltpu.CompilerParams(vmem_limit_bytes=8 << 20),
        name="finish",
    )(acc, sa, last)


def per_device_square(eigvecs, reflectors, factors, frequencies, region_blocks):
    local_blocks = eigvecs.shape[0] // BLOCK
    in_hbm = functools.partial(pltpu.with_memory_space_constraint, memory_space=pltpu.HBM)
    acc, sa, last = spread(
        in_hbm(region_blocks),
        in_hbm(eigvecs.reshape(local_blocks, BLOCK, eigvecs.shape[1])),
        in_hbm(reflectors.reshape(2, local_blocks, BLOCK, reflectors.shape[2])),
        factors,
        frequencies.reshape(-1, 128),
    )
    return finish(acc, sa, last)


def solution(mesh):
    shape = mesh.shape
    if shape["row"] == 4 and shape["col"] == 8:
        body = per_device_square
    else:
        body = functools.partial(per_device, shape["row"])
    return jax.shard_map(
        body,
        mesh=mesh,
        in_specs=(P("row", "col"), P(None, "row", None), P(), P(), P("row")),
        out_specs=P("row", "col"),
        check_vma=False,
    )
```

```python
import functools

import jax
import jax.numpy as jnp
from jax import lax
from jax.experimental import pallas as pl
from jax.experimental.pallas import tpu as pltpu
from jax.sharding import PartitionSpec as P

BLOCK = 128
MESH = pl.DeviceIdType.MESH
SUB = 12


def contract_rows(left, right):
    return lax.dot_general(
        left, right, (((0,), (0,)), ((), ())), preferred_element_type=jnp.float32
    )


def contract_cols(left, right):
    return lax.dot_general(
        left, right, (((1,), (1,)), ((), ())), preferred_element_type=jnp.float32
    )


def exchange_kernel(
    n_row, sub, x_ref, a_ref, b_ref, half_buf,
    own_sem, send_plane, send_sib, recv_a, send_z, recv_b, fill_sem,
):
    r = lax.axis_index("row")
    c = lax.axis_index("col")
    k = c // 2
    h = lax.rem(c, 2)
    o = 1 - h
    sib = 2 * k + o
    rows, cols = x_ref.shape
    step = rows // sub
    hsub = sub // 2
    half = rows // 2
    has_up = (r < n_row - 1).astype(jnp.int32)
    has_dn = (r > 0).astype(jnp.int32)

    barrier = pltpu.get_barrier_semaphore()

    def greet(row, col):
        pl.semaphore_signal(barrier, inc=1, device_id=(row, col), device_id_type=MESH)

    greet(r, sib)
    for d in range(1, n_row):
        greet(r, 2 * (k ^ d) + h)

    @pl.when(r < n_row - 1)
    def _():
        greet(r + 1, c)

    @pl.when(r > 0)
    def _():
        greet(r - 1, c)

    pl.semaphore_wait(barrier, n_row + has_up + has_dn)

    def piece_cols(d, side):
        owner = 2 * (k ^ d) + (h if side == 0 else o)
        return pl.ds(pl.multiple_of(owner * cols, cols), cols)

    def a_at(d, side, s):
        return a_ref.at[pl.ds(s * step, step), piece_cols(d, side)]

    def plane_copy(d, s):
        return pltpu.make_async_remote_copy(
            src_ref=x_ref.at[pl.ds(s * step, step), :],
            dst_ref=a_ref.at[pl.ds(s * step, step), piece_cols(0, 0)],
            send_sem=send_plane.at[d, s], recv_sem=recv_a.at[d, 0, s],
            device_id=(r, 2 * (k ^ d) + h), device_id_type=MESH,
        )

    def sib_copy(d, s):
        src = x_ref.at[pl.ds(s * step, step), :] if d == 0 else a_at(d, 0, s)
        return pltpu.make_async_remote_copy(
            src_ref=src, dst_ref=a_at(d, 0, s),
            send_sem=send_sib.at[d, s], recv_sem=recv_a.at[d, 1, s],
            device_id=(r, sib), device_id_type=MESH,
        )

    def half_rows(t):
        return pl.ds(pl.multiple_of(h * half + t * step, step), step)

    def z_copy(src, way, target, d, side, t):
        return pltpu.make_async_remote_copy(
            src_ref=src,
            dst_ref=b_ref.at[pl.ds(t * step, step), piece_cols(d, side)],
            send_sem=send_z.at[way, d, side, t], recv_sem=recv_b.at[d, side, t],
            device_id=(target, c), device_id_type=MESH,
        )

    def from_source(way, target, d, side, t):
        if d == 0 and side == 0:
            src = x_ref.at[half_rows(t), :]
        else:
            src = a_ref.at[half_rows(t), piece_cols(d, side)]
        return z_copy(src, way, target, d, side, t)

    def relay(way, target, d, side, t):
        src = b_ref.at[pl.ds(t * step, step), piece_cols(d, side)]
        return z_copy(src, way, target, d, side, t)

    own = pltpu.make_async_copy(x_ref, a_ref.at[:, piece_cols(0, 0)], own_sem)
    own.start()
    for s in range(sub):
        sib_copy(0, s).start()
    for d in range(1, n_row):
        for s in range(sub):
            plane_copy(d, s).start()

    arrivals = [(d, s) for d in range(1, n_row) for s in range(sub)]
    parts = [(d, side, t) for d in range(n_row) for side in (0, 1) for t in range(hsub)]

    def take_a(d, s):
        plane_copy(d, s).wait_recv()
        sib_copy(d, s).start()

    at_source = r == k
    above = r > k
    below = r < k

    @pl.when(at_source)
    def _():
        def push(d, side, t):
            @pl.when(r < n_row - 1)
            def _():
                from_source(0, r + 1, d, side, t).start()

            @pl.when(r > 0)
            def _():
                from_source(1, r - 1, d, side, t).start()

        for d in range(n_row):
            if d:
                for s in range(sub):
                    take_a(d, s)
            else:
                for t in range(hsub):
                    push(d, 0, t)
            for s in range(sub):
                sib_copy(d, s).wait_recv()
            for side in (0, 1) if d else (1,):
                for t in range(hsub):
                    push(d, side, t)
        own.wait()
        fill = pltpu.make_async_copy(
            a_ref.at[pl.ds(pl.multiple_of(h * half, half), half), :], half_buf, fill_sem
        )
        fill.start()
        fill.wait()
        out = pltpu.make_async_copy(half_buf, b_ref, fill_sem)
        out.start()
        out.wait()

    @pl.when(jnp.logical_not(at_source))
    def _():
        for i, (d, side, t) in enumerate(parts):
            if i < len(arrivals):
                take_a(*arrivals[i])
            relay(0, r, d, side, t).wait_recv()

            @pl.when(above & (r < n_row - 1))
            def _():
                relay(0, r + 1, d, side, t).start()

            @pl.when(below & (r > 0))
            def _():
                relay(1, r - 1, d, side, t).start()

        for d, s in arrivals[len(parts):]:
            take_a(d, s)
        for d in range(n_row):
            for s in range(sub):
                sib_copy(d, s).wait_recv()
        own.wait()

    for d in range(n_row):
        for s in range(sub):
            sib_copy(d, s).wait_send()
            if d:
                plane_copy(d, s).wait_send()
    for d, side, t in parts:
        @pl.when((r >= k) & (r < n_row - 1))
        def _():
            relay(0, r, d, side, t).wait_send()

        @pl.when((r <= k) & (r > 0))
        def _():
            relay(1, r, d, side, t).wait_send()


def exchange(x, n_row):
    rows, cols = x.shape
    n_col = 2 * n_row
    sub = SUB if n_row <= 4 else SUB // 2
    hsub = sub // 2
    dma = pltpu.SemaphoreType.DMA
    return pl.pallas_call(
        functools.partial(exchange_kernel, n_row, sub),
        out_shape=(
            jax.ShapeDtypeStruct((rows, cols * n_col), x.dtype),
            jax.ShapeDtypeStruct((rows // 2, cols * n_col), x.dtype),
        ),
        in_specs=[pl.BlockSpec(memory_space=pltpu.VMEM)],
        out_specs=(pl.BlockSpec(memory_space=pl.ANY),) * 2,
        scratch_shapes=[
            pltpu.VMEM((rows // 2, cols * n_col), x.dtype),
            dma,
            dma((n_row, sub)),
            dma((n_row, sub)),
            dma((n_row, 2, sub)),
            dma((2, n_row, 2, hsub)),
            dma((n_row, 2, hsub)),
            dma,
        ],
        compiler_params=pltpu.CompilerParams(collective_id=0, has_side_effects=True),
        name="exchange",
    )(x)


def project_kernel(
    n_row, w_ref, g_ref, t_ref, p_ref,
    w_in, g_in, w_sum, g_sum, w_full, g_full, send_1, recv_1, send_2, recv_2,
):
    r = lax.axis_index("row")
    c = lax.axis_index("col")
    barrier = pltpu.get_barrier_semaphore()
    for d in range(1, n_row):
        pl.semaphore_signal(barrier, inc=1, device_id=(r ^ d, c), device_id_type=MESH)
    pl.semaphore_wait(barrier, n_row - 1)
    pairs = ((w_ref, w_in, w_sum, w_full), (g_ref, g_in, g_sum, g_full))

    def part(array, owner):
        size = array.shape[0] // n_row
        return pl.ds(pl.multiple_of(owner * size, size), size)

    def scatter(d, i):
        array, landing, _, _ = pairs[i]
        return pltpu.make_async_remote_copy(
            src_ref=array.at[part(array, r ^ d), :], dst_ref=landing.at[d],
            send_sem=send_1.at[d, i], recv_sem=recv_1.at[d, i],
            device_id=(r ^ d, c), device_id_type=MESH,
        )

    def spread(d, i):
        array, _, total, full = pairs[i]
        return pltpu.make_async_remote_copy(
            src_ref=total, dst_ref=full.at[part(array, r), :],
            send_sem=send_2.at[d, i], recv_sem=recv_2.at[d, i],
            device_id=(r ^ d, c), device_id_type=MESH,
        )

    every = [(d, i) for d in range(1, n_row) for i in (1, 0)]
    for d, i in every:
        scatter(d, i).start()
    for d, i in every:
        scatter(d, i).wait_recv()
    for i in (1, 0):
        array, landing, total, full = pairs[i]
        value = array[part(array, r), :]
        for d in range(1, n_row):
            value = value + landing[d]
        total[...] = value
    for i in (1, 0):
        array, _, total, full = pairs[i]
        full[part(array, r), :] = total[...]
    for d, i in every:
        spread(d, i).start()
    for d, i in every:
        spread(d, i).wait_recv()
    highest = lax.Precision.HIGHEST
    width = g_ref.shape[0]
    second = jnp.dot(
        t_ref[1], w_full[width:, :], precision=highest, preferred_element_type=jnp.float32
    ).astype(jnp.bfloat16)
    first = w_full[:width, :] - jnp.dot(
        g_full[...], second.astype(jnp.float32),
        precision=highest, preferred_element_type=jnp.float32,
    )
    first = jnp.dot(t_ref[0], first, precision=highest, preferred_element_type=jnp.float32)
    p_ref[0] = first.astype(jnp.bfloat16)
    p_ref[1] = second
    for d, i in every:
        scatter(d, i).wait_send()
        spread(d, i).wait_send()


def project(w, g, factors, n_row):
    dma = pltpu.SemaphoreType.DMA((n_row, 2))
    width, columns = g.shape[0], w.shape[1]
    vmem = pl.BlockSpec(memory_space=pltpu.VMEM)

    def landing(array):
        return pltpu.VMEM((n_row, array.shape[0] // n_row, array.shape[1]), jnp.float32)

    def total(array):
        return pltpu.VMEM((array.shape[0] // n_row, array.shape[1]), jnp.float32)

    return pl.pallas_call(
        functools.partial(project_kernel, n_row),
        out_shape=jax.ShapeDtypeStruct((2, width, columns), jnp.bfloat16),
        in_specs=[vmem] * 3,
        out_specs=vmem,
        scratch_shapes=[
            landing(w), landing(g), total(w), total(g),
            pltpu.VMEM(w.shape, jnp.float32), pltpu.VMEM(g.shape, jnp.float32),
            dma, dma, dma, dma,
        ],
        compiler_params=pltpu.CompilerParams(collective_id=1, has_side_effects=True),
        name="project",
    )(w, g, factors)


def region_kernel(index_ref, p_ref, vecs_ref, refl_ref, out_ref, vecs, refl, sems):
    count = vecs.shape[0]

    def copies(b):
        at = index_ref[b]
        return (
            pltpu.make_async_copy(vecs_ref.at[at], vecs.at[b], sems.at[b, 0]),
            pltpu.make_async_copy(refl_ref.at[0, at], refl.at[0, b], sems.at[b, 1]),
            pltpu.make_async_copy(refl_ref.at[1, at], refl.at[1, b], sems.at[b, 2]),
        )

    for b in range(count):
        for copy in copies(b):
            copy.start()
    for b in range(count):
        for copy in copies(b):
            copy.wait()
        value = vecs[b].astype(jnp.float32)
        value = value - jnp.dot(refl[1, b], p_ref[1], preferred_element_type=jnp.float32)
        value = value - jnp.dot(refl[0, b], p_ref[0], preferred_element_type=jnp.float32)
        out_ref[b] = value.astype(out_ref.dtype)


def region_rows(index, applied, vecs, refl):
    count = index.shape[0]
    columns, width = vecs.shape[2], refl.shape[3]
    vmem = pl.BlockSpec(memory_space=pltpu.VMEM)
    hbm = pl.BlockSpec(memory_space=pl.ANY)
    return pl.pallas_call(
        region_kernel,
        out_shape=jax.ShapeDtypeStruct((count, BLOCK, columns), vecs.dtype),
        in_specs=[pl.BlockSpec(memory_space=pltpu.SMEM), vmem, hbm, hbm],
        out_specs=vmem,
        scratch_shapes=[
            pltpu.VMEM((count, BLOCK, columns), vecs.dtype),
            pltpu.VMEM((2, count, BLOCK, width), refl.dtype),
            pltpu.SemaphoreType.DMA((count, 3)),
        ],
        name="region",
    )(index, applied, vecs, refl)


def per_device(n_row, eigvecs, reflectors, factors, frequencies, region_blocks):
    columns = eigvecs.shape[1]
    width = reflectors.shape[2]
    local = lax.dot_general(
        reflectors, eigvecs, (((1,), (0,)), ((), ())), preferred_element_type=jnp.float32
    ).reshape(2 * width, columns)
    cross_local = contract_rows(reflectors[0], reflectors[1])
    applied = project(local, cross_local, jnp.triu(factors), n_row)
    local_blocks = eigvecs.shape[0] // BLOCK
    local_index = region_blocks - lax.axis_index("row") * local_blocks
    region = region_rows(
        local_index,
        applied,
        eigvecs.reshape(local_blocks, BLOCK, columns),
        reflectors.reshape(2, local_blocks, BLOCK, width),
    ).reshape(-1, columns)
    weight = 1.0 / jnp.tanh(frequencies / 2.0) / (2.0 * frequencies)
    mine, partner = exchange(region, n_row)
    scaled = (mine.astype(jnp.float32) * weight[None, :]).astype(jnp.bfloat16)
    return contract_cols(scaled, partner)


BF = jnp.bfloat16
F32 = jnp.float32
HIGH = lax.Precision.HIGHEST


def dot_nt(left, right, **kw):
    return lax.dot_general(left, right, (((1,), (1,)), ((), ())), preferred_element_type=F32, **kw)


def dot_tn(left, right):
    return lax.dot_general(left, right, (((0,), (0,)), ((), ())), preferred_element_type=F32)


def spread_kernel(
    chunks, index_ref, vecs_ref, refl_ref, t_ref, f_ref, acc_ref, sa_ref, last_ref,
    index, vecs, refl, w_sum, g_sum, w_ref, index_sem, vec_sem, refl_sem, buf, tbuf, rbuf, w_in, g_in, g_full, p_full, weight,
    w_send, w_recv, g_send, g_recv, h_send, h_recv, p_send, p_recv,
    own_send, relay_send, zrel_send, zsrc_send, detz_send, deti_send, rr_send,
    ax, ay, ad, asib, zb, det, tz, rr,
):
    r = lax.axis_index("row")
    c = lax.axis_index("col")
    k = c // 2
    h = lax.rem(c, 2)
    o = 1 - h
    count = index.shape[0]
    half = count // 2
    columns = vecs.shape[2]
    width = refl.shape[3]
    blocks = vecs.shape[0] // chunks
    quarter = columns // 4
    last_row = 3

    def col(chip, core):
        return 2 * chip + core

    barrier = pltpu.get_barrier_semaphore()

    def greet(row, column):
        pl.semaphore_signal(barrier, inc=1, device_id=(row, column), device_id_type=MESH)

    for d in range(1, 4):
        greet(lax.rem(r + d, 4), c)
    for e in range(1, 8):
        greet(r, c ^ e)

    def load(i):
        part = pl.ds(i * blocks, blocks)
        return (
            pltpu.make_async_copy(vecs_ref.at[part], vecs.at[part], vec_sem.at[i]),
            pltpu.make_async_copy(refl_ref.at[:, part], refl.at[:, part], refl_sem.at[i]),
        )

    ahead = 3
    for i in range(ahead):
        for copy in load(i):
            copy.start()
    index_copy = pltpu.make_async_copy(index_ref, index, index_sem)
    index_copy.start()
    rows = blocks * BLOCK
    for i in range(chunks):
        if i + ahead < chunks:
            for copy in load(i + ahead):
                copy.start()
        for copy in load(i):
            copy.wait()
        part = pl.ds(i * blocks, blocks)
        e = vecs[part].reshape(rows, columns)
        y0 = refl[0, part].reshape(rows, width)
        y1 = refl[1, part].reshape(rows, width)
        w = dot_tn(e, jnp.concatenate([y0, y1], axis=1))
        g = dot_tn(y0, y1)
        if i:
            w = w + w_sum[...]
            g = g + g_sum[...]
        w_sum[...] = w
        g_sum[...] = g
    w_ref[...] = w.astype(BF)
    index_copy.wait()

    pl.semaphore_wait(barrier, 10)

    def remote(src, dst, send, recv, row, column):
        return pltpu.make_async_remote_copy(
            src_ref=src, dst_ref=dst, send_sem=send, recv_sem=recv,
            device_id=(row, column), device_id_type=MESH,
        )

    def w_copy(d):
        q = lax.rem(r + d, 4)
        part = pl.ds(pl.multiple_of(q * quarter, quarter), quarter)
        return remote(w_ref.at[part], w_in.at[d], w_send.at[d], w_recv.at[d], q, c)

    g_rows = width // 8
    g_part = pl.ds(pl.multiple_of(c * g_rows, g_rows), g_rows)

    def g_copy(d):
        q = lax.rem(r + d, 4)
        return remote(g_sum.at[g_part], g_in.at[d], g_send.at[d], g_recv.at[d], q, c)

    for d in (2, 1, 3):
        g_copy(d).start()
        w_copy(d).start()

    f = f_ref[...]
    weight[...] = 1.0 / jnp.tanh(f / 2.0) / (2.0 * f)
    row_at = lax.broadcasted_iota(jnp.int32, (width, width), 0)
    col_at = lax.broadcasted_iota(jnp.int32, (width, width), 1)
    upper = row_at <= col_at
    zero = jnp.zeros((width, width), F32)
    t0 = jnp.where(upper, t_ref[0], zero)
    t1 = jnp.where(upper, t_ref[1], zero)

    for d in (1, 2, 3):
        g_copy(d).wait_recv()
    value = g_sum[g_part, :]
    for d in (1, 2, 3):
        value = value + g_in[d]
    g_full[c] = value

    def h_copy(e):
        return remote(g_full.at[c], g_full.at[c], h_send.at[e], h_recv.at[e], r, c ^ e)

    def h_arrival(e):
        return remote(g_full.at[c ^ e], g_full.at[c ^ e], h_send.at[e], h_recv.at[e], r, c ^ e)

    for e in range(1, 8):
        h_copy(e).start()
    for d in (1, 2, 3):
        w_copy(d).wait_recv()
    mine = pl.ds(pl.multiple_of(r * quarter, quarter), quarter)
    w = w_sum[mine, :]
    for d in (1, 2, 3):
        w = w + w_in[d].astype(F32)
    second = dot_nt(w[:, width:], t1, precision=HIGH).astype(BF)
    for e in range(1, 8):
        h_arrival(e).wait_recv()
    g = g_full[...].reshape(width, width)
    first = w[:, :width] - dot_nt(second.astype(F32), g, precision=HIGH)
    first = dot_nt(first, t0, precision=HIGH).astype(BF)
    p_full[r, :, :width] = first
    p_full[r, :, width:] = second

    def p_copy(d):
        return remote(p_full.at[r], p_full.at[r], p_send.at[d], p_recv.at[d], lax.rem(r + d, 4), c)

    def p_arrival(d):
        q = lax.rem(r + d, 4)
        return remote(p_full.at[q], p_full.at[q], p_send.at[d], p_recv.at[4 - d], q, c)

    for d in (2, 1, 3):
        p_copy(d).start()
    for d in (1, 2, 3):
        p_arrival(d).wait_recv()

    def block_of(n):
        return lax.rem(n, 2) * half + n // 2

    def a_copy(way, n):
        b = block_of(n)
        src = buf.at[c, b]
        if way == 2:
            return remote(src, buf.at[c, b], own_send.at[2], asib.at[0, n], r, col(k, o))
        sem = ax if way == 0 else ay
        return remote(src, buf.at[c, b], own_send.at[way], sem.at[n], r, col(k ^ (way + 1), h))

    corner = (k == 0) | (k == 3)
    is_low = k == 0
    rank = jnp.where(is_low, r, 3 - r)
    away = jnp.where(is_low, -1, 1)
    slot = jnp.where(is_low, 0, 1)
    early = 3

    def det_own(hops, n):
        b = block_of(n)
        return remote(
            buf.at[c, b], tbuf.at[rank - 1, b], detz_send.at[hops - 1], tz.at[rank - 1, n],
            r + away * hops, c,
        )

    down = r < k
    at_source = r == k
    step = jnp.where(down, -1, 1)
    depth = jnp.where(down, k, 3 - k)

    def z_piece(t, depth, is_down):
        third = t // (2 * half)
        n = jnp.where(third == 0, lax.rem(t, half), lax.rem(t, 2 * half) // 2)
        e = jnp.where(third == 0, t // half, lax.rem(t, 2))
        j1 = jnp.where(depth == 3, 2, 3)
        j2 = 6 - depth - j1
        j = jnp.where(third == 0, depth, jnp.where(third == 1, j1, j2))
        j = jnp.where(is_down, j, 3 - j)
        return col(j, lax.rem(h + e, 2)), n

    steps = 3 * 2 * half

    def z_relay(t):
        src, n = z_piece(t, depth, down)
        at = buf.at[src, count + n]
        return remote(at, at, zrel_send, zb.at[t], r + step, c)

    def z_source(t, is_down):
        src, n = z_piece(t, k if is_down else 3 - k, jnp.bool_(is_down))
        return remote(
            buf.at[src, h * half + n], buf.at[src, count + n],
            zsrc_send.at[0 if is_down else 1], zb.at[t], r + (-1 if is_down else 1), c,
        )

    def z_source_step(t):
        @pl.when(at_source)
        def _():
            @pl.when(r > 0)
            def _():
                z_source(t, True).start()

            @pl.when(r < last_row)
            def _():
                z_source(t, False).start()

    applied = p_full[...].reshape(columns, 2 * width)

    base = r * vecs.shape[0]

    def make_region(n, _):
        b = block_of(n)
        at = jnp.clip(index[b] - base, 0, vecs.shape[0] - 1)
        y = jnp.concatenate([refl[0, at], refl[1, at]], axis=1)
        buf[c, b] = (vecs[at].astype(F32) - dot_nt(y, applied)).astype(BF)
        for way in (0, 1, 2):
            a_copy(way, n).start()

        @pl.when(corner & ((rank > 1) | ((rank == 1) & (n < early))))
        def _():
            @pl.when(rank == 3)
            def _():
                det_own(2, n).start()

            det_own(1, n).start()

        @pl.when(lax.rem(n, 2) == h)
        def _():
            z_source_step(n // 2)

        return 0

    lax.fori_loop(0, count, make_region, 0)

    def a_arrival(way, n):
        src = col(k ^ (way + 1), h)
        b = block_of(n)
        at = buf.at[src, b]
        sem = (ax, ay, ad)[way]
        return remote(at, at, own_send.at[2], sem.at[n], r, col(k, o))

    def sib_copy(j, n):
        src = col(k ^ j, h)
        b = block_of(n)
        at = buf.at[src, b]
        return remote(at, at, own_send.at[2], asib.at[j, n], r, col(k, o))

    def sib_arrival(j, n):
        src = col(k ^ j, o)
        b = block_of(n)
        at = buf.at[src, b]
        return remote(at, at, own_send.at[2], asib.at[j, n], r, col(k, o))

    def relay(way, n):
        src = col(k ^ (way + 1), h)
        at = buf.at[src, block_of(n)]
        to = k ^ (2 - way)
        return remote(at, at, relay_send.at[way], ad.at[n], r, col(to, h))

    def det_z(p, n):
        at = tbuf.at[p - 1, block_of(n)]
        return remote(at, at, detz_send.at[p], tz.at[p - 1, n], r + away, c)

    def det_plane(p, n):
        b = block_of(n)
        src = tbuf.at[p - 1, b]
        core = lax.rem(n, 2)
        if p < 3:
            return remote(
                src, buf.at[c, count + n // 2], deti_send.at[p], det.at[h, n // 2],
                r, col(k ^ p, core),
            )
        return remote(
            src, rbuf.at[slot, n // 2], deti_send.at[p], rr.at[slot, n // 2],
            r, col(k ^ (1 + h), core),
        )

    between = (k == 1) | (k == 2)

    def rr_copy(way, n):
        low = k - 1 if way == 0 else 2 - k
        src = low if way == 0 else low + 6
        return remote(
            rbuf.at[way, n], buf.at[src, count + n], rr_send.at[way], det.at[low, n],
            r, col(3 if way == 0 else 0, h),
        )

    def det_arrival(low, n):
        src = jnp.where(down, low, low + 6)
        at = buf.at[src, count + n]
        return remote(at, at, own_send.at[2], det.at[low, n], r, col(k, o))

    mine_at = jnp.where(at_source, h * half, count)

    from_low = jnp.logical_not(down | (at_source & (k >= 2)))
    deep = jnp.where(from_low, 3 - k, k)
    mid = jnp.where(deep == 3, 2, 3)
    order = []
    for j in (deep, mid, 6 - deep - mid, 0):
        j = jnp.where(from_low, 3 - j, j)
        order += [col(j, 0), col(j, 1)]

    def at_place(s):
        src = order[0]
        for i in range(1, 8):
            src = jnp.where(s == i, order[i], src)
        return src

    def scale(s, part):
        src = at_place(s)
        wt = jnp.concatenate([weight[pl.ds(2 * src, 1), :], weight[pl.ds(2 * src + 1, 1), :]], axis=1)

        def one(i, _):
            b = part * half + i
            rows = pl.ds(pl.multiple_of(b * BLOCK, BLOCK), BLOCK)
            sa_ref[s, rows, :] = (buf[src, b].astype(F32) * wt).astype(BF)
            return 0

        lax.fori_loop(0, half, one, 0)

    tile = 2 * BLOCK
    row_tile = acc_ref.shape[0] // 3

    def product(block, lane, size, third, places, add):
        at = mine_at + block
        lanes = pl.ds(pl.multiple_of(lane, BLOCK), size * BLOCK)
        rows = pl.ds(pl.multiple_of(third * row_tile, row_tile), row_tile)
        total = jnp.zeros((row_tile, size * BLOCK), F32)
        for s in places:
            right = buf[order[s], pl.ds(at, size)].reshape(size * BLOCK, columns)
            total = total + dot_nt(sa_ref[s, rows, :], right)
        if add:
            total = total + acc_ref[rows, lanes]
        acc_ref[rows, lanes] = total

    def pair(q, third, places, add):
        product(2 * q, q * tile, 2, third, places, add)

    def wait_detours(n):
        @pl.when(jnp.logical_not(at_source))
        def _():
            for low in (0, 1):
                det_arrival(low, n).wait_recv()

    hops = jnp.where(down, k - r, r - k)
    lag = 2

    def z_relay_step(u):
        t = u - lag * hops

        @pl.when(jnp.logical_not(at_source) & (t >= 0) & (t < steps))
        def _():
            z_relay(t).wait_recv()

            @pl.when((down & (r > 0)) | (jnp.logical_not(down) & (r < last_row)))
            def _():
                z_relay(t).start()

    def first_third(n, _):
        sib_arrival(0, 2 * n).wait_recv()
        sib_arrival(0, 2 * n + 1).wait_recv()
        z_source_step(half + n)
        return 0

    lax.fori_loop(0, half, first_third, 0)


    def beat(u, _):
        def span(first, length):
            return (u >= first) & (u < first + length)

        z_relay_step(u)

        @pl.when(span(2, count))
        def _():
            n = u - 2
            for way in (0, 1):
                a_arrival(way, n).wait_recv()
                sib_copy(way + 1, n).start()
            even = lax.rem(n, 2) == 0

            @pl.when(even)
            def _():
                relay(0, n).start()

            @pl.when(jnp.logical_not(even))
            def _():
                relay(1, n).start()

        @pl.when(span(4, count))
        def _():
            n = u - 4
            sib_arrival(1, n).wait_recv()
            sib_arrival(2, n).wait_recv()

        @pl.when(span(6, count))
        def _():
            z_source_step(u + count - 6)

        @pl.when(corner)
        def _():
            n5 = (u - 3) // 2

            @pl.when((rank == 1) & span(3, 2 * count) & (lax.rem(u - 3, 2) == 0))
            def _():
                for p in (3, 2):
                    det_z(p, n5).wait_recv()
                    det_z(p, n5).start()

            @pl.when((rank == 1) & span(36, count - early))
            def _():
                det_own(1, u - 36 + early).start()

            v = u - 22
            n3 = (4 * v + 4) // 5

            @pl.when((rank < 3) & span(22, 22) & (lax.rem(v, 5) != 4))
            def _():
                @pl.when(rank != 1)
                def _():
                    det_z(3, n3).wait_recv()

                det_plane(3, n3).start()

            v2 = u - 28
            n2 = (2 * v2) // 3

            @pl.when((rank < 2) & span(28, 27) & (lax.rem(v2, 3) != 1))
            def _():
                @pl.when(rank != 1)
                def _():
                    det_z(2, n2).wait_recv()

                det_plane(2, n2).start()

            @pl.when((rank == 0) & (span(22, early) | span(40 + early, count - early)))
            def _():
                n = jnp.where(u < 40, u - 22, u - 40)
                det_z(1, n).wait_recv()
                det_plane(1, n).start()

        w = u - 26 - 2 * h
        @pl.when(between & (w >= 0) & (w < 3 * half) & (lax.rem(w, 3) == 0))
        def _():
            n = w // 3
            for way in (0, 1):
                @pl.when(r < last_row if way == 0 else r > 0)
                def _():
                    at = rbuf.at[way, n]
                    remote(at, at, rr_send.at[way], rr.at[way, n], r, col(k, o)).wait_recv()
                    rr_copy(way, n).start()

        @pl.when(span(23, half))
        def _():
            for i in range(2):
                n = 2 * (u - 23) + i
                a_arrival(2, n).wait_recv()
                sib_copy(3, n).start()

        @pl.when(span(25, half))
        def _():
            for i in range(2):
                sib_arrival(3, 2 * (u - 25) + i).wait_recv()

        @pl.when(span(27, count))
        def _():
            z_source_step(u + 2 * count - 27)

        for first, length, place in ((6, 4, 0), (22, 4, 2), (34, 8, 4)):
            @pl.when(span(first, length))
            def _():
                scale(place + (u - first) // 2, lax.rem(u - first, 2))

        for first, q in ((27, 0), (31, 1), (42, 2)):
            @pl.when(span(first, 3))
            def _():
                pair(q, u - first, range(4), False)

        q = (u - 46) // 4
        i = lax.rem(u - 46, 4)

        @pl.when((u == 45) | (u == 49) | (u == 53))
        def _():
            pair(3, (u - 45) // 4, range(4), False)

        @pl.when(span(46, 12) & (i == 0))
        def _():
            wait_detours(2 * q)
            wait_detours(2 * q + 1)

        @pl.when(span(46, 12) & (i < 3))
        def _():
            pair(q, i, range(4, 8), True)

        @pl.when(span(57, 3))
        def _():
            product(8, 4 * tile, 1, u - 57, range(4), False)

        return 0

    lax.fori_loop(0, steps + 3 * lag, beat, 0)
    wait_detours(6)
    wait_detours(7)
    wait_detours(8)
    for s in range(4):
        last_ref[s] = buf[order[4 + s], pl.ds(mine_at + 6, 3)]

    def drain(ref, sem):
        pltpu.make_async_copy(ref, ref, sem).wait()

    for d in (1, 2, 3):
        w_copy(d).wait_send()
        g_copy(d).wait_send()
        p_copy(d).wait_send()
    for e in range(1, 8):
        h_copy(e).wait_send()
    shard = buf.at[0, pl.ds(0, count)]
    for way in (0, 1):
        drain(shard, own_send.at[way])
        drain(buf.at[0, pl.ds(0, half)], relay_send.at[way])
    drain(buf.at[:, pl.ds(0, half)], own_send.at[2])

    @pl.when(at_source)
    def _():
        @pl.when(r > 0)
        def _():
            drain(buf.at[pl.ds(0, 2)], zsrc_send.at[0])

        @pl.when(r < last_row)
        def _():
            drain(buf.at[pl.ds(0, 2)], zsrc_send.at[1])

    @pl.when((down & (r > 0)) | ((r > k) & (r < last_row)))
    def _():
        drain(buf.at[pl.ds(0, 2)], zrel_send)

    @pl.when(corner)
    def _():
        for p in (3, 2, 1):
            @pl.when(p > rank)
            def _():
                drain(shard, deti_send.at[p])

        @pl.when(rank == 1)
        def _():
            for p in (3, 2):
                drain(shard, detz_send.at[p])

        @pl.when(rank > 0)
        def _():
            drain(shard, detz_send.at[0])

        @pl.when(rank == 3)
        def _():
            drain(shard, detz_send.at[1])

    @pl.when(between)
    def _():
        for way in (0, 1):
            @pl.when(r < last_row if way == 0 else r > 0)
            def _():
                drain(rbuf.at[0], rr_send.at[way])


def spread(index, vecs, refl, factors, frequencies):
    count = index.shape[0]
    columns, width = vecs.shape[2], refl.shape[3]
    chunks = 5
    half = count // 2
    dma = pltpu.SemaphoreType.DMA
    vmem = pl.BlockSpec(memory_space=pltpu.VMEM)
    hbm = pl.BlockSpec(memory_space=pltpu.HBM)
    return pl.pallas_call(
        functools.partial(spread_kernel, chunks),
        out_shape=(
            pltpu.VMEM((count * BLOCK, half * BLOCK), F32),
            pltpu.VMEM((8, count * BLOCK, columns), BF),
            pltpu.VMEM((4, 3, BLOCK, columns), BF),
        ),
        in_specs=[hbm] * 3 + [vmem] * 2,
        out_specs=(vmem,) * 3,
        scratch_shapes=[
            pltpu.SMEM((count,), jnp.int32),
            pltpu.VMEM(vecs.shape, BF),
            pltpu.VMEM(refl.shape, BF),
            pltpu.VMEM((columns, 2 * width), F32),
            pltpu.VMEM((width, width), F32),
            pltpu.VMEM((columns, 2 * width), BF),
            dma, dma((chunks,)), dma((chunks,)),
            pltpu.VMEM((8, count + half, BLOCK, columns), BF),
            pltpu.VMEM((3, count, BLOCK, columns), BF),
            pltpu.VMEM((2, half, BLOCK, columns), BF),
            pltpu.VMEM((4, columns // 4, 2 * width), BF),
            pltpu.VMEM((4, width // 8, width), F32),
            pltpu.VMEM((8, width // 8, width), F32),
            pltpu.VMEM((4, columns // 4, 2 * width), BF),
            pltpu.VMEM(frequencies.shape, F32),
            dma((4,)), dma((4,)), dma((4,)), dma((4,)), dma((8,)), dma((8,)), dma((4,)), dma((4,)),
            dma((3,)), dma((2,)), dma, dma((2,)), dma((4,)), dma((4,)), dma((2,)),
            dma((count,)), dma((count,)), dma((count,)), dma((4, count)),
            dma((3 * count,)), dma((2, half)), dma((3, count)), dma((2, half)),
        ],
        compiler_params=pltpu.CompilerParams(
            collective_id=2, has_side_effects=True, vmem_limit_bytes=36 << 20
        ),
        name="spread",
    )(index, vecs, refl, factors, frequencies)


def finish_kernel(acc_ref, sa_ref, last_ref, out_ref, tail, sem, pair_sem, single_sem):
    rows, columns = acc_ref.shape
    held, blocks, lane, depth = last_ref.shape
    parts = 4
    size = rows // parts
    done = columns - blocks * lane

    def at(i):
        return pl.ds(i * size, size)

    def main_copy(i):
        lanes = pl.ds(0, done)
        return pltpu.make_async_copy(acc_ref.at[at(i), lanes], out_ref.at[at(i), lanes], sem.at[i])

    def pair_copy(i):
        return pltpu.make_async_copy(
            tail.at[at(i), pl.ds(0, 2 * lane)], out_ref.at[at(i), pl.ds(done, 2 * lane)], pair_sem.at[i]
        )

    def single_copy(i):
        return pltpu.make_async_copy(
            tail.at[at(i), pl.ds(2 * lane, lane)],
            out_ref.at[at(i), pl.ds(columns - lane, lane)], single_sem.at[i],
        )

    for i in range(parts):
        main_copy(i).start()
    for first, count, copy in ((0, 2, pair_copy), (2, 1, single_copy)):
        lanes = pl.ds(first * lane, count * lane)
        for i in range(parts):
            total = acc_ref[at(i), pl.ds(done + first * lane, count * lane)]
            for s in range(held):
                right = last_ref[s, first:first + count].reshape(count * lane, depth)
                total = total + dot_nt(sa_ref[held + s, at(i), :], right)
            tail[at(i), lanes] = total
            copy(i).start()
    for i in range(parts):
        main_copy(i).wait()
        pair_copy(i).wait()
        single_copy(i).wait()


def finish(acc, sa, last):
    vmem = pl.BlockSpec(memory_space=pltpu.VMEM)
    dma = pltpu.SemaphoreType.DMA
    return pl.pallas_call(
        finish_kernel,
        out_shape=jax.ShapeDtypeStruct(acc.shape, F32),
        in_specs=[vmem] * 3,
        out_specs=pl.BlockSpec(memory_space=pl.ANY),
        scratch_shapes=[pltpu.VMEM((acc.shape[0], last.shape[1] * last.shape[2]), F32), dma((4,)), dma((4,)), dma((4,))],
        compiler_params=pltpu.CompilerParams(vmem_limit_bytes=8 << 20),
        name="finish",
    )(acc, sa, last)


def per_device_square(eigvecs, reflectors, factors, frequencies, region_blocks):
    local_blocks = eigvecs.shape[0] // BLOCK
    in_hbm = functools.partial(pltpu.with_memory_space_constraint, memory_space=pltpu.HBM)
    acc, sa, last = spread(
        in_hbm(region_blocks),
        in_hbm(eigvecs.reshape(local_blocks, BLOCK, eigvecs.shape[1])),
        in_hbm(reflectors.reshape(2, local_blocks, BLOCK, reflectors.shape[2])),
        factors,
        frequencies.reshape(-1, 128),
    )
    return finish(acc, sa, last)


def solution(mesh):
    shape = mesh.shape
    if shape["row"] == 4 and shape["col"] == 8:
        body = per_device_square
    else:
        body = functools.partial(per_device, shape["row"])
    return jax.shard_map(
        body,
        mesh=mesh,
        in_specs=(P("row", "col"), P(None, "row", None), P(), P(), P("row")),
        out_specs=P("row", "col"),
        check_vma=False,
    )
```

```python
import functools

import jax
import jax.numpy as jnp
from jax import lax
from jax.experimental import pallas as pl
from jax.experimental.pallas import tpu as pltpu
from jax.sharding import PartitionSpec as P

BLOCK = 128
MESH = pl.DeviceIdType.MESH
SUB = 12


def contract_rows(left, right):
    return lax.dot_general(
        left, right, (((0,), (0,)), ((), ())), preferred_element_type=jnp.float32
    )


def contract_cols(left, right):
    return lax.dot_general(
        left, right, (((1,), (1,)), ((), ())), preferred_element_type=jnp.float32
    )


def exchange_kernel(
    n_row, sub, x_ref, a_ref, b_ref, half_buf,
    own_sem, send_plane, send_sib, recv_a, send_z, recv_b, fill_sem,
):
    r = lax.axis_index("row")
    c = lax.axis_index("col")
    k = c // 2
    h = lax.rem(c, 2)
    o = 1 - h
    sib = 2 * k + o
    rows, cols = x_ref.shape
    step = rows // sub
    hsub = sub // 2
    half = rows // 2
    has_up = (r < n_row - 1).astype(jnp.int32)
    has_dn = (r > 0).astype(jnp.int32)

    barrier = pltpu.get_barrier_semaphore()

    def greet(row, col):
        pl.semaphore_signal(barrier, inc=1, device_id=(row, col), device_id_type=MESH)

    greet(r, sib)
    for d in range(1, n_row):
        greet(r, 2 * (k ^ d) + h)

    @pl.when(r < n_row - 1)
    def _():
        greet(r + 1, c)

    @pl.when(r > 0)
    def _():
        greet(r - 1, c)

    pl.semaphore_wait(barrier, n_row + has_up + has_dn)

    def piece_cols(d, side):
        owner = 2 * (k ^ d) + (h if side == 0 else o)
        return pl.ds(pl.multiple_of(owner * cols, cols), cols)

    def a_at(d, side, s):
        return a_ref.at[pl.ds(s * step, step), piece_cols(d, side)]

    def plane_copy(d, s):
        return pltpu.make_async_remote_copy(
            src_ref=x_ref.at[pl.ds(s * step, step), :],
            dst_ref=a_ref.at[pl.ds(s * step, step), piece_cols(0, 0)],
            send_sem=send_plane.at[d, s], recv_sem=recv_a.at[d, 0, s],
            device_id=(r, 2 * (k ^ d) + h), device_id_type=MESH,
        )

    def sib_copy(d, s):
        src = x_ref.at[pl.ds(s * step, step), :] if d == 0 else a_at(d, 0, s)
        return pltpu.make_async_remote_copy(
            src_ref=src, dst_ref=a_at(d, 0, s),
            send_sem=send_sib.at[d, s], recv_sem=recv_a.at[d, 1, s],
            device_id=(r, sib), device_id_type=MESH,
        )

    def half_rows(t):
        return pl.ds(pl.multiple_of(h * half + t * step, step), step)

    def z_copy(src, way, target, d, side, t):
        return pltpu.make_async_remote_copy(
            src_ref=src,
            dst_ref=b_ref.at[pl.ds(t * step, step), piece_cols(d, side)],
            send_sem=send_z.at[way, d, side, t], recv_sem=recv_b.at[d, side, t],
            device_id=(target, c), device_id_type=MESH,
        )

    def from_source(way, target, d, side, t):
        if d == 0 and side == 0:
            src = x_ref.at[half_rows(t), :]
        else:
            src = a_ref.at[half_rows(t), piece_cols(d, side)]
        return z_copy(src, way, target, d, side, t)

    def relay(way, target, d, side, t):
        src = b_ref.at[pl.ds(t * step, step), piece_cols(d, side)]
        return z_copy(src, way, target, d, side, t)

    own = pltpu.make_async_copy(x_ref, a_ref.at[:, piece_cols(0, 0)], own_sem)
    own.start()
    for s in range(sub):
        sib_copy(0, s).start()
    for d in range(1, n_row):
        for s in range(sub):
            plane_copy(d, s).start()

    arrivals = [(d, s) for d in range(1, n_row) for s in range(sub)]
    parts = [(d, side, t) for d in range(n_row) for side in (0, 1) for t in range(hsub)]

    def take_a(d, s):
        plane_copy(d, s).wait_recv()
        sib_copy(d, s).start()

    at_source = r == k
    above = r > k
    below = r < k

    @pl.when(at_source)
    def _():
        def push(d, side, t):
            @pl.when(r < n_row - 1)
            def _():
                from_source(0, r + 1, d, side, t).start()

            @pl.when(r > 0)
            def _():
                from_source(1, r - 1, d, side, t).start()

        for d in range(n_row):
            if d:
                for s in range(sub):
                    take_a(d, s)
            else:
                for t in range(hsub):
                    push(d, 0, t)
            for s in range(sub):
                sib_copy(d, s).wait_recv()
            for side in (0, 1) if d else (1,):
                for t in range(hsub):
                    push(d, side, t)
        own.wait()
        fill = pltpu.make_async_copy(
            a_ref.at[pl.ds(pl.multiple_of(h * half, half), half), :], half_buf, fill_sem
        )
        fill.start()
        fill.wait()
        out = pltpu.make_async_copy(half_buf, b_ref, fill_sem)
        out.start()
        out.wait()

    @pl.when(jnp.logical_not(at_source))
    def _():
        for i, (d, side, t) in enumerate(parts):
            if i < len(arrivals):
                take_a(*arrivals[i])
            relay(0, r, d, side, t).wait_recv()

            @pl.when(above & (r < n_row - 1))
            def _():
                relay(0, r + 1, d, side, t).start()

            @pl.when(below & (r > 0))
            def _():
                relay(1, r - 1, d, side, t).start()

        for d, s in arrivals[len(parts):]:
            take_a(d, s)
        for d in range(n_row):
            for s in range(sub):
                sib_copy(d, s).wait_recv()
        own.wait()

    for d in range(n_row):
        for s in range(sub):
            sib_copy(d, s).wait_send()
            if d:
                plane_copy(d, s).wait_send()
    for d, side, t in parts:
        @pl.when((r >= k) & (r < n_row - 1))
        def _():
            relay(0, r, d, side, t).wait_send()

        @pl.when((r <= k) & (r > 0))
        def _():
            relay(1, r, d, side, t).wait_send()


def exchange(x, n_row):
    rows, cols = x.shape
    n_col = 2 * n_row
    sub = SUB if n_row <= 4 else SUB // 2
    hsub = sub // 2
    dma = pltpu.SemaphoreType.DMA
    return pl.pallas_call(
        functools.partial(exchange_kernel, n_row, sub),
        out_shape=(
            jax.ShapeDtypeStruct((rows, cols * n_col), x.dtype),
            jax.ShapeDtypeStruct((rows // 2, cols * n_col), x.dtype),
        ),
        in_specs=[pl.BlockSpec(memory_space=pltpu.VMEM)],
        out_specs=(pl.BlockSpec(memory_space=pl.ANY),) * 2,
        scratch_shapes=[
            pltpu.VMEM((rows // 2, cols * n_col), x.dtype),
            dma,
            dma((n_row, sub)),
            dma((n_row, sub)),
            dma((n_row, 2, sub)),
            dma((2, n_row, 2, hsub)),
            dma((n_row, 2, hsub)),
            dma,
        ],
        compiler_params=pltpu.CompilerParams(collective_id=0, has_side_effects=True),
        name="exchange",
    )(x)


def project_kernel(
    n_row, w_ref, g_ref, t_ref, p_ref,
    w_in, g_in, w_sum, g_sum, w_full, g_full, send_1, recv_1, send_2, recv_2,
):
    r = lax.axis_index("row")
    c = lax.axis_index("col")
    barrier = pltpu.get_barrier_semaphore()
    for d in range(1, n_row):
        pl.semaphore_signal(barrier, inc=1, device_id=(r ^ d, c), device_id_type=MESH)
    pl.semaphore_wait(barrier, n_row - 1)
    pairs = ((w_ref, w_in, w_sum, w_full), (g_ref, g_in, g_sum, g_full))

    def part(array, owner):
        size = array.shape[0] // n_row
        return pl.ds(pl.multiple_of(owner * size, size), size)

    def scatter(d, i):
        array, landing, _, _ = pairs[i]
        return pltpu.make_async_remote_copy(
            src_ref=array.at[part(array, r ^ d), :], dst_ref=landing.at[d],
            send_sem=send_1.at[d, i], recv_sem=recv_1.at[d, i],
            device_id=(r ^ d, c), device_id_type=MESH,
        )

    def spread(d, i):
        array, _, total, full = pairs[i]
        return pltpu.make_async_remote_copy(
            src_ref=total, dst_ref=full.at[part(array, r), :],
            send_sem=send_2.at[d, i], recv_sem=recv_2.at[d, i],
            device_id=(r ^ d, c), device_id_type=MESH,
        )

    every = [(d, i) for d in range(1, n_row) for i in (1, 0)]
    for d, i in every:
        scatter(d, i).start()
    for d, i in every:
        scatter(d, i).wait_recv()
    for i in (1, 0):
        array, landing, total, full = pairs[i]
        value = array[part(array, r), :]
        for d in range(1, n_row):
            value = value + landing[d]
        total[...] = value
    for i in (1, 0):
        array, _, total, full = pairs[i]
        full[part(array, r), :] = total[...]
    for d, i in every:
        spread(d, i).start()
    for d, i in every:
        spread(d, i).wait_recv()
    highest = lax.Precision.HIGHEST
    width = g_ref.shape[0]
    second = jnp.dot(
        t_ref[1], w_full[width:, :], precision=highest, preferred_element_type=jnp.float32
    ).astype(jnp.bfloat16)
    first = w_full[:width, :] - jnp.dot(
        g_full[...], second.astype(jnp.float32),
        precision=highest, preferred_element_type=jnp.float32,
    )
    first = jnp.dot(t_ref[0], first, precision=highest, preferred_element_type=jnp.float32)
    p_ref[0] = first.astype(jnp.bfloat16)
    p_ref[1] = second
    for d, i in every:
        scatter(d, i).wait_send()
        spread(d, i).wait_send()


def project(w, g, factors, n_row):
    dma = pltpu.SemaphoreType.DMA((n_row, 2))
    width, columns = g.shape[0], w.shape[1]
    vmem = pl.BlockSpec(memory_space=pltpu.VMEM)

    def landing(array):
        return pltpu.VMEM((n_row, array.shape[0] // n_row, array.shape[1]), jnp.float32)

    def total(array):
        return pltpu.VMEM((array.shape[0] // n_row, array.shape[1]), jnp.float32)

    return pl.pallas_call(
        functools.partial(project_kernel, n_row),
        out_shape=jax.ShapeDtypeStruct((2, width, columns), jnp.bfloat16),
        in_specs=[vmem] * 3,
        out_specs=vmem,
        scratch_shapes=[
            landing(w), landing(g), total(w), total(g),
            pltpu.VMEM(w.shape, jnp.float32), pltpu.VMEM(g.shape, jnp.float32),
            dma, dma, dma, dma,
        ],
        compiler_params=pltpu.CompilerParams(collective_id=1, has_side_effects=True),
        name="project",
    )(w, g, factors)


def region_kernel(index_ref, p_ref, vecs_ref, refl_ref, out_ref, vecs, refl, sems):
    count = vecs.shape[0]

    def copies(b):
        at = index_ref[b]
        return (
            pltpu.make_async_copy(vecs_ref.at[at], vecs.at[b], sems.at[b, 0]),
            pltpu.make_async_copy(refl_ref.at[0, at], refl.at[0, b], sems.at[b, 1]),
            pltpu.make_async_copy(refl_ref.at[1, at], refl.at[1, b], sems.at[b, 2]),
        )

    for b in range(count):
        for copy in copies(b):
            copy.start()
    for b in range(count):
        for copy in copies(b):
            copy.wait()
        value = vecs[b].astype(jnp.float32)
        value = value - jnp.dot(refl[1, b], p_ref[1], preferred_element_type=jnp.float32)
        value = value - jnp.dot(refl[0, b], p_ref[0], preferred_element_type=jnp.float32)
        out_ref[b] = value.astype(out_ref.dtype)


def region_rows(index, applied, vecs, refl):
    count = index.shape[0]
    columns, width = vecs.shape[2], refl.shape[3]
    vmem = pl.BlockSpec(memory_space=pltpu.VMEM)
    hbm = pl.BlockSpec(memory_space=pl.ANY)
    return pl.pallas_call(
        region_kernel,
        out_shape=jax.ShapeDtypeStruct((count, BLOCK, columns), vecs.dtype),
        in_specs=[pl.BlockSpec(memory_space=pltpu.SMEM), vmem, hbm, hbm],
        out_specs=vmem,
        scratch_shapes=[
            pltpu.VMEM((count, BLOCK, columns), vecs.dtype),
            pltpu.VMEM((2, count, BLOCK, width), refl.dtype),
            pltpu.SemaphoreType.DMA((count, 3)),
        ],
        name="region",
    )(index, applied, vecs, refl)


def per_device(n_row, eigvecs, reflectors, factors, frequencies, region_blocks):
    columns = eigvecs.shape[1]
    width = reflectors.shape[2]
    local = lax.dot_general(
        reflectors, eigvecs, (((1,), (0,)), ((), ())), preferred_element_type=jnp.float32
    ).reshape(2 * width, columns)
    cross_local = contract_rows(reflectors[0], reflectors[1])
    applied = project(local, cross_local, jnp.triu(factors), n_row)
    local_blocks = eigvecs.shape[0] // BLOCK
    local_index = region_blocks - lax.axis_index("row") * local_blocks
    region = region_rows(
        local_index,
        applied,
        eigvecs.reshape(local_blocks, BLOCK, columns),
        reflectors.reshape(2, local_blocks, BLOCK, width),
    ).reshape(-1, columns)
    weight = 1.0 / jnp.tanh(frequencies / 2.0) / (2.0 * frequencies)
    mine, partner = exchange(region, n_row)
    scaled = (mine.astype(jnp.float32) * weight[None, :]).astype(jnp.bfloat16)
    return contract_cols(scaled, partner)


BF = jnp.bfloat16
F32 = jnp.float32
HIGH = lax.Precision.HIGHEST


def dot_nt(left, right, **kw):
    return lax.dot_general(left, right, (((1,), (1,)), ((), ())), preferred_element_type=F32, **kw)


def dot_tn(left, right):
    return lax.dot_general(left, right, (((0,), (0,)), ((), ())), preferred_element_type=F32)


def spread_kernel(
    chunks, index_ref, vecs_ref, refl_ref, factor_ref, freq_ref, acc_ref, sa_ref, last_ref,
    index, vecs, refl, w_sum, g_sum, w_ref, t_ref, f_ref, small_sem, vec_sem, refl_sem, buf, tbuf, rbuf, w_in, g_in, g_full, p_full, weight,
    w_send, w_recv, g_send, g_recv, h_send, h_recv, p_send, p_recv,
    own_send, relay_send, zrel_send, zsrc_send, detz_send, deti_send, rr_send,
    ax, ay, ad, asib, zb, det, tz, rr,
):
    r = lax.axis_index("row")
    c = lax.axis_index("col")
    k = c // 2
    h = lax.rem(c, 2)
    o = 1 - h
    count = index.shape[0]
    half = count // 2
    columns = vecs.shape[2]
    width = refl.shape[3]
    blocks = vecs.shape[0] // chunks
    quarter = columns // 4
    last_row = 3

    def col(chip, core):
        return 2 * chip + core

    barrier = pltpu.get_barrier_semaphore()

    def greet(row, column):
        pl.semaphore_signal(barrier, inc=1, device_id=(row, column), device_id_type=MESH)

    for d in range(1, 4):
        greet(lax.rem(r + d, 4), c)
    for e in range(1, 8):
        greet(r, c ^ e)

    def load_vecs(i):
        part = pl.ds(i * blocks, blocks)
        return pltpu.make_async_copy(vecs_ref.at[part], vecs.at[part], vec_sem.at[i])

    def load_refl(i):
        part = pl.ds(i * blocks, blocks)
        return pltpu.make_async_copy(refl_ref.at[:, part], refl.at[:, part], refl_sem.at[i])

    def rows_of(array, i):
        return array[pl.ds(i * blocks, blocks)].reshape(blocks * BLOCK, array.shape[2])

    for i in range(chunks):
        load_refl(i).start()
    load_vecs(0).start()
    small = [
        pltpu.make_async_copy(src, dst, small_sem.at[i])
        for i, (src, dst) in enumerate(((index_ref, index), (factor_ref, t_ref), (freq_ref, f_ref)))
    ]
    for copy in small:
        copy.start()
    for i in range(chunks):
        if i + 1 < chunks:
            load_vecs(i + 1).start()
        load_refl(i).wait()
        g = dot_tn(rows_of(refl.at[0], i), rows_of(refl.at[1], i))
        if i:
            g = g + g_sum[...]
        g_sum[...] = g
    for copy in small:
        copy.wait()

    pl.semaphore_wait(barrier, 10)

    def remote(src, dst, send, recv, row, column):
        return pltpu.make_async_remote_copy(
            src_ref=src, dst_ref=dst, send_sem=send, recv_sem=recv,
            device_id=(row, column), device_id_type=MESH,
        )

    far = [jnp.where(r < 2, 3, 0), jnp.where(r < 2, 2, 1), jnp.where(r < 2, 1 - r, 5 - r)]

    def w_copy(q, part):
        d = lax.rem(q - r + 4, 4)
        rows = pl.ds(pl.multiple_of(q * quarter, quarter), quarter)
        lanes = pl.ds(part * width, width)
        return remote(
            w_ref.at[rows, lanes], w_in.at[d, :, lanes], w_send.at[d, part], w_recv.at[d, part], q, c
        )

    g_rows = width // 8
    g_part = pl.ds(pl.multiple_of(c * g_rows, g_rows), g_rows)

    def g_copy(q):
        d = lax.rem(q - r + 4, 4)
        return remote(g_sum.at[g_part], g_in.at[d], g_send.at[d], g_recv.at[d], q, c)

    for q in far:
        g_copy(q).start()
    for i in range(chunks):
        load_vecs(i).wait()
        y = jnp.concatenate([rows_of(refl.at[0], i), rows_of(refl.at[1], i)], axis=1)
        w = dot_tn(rows_of(vecs, i), y)
        if i:
            w = w + w_sum[...]
        w_sum[...] = w
    w_ref[...] = w.astype(BF)
    for part in (1, 0):
        for q in far:
            w_copy(q, part).start()
    for q in far:
        g_copy(q).wait_recv()
    value = g_sum[g_part, :]
    for d in (1, 2, 3):
        value = value + g_in[d]
    g_full[c] = value

    def h_copy(e):
        return remote(g_full.at[c], g_full.at[c], h_send.at[e], h_recv.at[e], r, c ^ e)

    def h_arrival(e):
        return remote(g_full.at[c ^ e], g_full.at[c ^ e], h_send.at[e], h_recv.at[e], r, c ^ e)

    for e in range(1, 8):
        h_copy(e).start()

    f = f_ref[...]
    weight[...] = 1.0 / jnp.tanh(f / 2.0) / (2.0 * f)
    row_at = lax.broadcasted_iota(jnp.int32, (width, width), 0)
    col_at = lax.broadcasted_iota(jnp.int32, (width, width), 1)
    upper = row_at <= col_at
    zero = jnp.zeros((width, width), F32)
    t0 = jnp.where(upper, t_ref[0], zero)
    t1 = jnp.where(upper, t_ref[1], zero)

    mine = pl.ds(pl.multiple_of(r * quarter, quarter), quarter)

    def w_total(part):
        lanes = pl.ds(part * width, width)
        for q in far:
            w_copy(q, part).wait_recv()
        w = w_sum[mine, lanes]
        for d in (1, 2, 3):
            w = w + w_in[d, :, lanes].astype(F32)
        return w

    def p_copy(q, part):
        d = lax.rem(q - r + 4, 4)
        at = p_full.at[r, :, pl.ds(part * width, width)]
        return remote(at, at, p_send.at[d, part], p_recv.at[d, part], q, c)

    def p_arrival(q, part):
        d = lax.rem(r - q + 4, 4)
        at = p_full.at[q, :, pl.ds(part * width, width)]
        return remote(at, at, p_send.at[d, part], p_recv.at[d, part], q, c)

    second = dot_nt(w_total(1), t1, precision=HIGH).astype(BF)
    p_full[r, :, width:] = second
    for q in far:
        p_copy(q, 1).start()
    first = w_total(0)
    for e in range(1, 8):
        h_arrival(e).wait_recv()
    g = g_full[...].reshape(width, width)
    first = first - dot_nt(second.astype(F32), g, precision=HIGH)
    p_full[r, :, :width] = dot_nt(first, t0, precision=HIGH).astype(BF)
    for q in far:
        p_copy(q, 0).start()
    for part in (1, 0):
        for q in far:
            p_arrival(q, part).wait_recv()

    def block_of(n):
        return lax.rem(n, 2) * half + n // 2

    def a_copy(way, n):
        b = block_of(n)
        src = buf.at[c, b]
        if way == 2:
            return remote(src, buf.at[c, b], own_send.at[2], asib.at[0, n], r, col(k, o))
        sem = ax if way == 0 else ay
        return remote(src, buf.at[c, b], own_send.at[way], sem.at[n], r, col(k ^ (way + 1), h))

    corner = (k == 0) | (k == 3)
    is_low = k == 0
    rank = jnp.where(is_low, r, 3 - r)
    away = jnp.where(is_low, -1, 1)
    slot = jnp.where(is_low, 0, 1)
    early = 4

    def det_own(hops, n):
        b = block_of(n)
        return remote(
            buf.at[c, b], tbuf.at[rank - 1, b], detz_send.at[hops - 1], tz.at[rank - 1, n],
            r + away * hops, c,
        )

    down = r < k
    at_source = r == k
    step = jnp.where(down, -1, 1)
    depth = jnp.where(down, k, 3 - k)

    def z_piece(t, depth, is_down):
        third = t // (2 * half)
        n = jnp.where(third == 0, lax.rem(t, half), lax.rem(t, 2 * half) // 2)
        e = jnp.where(third == 0, t // half, lax.rem(t, 2))
        j1 = jnp.where(depth == 3, 2, 3)
        j2 = 6 - depth - j1
        j = jnp.where(third == 0, depth, jnp.where(third == 1, j1, j2))
        j = jnp.where(is_down, j, 3 - j)
        return col(j, lax.rem(h + e, 2)), n

    steps = 3 * 2 * half

    def z_relay(t):
        src, n = z_piece(t, depth, down)
        at = buf.at[src, count + n]
        return remote(at, at, zrel_send, zb.at[t], r + step, c)

    def z_source(t, is_down):
        src, n = z_piece(t, k if is_down else 3 - k, jnp.bool_(is_down))
        return remote(
            buf.at[src, h * half + n], buf.at[src, count + n],
            zsrc_send.at[0 if is_down else 1], zb.at[t], r + (-1 if is_down else 1), c,
        )

    def z_source_step(t):
        @pl.when(at_source)
        def _():
            @pl.when(r > 0)
            def _():
                z_source(t, True).start()

            @pl.when(r < last_row)
            def _():
                z_source(t, False).start()

    applied = p_full[...].reshape(columns, 2 * width)

    base = r * vecs.shape[0]

    def make_region(n, _):
        b = block_of(n)
        at = jnp.clip(index[b] - base, 0, vecs.shape[0] - 1)
        y = jnp.concatenate([refl[0, at], refl[1, at]], axis=1)
        buf[c, b] = (vecs[at].astype(F32) - dot_nt(y, applied)).astype(BF)
        for way in (0, 1, 2):
            a_copy(way, n).start()

        @pl.when(corner & ((rank > 1) | ((rank == 1) & (n < early))))
        def _():
            @pl.when(rank == 3)
            def _():
                det_own(2, n).start()

            det_own(1, n).start()

        @pl.when(lax.rem(n, 2) == h)
        def _():
            z_source_step(n // 2)

        return 0

    lax.fori_loop(0, count, make_region, 0)

    def a_arrival(way, n):
        src = col(k ^ (way + 1), h)
        b = block_of(n)
        at = buf.at[src, b]
        sem = (ax, ay, ad)[way]
        return remote(at, at, own_send.at[2], sem.at[n], r, col(k, o))

    def sib_copy(j, n):
        src = col(k ^ j, h)
        b = block_of(n)
        at = buf.at[src, b]
        return remote(at, at, own_send.at[2], asib.at[j, n], r, col(k, o))

    def sib_arrival(j, n):
        src = col(k ^ j, o)
        b = block_of(n)
        at = buf.at[src, b]
        return remote(at, at, own_send.at[2], asib.at[j, n], r, col(k, o))

    def relay(way, n):
        src = col(k ^ (way + 1), h)
        at = buf.at[src, block_of(n)]
        to = k ^ (2 - way)
        return remote(at, at, relay_send.at[way], ad.at[n], r, col(to, h))

    def det_z(p, n):
        at = tbuf.at[p - 1, block_of(n)]
        return remote(at, at, detz_send.at[p], tz.at[p - 1, n], r + away, c)

    def det_plane(p, n):
        b = block_of(n)
        src = tbuf.at[p - 1, b]
        core = lax.rem(n, 2)
        if p < 3:
            return remote(
                src, buf.at[c, count + n // 2], deti_send.at[p], det.at[h, n // 2],
                r, col(k ^ p, core),
            )
        return remote(
            src, rbuf.at[slot, n // 2], deti_send.at[p], rr.at[slot, n // 2],
            r, col(k ^ (1 + h), core),
        )

    between = (k == 1) | (k == 2)

    def rr_copy(way, n):
        low = k - 1 if way == 0 else 2 - k
        src = low if way == 0 else low + 6
        return remote(
            rbuf.at[way, n], buf.at[src, count + n], rr_send.at[way], det.at[low, n],
            r, col(3 if way == 0 else 0, h),
        )

    def det_arrival(low, n):
        src = jnp.where(down, low, low + 6)
        at = buf.at[src, count + n]
        return remote(at, at, own_send.at[2], det.at[low, n], r, col(k, o))

    mine_at = jnp.where(at_source, h * half, count)

    from_low = jnp.logical_not(down | (at_source & (k >= 2)))
    deep = jnp.where(from_low, 3 - k, k)
    mid = jnp.where(deep == 3, 2, 3)
    order = []
    for j in (deep, mid, 6 - deep - mid, 0):
        j = jnp.where(from_low, 3 - j, j)
        order += [col(j, 0), col(j, 1)]

    def at_place(s):
        src = order[0]
        for i in range(1, 8):
            src = jnp.where(s == i, order[i], src)
        return src

    def scale(s, part):
        src = at_place(s)
        wt = jnp.concatenate([weight[pl.ds(2 * src, 1), :], weight[pl.ds(2 * src + 1, 1), :]], axis=1)

        def one(i, _):
            b = part * half + i
            rows = pl.ds(pl.multiple_of(b * BLOCK, BLOCK), BLOCK)
            sa_ref[s, rows, :] = (buf[src, b].astype(F32) * wt).astype(BF)
            return 0

        lax.fori_loop(0, half, one, 0)

    tile = 2 * BLOCK
    row_tile = acc_ref.shape[0] // 3

    def product(block, lane, size, third, places, add):
        at = mine_at + block
        lanes = pl.ds(pl.multiple_of(lane, BLOCK), size * BLOCK)
        rows = pl.ds(pl.multiple_of(third * row_tile, row_tile), row_tile)
        total = jnp.zeros((row_tile, size * BLOCK), F32)
        for s in places:
            right = buf[order[s], pl.ds(at, size)].reshape(size * BLOCK, columns)
            total = total + dot_nt(sa_ref[s, rows, :], right)
        if add:
            total = total + acc_ref[rows, lanes]
        acc_ref[rows, lanes] = total

    def pair(q, third, places, add):
        product(2 * q, q * tile, 2, third, places, add)

    def wait_detours(n):
        @pl.when(jnp.logical_not(at_source))
        def _():
            for low in (0, 1):
                det_arrival(low, n).wait_recv()

    hops = jnp.where(down, k - r, r - k)
    lag = 2

    def z_relay_step(u):
        t = u - lag * hops

        @pl.when(jnp.logical_not(at_source) & (t >= 0) & (t < steps))
        def _():
            z_relay(t).wait_recv()

            @pl.when((down & (r > 0)) | (jnp.logical_not(down) & (r < last_row)))
            def _():
                z_relay(t).start()

    def first_third(n, _):
        sib_arrival(0, 2 * n).wait_recv()
        sib_arrival(0, 2 * n + 1).wait_recv()
        z_source_step(half + n)
        return 0

    lax.fori_loop(0, half, first_third, 0)


    def beat(u, _):
        def span(first, length):
            return (u >= first) & (u < first + length)

        z_relay_step(u)

        @pl.when(span(2, count))
        def _():
            n = u - 2
            for way in (0, 1):
                a_arrival(way, n).wait_recv()
                sib_copy(way + 1, n).start()
            even = lax.rem(n, 2) == 0

            @pl.when(even)
            def _():
                relay(0, n).start()

            @pl.when(jnp.logical_not(even))
            def _():
                relay(1, n).start()

        @pl.when(span(4, count))
        def _():
            n = u - 4
            sib_arrival(1, n).wait_recv()
            sib_arrival(2, n).wait_recv()

        @pl.when(span(6, count))
        def _():
            z_source_step(u + count - 6)

        @pl.when(corner)
        def _():
            n5 = (u - 3) // 2

            @pl.when((rank == 1) & span(3, 2 * count) & (lax.rem(u - 3, 2) == 0))
            def _():
                for p in (3, 2):
                    det_z(p, n5).wait_recv()
                    det_z(p, n5).start()

            @pl.when((rank == 1) & span(36, count - early))
            def _():
                det_own(1, u - 36 + early).start()

            v = u - 22
            n3 = (4 * v + 4) // 5

            @pl.when((rank < 3) & span(22, 22) & (lax.rem(v, 5) != 4))
            def _():
                @pl.when(rank != 1)
                def _():
                    det_z(3, n3).wait_recv()

                det_plane(3, n3).start()

            v2 = u - 28
            n2 = (2 * v2) // 3

            @pl.when((rank < 2) & span(28, 27) & (lax.rem(v2, 3) != 1))
            def _():
                @pl.when(rank != 1)
                def _():
                    det_z(2, n2).wait_recv()

                det_plane(2, n2).start()

            @pl.when((rank == 0) & (span(22, early) | span(39 + early, count - early)))
            def _():
                n = jnp.where(u < 40, u - 22, u - 39)
                det_z(1, n).wait_recv()
                det_plane(1, n).start()

        w = u - 26 - 2 * h
        @pl.when(between & (w >= 0) & (w < 3 * half) & (lax.rem(w, 3) == 0))
        def _():
            n = w // 3
            for way in (0, 1):
                @pl.when(r < last_row if way == 0 else r > 0)
                def _():
                    at = rbuf.at[way, n]
                    remote(at, at, rr_send.at[way], rr.at[way, n], r, col(k, o)).wait_recv()
                    rr_copy(way, n).start()

        @pl.when(span(23, half))
        def _():
            for i in range(2):
                n = 2 * (u - 23) + i
                a_arrival(2, n).wait_recv()
                sib_copy(3, n).start()

        @pl.when(span(25, half))
        def _():
            for i in range(2):
                sib_arrival(3, 2 * (u - 25) + i).wait_recv()

        @pl.when(span(27, count))
        def _():
            z_source_step(u + 2 * count - 27)

        for first, length, place in ((6, 4, 0), (22, 4, 2), (34, 8, 4)):
            @pl.when(span(first, length))
            def _():
                scale(place + (u - first) // 2, lax.rem(u - first, 2))

        for first, q in ((27, 0), (31, 1), (42, 2)):
            @pl.when(span(first, 3))
            def _():
                pair(q, u - first, range(4), False)

        q = (u - 46) // 4
        i = lax.rem(u - 46, 4)

        @pl.when((u == 45) | (u == 49) | (u == 53))
        def _():
            pair(3, (u - 45) // 4, range(4), False)

        @pl.when(span(46, 12) & (i == 0))
        def _():
            wait_detours(2 * q)
            wait_detours(2 * q + 1)

        @pl.when(span(46, 12) & (i < 3))
        def _():
            pair(q, i, range(4, 8), True)

        @pl.when(span(57, 3))
        def _():
            product(8, 4 * tile, 1, u - 57, range(4), False)

        return 0

    lax.fori_loop(0, steps + 3 * lag, beat, 0)
    wait_detours(6)
    wait_detours(7)
    wait_detours(8)
    for s in range(4):
        last_ref[s] = buf[order[4 + s], pl.ds(mine_at + 6, 3)]

    def drain(ref, sem):
        pltpu.make_async_copy(ref, ref, sem).wait()

    for q in far:
        g_copy(q).wait_send()
        for part in (0, 1):
            w_copy(q, part).wait_send()
            p_copy(q, part).wait_send()
    for e in range(1, 8):
        h_copy(e).wait_send()
    shard = buf.at[0, pl.ds(0, count)]
    for way in (0, 1):
        drain(shard, own_send.at[way])
        drain(buf.at[0, pl.ds(0, half)], relay_send.at[way])
    drain(buf.at[:, pl.ds(0, half)], own_send.at[2])

    @pl.when(at_source)
    def _():
        @pl.when(r > 0)
        def _():
            drain(buf.at[pl.ds(0, 2)], zsrc_send.at[0])

        @pl.when(r < last_row)
        def _():
            drain(buf.at[pl.ds(0, 2)], zsrc_send.at[1])

    @pl.when((down & (r > 0)) | ((r > k) & (r < last_row)))
    def _():
        drain(buf.at[pl.ds(0, 2)], zrel_send)

    @pl.when(corner)
    def _():
        for p in (3, 2, 1):
            @pl.when(p > rank)
            def _():
                drain(shard, deti_send.at[p])

        @pl.when(rank == 1)
        def _():
            for p in (3, 2):
                drain(shard, detz_send.at[p])

        @pl.when(rank > 0)
        def _():
            drain(shard, detz_send.at[0])

        @pl.when(rank == 3)
        def _():
            drain(shard, detz_send.at[1])

    @pl.when(between)
    def _():
        for way in (0, 1):
            @pl.when(r < last_row if way == 0 else r > 0)
            def _():
                drain(rbuf.at[0], rr_send.at[way])


def spread(index, vecs, refl, factors, frequencies):
    count = index.shape[0]
    columns, width = vecs.shape[2], refl.shape[3]
    chunks = 5
    half = count // 2
    dma = pltpu.SemaphoreType.DMA
    vmem = pl.BlockSpec(memory_space=pltpu.VMEM)
    hbm = pl.BlockSpec(memory_space=pltpu.HBM)
    return pl.pallas_call(
        functools.partial(spread_kernel, chunks),
        out_shape=(
            pltpu.VMEM((count * BLOCK, half * BLOCK), F32),
            pltpu.VMEM((8, count * BLOCK, columns), BF),
            pltpu.VMEM((4, 3, BLOCK, columns), BF),
        ),
        in_specs=[hbm] * 5,
        out_specs=(vmem,) * 3,
        scratch_shapes=[
            pltpu.SMEM((count,), jnp.int32),
            pltpu.VMEM(vecs.shape, BF),
            pltpu.VMEM(refl.shape, BF),
            pltpu.VMEM((columns, 2 * width), F32),
            pltpu.VMEM((width, width), F32),
            pltpu.VMEM((columns, 2 * width), BF),
            pltpu.VMEM(factors.shape, F32),
            pltpu.VMEM(frequencies.shape, F32),
            dma((3,)), dma((chunks,)), dma((chunks,)),
            pltpu.VMEM((8, count + half, BLOCK, columns), BF),
            pltpu.VMEM((3, count, BLOCK, columns), BF),
            pltpu.VMEM((2, half, BLOCK, columns), BF),
            pltpu.VMEM((4, columns // 4, 2 * width), BF),
            pltpu.VMEM((4, width // 8, width), F32),
            pltpu.VMEM((8, width // 8, width), F32),
            pltpu.VMEM((4, columns // 4, 2 * width), BF),
            pltpu.VMEM(frequencies.shape, F32),
            dma((4, 2)), dma((4, 2)), dma((4,)), dma((4,)), dma((8,)), dma((8,)), dma((4, 2)), dma((4, 2)),
            dma((3,)), dma((2,)), dma, dma((2,)), dma((4,)), dma((4,)), dma((2,)),
            dma((count,)), dma((count,)), dma((count,)), dma((4, count)),
            dma((3 * count,)), dma((2, half)), dma((3, count)), dma((2, half)),
        ],
        compiler_params=pltpu.CompilerParams(
            collective_id=2, has_side_effects=True, vmem_limit_bytes=36 << 20
        ),
        name="spread",
    )(index, vecs, refl, factors, frequencies)


def finish_kernel(acc_ref, sa_ref, last_ref, out_ref, tail, sem, pair_sem, single_sem):
    rows, columns = acc_ref.shape
    held, blocks, lane, depth = last_ref.shape
    parts = 4
    size = rows // parts
    done = columns - blocks * lane

    def at(i):
        return pl.ds(i * size, size)

    def main_copy(i):
        lanes = pl.ds(0, done)
        return pltpu.make_async_copy(acc_ref.at[at(i), lanes], out_ref.at[at(i), lanes], sem.at[i])

    def pair_copy(i):
        return pltpu.make_async_copy(
            tail.at[at(i), pl.ds(0, 2 * lane)], out_ref.at[at(i), pl.ds(done, 2 * lane)], pair_sem.at[i]
        )

    def single_copy(i):
        return pltpu.make_async_copy(
            tail.at[at(i), pl.ds(2 * lane, lane)],
            out_ref.at[at(i), pl.ds(columns - lane, lane)], single_sem.at[i],
        )

    for i in range(parts):
        main_copy(i).start()
    for first, count, copy in ((0, 2, pair_copy), (2, 1, single_copy)):
        lanes = pl.ds(first * lane, count * lane)
        for i in range(parts):
            total = acc_ref[at(i), pl.ds(done + first * lane, count * lane)]
            for s in range(held):
                right = last_ref[s, first:first + count].reshape(count * lane, depth)
                total = total + dot_nt(sa_ref[held + s, at(i), :], right)
            tail[at(i), lanes] = total
            copy(i).start()
    for i in range(parts):
        main_copy(i).wait()
        pair_copy(i).wait()
        single_copy(i).wait()


def finish(acc, sa, last):
    vmem = pl.BlockSpec(memory_space=pltpu.VMEM)
    dma = pltpu.SemaphoreType.DMA
    return pl.pallas_call(
        finish_kernel,
        out_shape=jax.ShapeDtypeStruct(acc.shape, F32),
        in_specs=[vmem] * 3,
        out_specs=pl.BlockSpec(memory_space=pl.ANY),
        scratch_shapes=[pltpu.VMEM((acc.shape[0], last.shape[1] * last.shape[2]), F32), dma((4,)), dma((4,)), dma((4,))],
        compiler_params=pltpu.CompilerParams(vmem_limit_bytes=8 << 20),
        name="finish",
    )(acc, sa, last)


def per_device_square(eigvecs, reflectors, factors, frequencies, region_blocks):
    local_blocks = eigvecs.shape[0] // BLOCK
    in_hbm = functools.partial(pltpu.with_memory_space_constraint, memory_space=pltpu.HBM)
    acc, sa, last = spread(
        in_hbm(region_blocks),
        in_hbm(eigvecs.reshape(local_blocks, BLOCK, eigvecs.shape[1])),
        in_hbm(reflectors.reshape(2, local_blocks, BLOCK, reflectors.shape[2])),
        in_hbm(factors),
        in_hbm(frequencies.reshape(-1, 128)),
    )
    return finish(acc, sa, last)


def solution(mesh):
    shape = mesh.shape
    if shape["row"] == 4 and shape["col"] == 8:
        body = per_device_square
    else:
        body = functools.partial(per_device, shape["row"])
    return jax.shard_map(
        body,
        mesh=mesh,
        in_specs=(P("row", "col"), P(None, "row", None), P(), P(), P("row")),
        out_specs=P("row", "col"),
        check_vma=False,
    )
```

```python
import functools

import jax
import jax.numpy as jnp
from jax import lax
from jax.experimental import pallas as pl
from jax.experimental.pallas import tpu as pltpu
from jax.sharding import PartitionSpec as P

BLOCK = 128
MESH = pl.DeviceIdType.MESH
SUB = 12


def contract_rows(left, right):
    return lax.dot_general(
        left, right, (((0,), (0,)), ((), ())), preferred_element_type=jnp.float32
    )


def contract_cols(left, right):
    return lax.dot_general(
        left, right, (((1,), (1,)), ((), ())), preferred_element_type=jnp.float32
    )


def exchange_kernel(
    n_row, sub, x_ref, a_ref, b_ref, half_buf,
    own_sem, send_plane, send_sib, recv_a, send_z, recv_b, fill_sem,
):
    r = lax.axis_index("row")
    c = lax.axis_index("col")
    k = c // 2
    h = lax.rem(c, 2)
    o = 1 - h
    sib = 2 * k + o
    rows, cols = x_ref.shape
    step = rows // sub
    hsub = sub // 2
    half = rows // 2
    has_up = (r < n_row - 1).astype(jnp.int32)
    has_dn = (r > 0).astype(jnp.int32)

    barrier = pltpu.get_barrier_semaphore()

    def greet(row, col):
        pl.semaphore_signal(barrier, inc=1, device_id=(row, col), device_id_type=MESH)

    greet(r, sib)
    for d in range(1, n_row):
        greet(r, 2 * (k ^ d) + h)

    @pl.when(r < n_row - 1)
    def _():
        greet(r + 1, c)

    @pl.when(r > 0)
    def _():
        greet(r - 1, c)

    pl.semaphore_wait(barrier, n_row + has_up + has_dn)

    def piece_cols(d, side):
        owner = 2 * (k ^ d) + (h if side == 0 else o)
        return pl.ds(pl.multiple_of(owner * cols, cols), cols)

    def a_at(d, side, s):
        return a_ref.at[pl.ds(s * step, step), piece_cols(d, side)]

    def plane_copy(d, s):
        return pltpu.make_async_remote_copy(
            src_ref=x_ref.at[pl.ds(s * step, step), :],
            dst_ref=a_ref.at[pl.ds(s * step, step), piece_cols(0, 0)],
            send_sem=send_plane.at[d, s], recv_sem=recv_a.at[d, 0, s],
            device_id=(r, 2 * (k ^ d) + h), device_id_type=MESH,
        )

    def sib_copy(d, s):
        src = x_ref.at[pl.ds(s * step, step), :] if d == 0 else a_at(d, 0, s)
        return pltpu.make_async_remote_copy(
            src_ref=src, dst_ref=a_at(d, 0, s),
            send_sem=send_sib.at[d, s], recv_sem=recv_a.at[d, 1, s],
            device_id=(r, sib), device_id_type=MESH,
        )

    def half_rows(t):
        return pl.ds(pl.multiple_of(h * half + t * step, step), step)

    def z_copy(src, way, target, d, side, t):
        return pltpu.make_async_remote_copy(
            src_ref=src,
            dst_ref=b_ref.at[pl.ds(t * step, step), piece_cols(d, side)],
            send_sem=send_z.at[way, d, side, t], recv_sem=recv_b.at[d, side, t],
            device_id=(target, c), device_id_type=MESH,
        )

    def from_source(way, target, d, side, t):
        if d == 0 and side == 0:
            src = x_ref.at[half_rows(t), :]
        else:
            src = a_ref.at[half_rows(t), piece_cols(d, side)]
        return z_copy(src, way, target, d, side, t)

    def relay(way, target, d, side, t):
        src = b_ref.at[pl.ds(t * step, step), piece_cols(d, side)]
        return z_copy(src, way, target, d, side, t)

    own = pltpu.make_async_copy(x_ref, a_ref.at[:, piece_cols(0, 0)], own_sem)
    own.start()
    for s in range(sub):
        sib_copy(0, s).start()
    for d in range(1, n_row):
        for s in range(sub):
            plane_copy(d, s).start()

    arrivals = [(d, s) for d in range(1, n_row) for s in range(sub)]
    parts = [(d, side, t) for d in range(n_row) for side in (0, 1) for t in range(hsub)]

    def take_a(d, s):
        plane_copy(d, s).wait_recv()
        sib_copy(d, s).start()

    at_source = r == k
    above = r > k
    below = r < k

    @pl.when(at_source)
    def _():
        def push(d, side, t):
            @pl.when(r < n_row - 1)
            def _():
                from_source(0, r + 1, d, side, t).start()

            @pl.when(r > 0)
            def _():
                from_source(1, r - 1, d, side, t).start()

        for d in range(n_row):
            if d:
                for s in range(sub):
                    take_a(d, s)
            else:
                for t in range(hsub):
                    push(d, 0, t)
            for s in range(sub):
                sib_copy(d, s).wait_recv()
            for side in (0, 1) if d else (1,):
                for t in range(hsub):
                    push(d, side, t)
        own.wait()
        fill = pltpu.make_async_copy(
            a_ref.at[pl.ds(pl.multiple_of(h * half, half), half), :], half_buf, fill_sem
        )
        fill.start()
        fill.wait()
        out = pltpu.make_async_copy(half_buf, b_ref, fill_sem)
        out.start()
        out.wait()

    @pl.when(jnp.logical_not(at_source))
    def _():
        for i, (d, side, t) in enumerate(parts):
            if i < len(arrivals):
                take_a(*arrivals[i])
            relay(0, r, d, side, t).wait_recv()

            @pl.when(above & (r < n_row - 1))
            def _():
                relay(0, r + 1, d, side, t).start()

            @pl.when(below & (r > 0))
            def _():
                relay(1, r - 1, d, side, t).start()

        for d, s in arrivals[len(parts):]:
            take_a(d, s)
        for d in range(n_row):
            for s in range(sub):
                sib_copy(d, s).wait_recv()
        own.wait()

    for d in range(n_row):
        for s in range(sub):
            sib_copy(d, s).wait_send()
            if d:
                plane_copy(d, s).wait_send()
    for d, side, t in parts:
        @pl.when((r >= k) & (r < n_row - 1))
        def _():
            relay(0, r, d, side, t).wait_send()

        @pl.when((r <= k) & (r > 0))
        def _():
            relay(1, r, d, side, t).wait_send()


def exchange(x, n_row):
    rows, cols = x.shape
    n_col = 2 * n_row
    sub = SUB if n_row <= 4 else SUB // 2
    hsub = sub // 2
    dma = pltpu.SemaphoreType.DMA
    return pl.pallas_call(
        functools.partial(exchange_kernel, n_row, sub),
        out_shape=(
            jax.ShapeDtypeStruct((rows, cols * n_col), x.dtype),
            jax.ShapeDtypeStruct((rows // 2, cols * n_col), x.dtype),
        ),
        in_specs=[pl.BlockSpec(memory_space=pltpu.VMEM)],
        out_specs=(pl.BlockSpec(memory_space=pl.ANY),) * 2,
        scratch_shapes=[
            pltpu.VMEM((rows // 2, cols * n_col), x.dtype),
            dma,
            dma((n_row, sub)),
            dma((n_row, sub)),
            dma((n_row, 2, sub)),
            dma((2, n_row, 2, hsub)),
            dma((n_row, 2, hsub)),
            dma,
        ],
        compiler_params=pltpu.CompilerParams(collective_id=0, has_side_effects=True),
        name="exchange",
    )(x)


def project_kernel(
    n_row, w_ref, g_ref, t_ref, p_ref,
    w_in, g_in, w_sum, g_sum, w_full, g_full, send_1, recv_1, send_2, recv_2,
):
    r = lax.axis_index("row")
    c = lax.axis_index("col")
    barrier = pltpu.get_barrier_semaphore()
    for d in range(1, n_row):
        pl.semaphore_signal(barrier, inc=1, device_id=(r ^ d, c), device_id_type=MESH)
    pl.semaphore_wait(barrier, n_row - 1)
    pairs = ((w_ref, w_in, w_sum, w_full), (g_ref, g_in, g_sum, g_full))

    def part(array, owner):
        size = array.shape[0] // n_row
        return pl.ds(pl.multiple_of(owner * size, size), size)

    def scatter(d, i):
        array, landing, _, _ = pairs[i]
        return pltpu.make_async_remote_copy(
            src_ref=array.at[part(array, r ^ d), :], dst_ref=landing.at[d],
            send_sem=send_1.at[d, i], recv_sem=recv_1.at[d, i],
            device_id=(r ^ d, c), device_id_type=MESH,
        )

    def spread(d, i):
        array, _, total, full = pairs[i]
        return pltpu.make_async_remote_copy(
            src_ref=total, dst_ref=full.at[part(array, r), :],
            send_sem=send_2.at[d, i], recv_sem=recv_2.at[d, i],
            device_id=(r ^ d, c), device_id_type=MESH,
        )

    every = [(d, i) for d in range(1, n_row) for i in (1, 0)]
    for d, i in every:
        scatter(d, i).start()
    for d, i in every:
        scatter(d, i).wait_recv()
    for i in (1, 0):
        array, landing, total, full = pairs[i]
        value = array[part(array, r), :]
        for d in range(1, n_row):
            value = value + landing[d]
        total[...] = value
    for i in (1, 0):
        array, _, total, full = pairs[i]
        full[part(array, r), :] = total[...]
    for d, i in every:
        spread(d, i).start()
    for d, i in every:
        spread(d, i).wait_recv()
    highest = lax.Precision.HIGHEST
    width = g_ref.shape[0]
    second = jnp.dot(
        t_ref[1], w_full[width:, :], precision=highest, preferred_element_type=jnp.float32
    ).astype(jnp.bfloat16)
    first = w_full[:width, :] - jnp.dot(
        g_full[...], second.astype(jnp.float32),
        precision=highest, preferred_element_type=jnp.float32,
    )
    first = jnp.dot(t_ref[0], first, precision=highest, preferred_element_type=jnp.float32)
    p_ref[0] = first.astype(jnp.bfloat16)
    p_ref[1] = second
    for d, i in every:
        scatter(d, i).wait_send()
        spread(d, i).wait_send()


def project(w, g, factors, n_row):
    dma = pltpu.SemaphoreType.DMA((n_row, 2))
    width, columns = g.shape[0], w.shape[1]
    vmem = pl.BlockSpec(memory_space=pltpu.VMEM)

    def landing(array):
        return pltpu.VMEM((n_row, array.shape[0] // n_row, array.shape[1]), jnp.float32)

    def total(array):
        return pltpu.VMEM((array.shape[0] // n_row, array.shape[1]), jnp.float32)

    return pl.pallas_call(
        functools.partial(project_kernel, n_row),
        out_shape=jax.ShapeDtypeStruct((2, width, columns), jnp.bfloat16),
        in_specs=[vmem] * 3,
        out_specs=vmem,
        scratch_shapes=[
            landing(w), landing(g), total(w), total(g),
            pltpu.VMEM(w.shape, jnp.float32), pltpu.VMEM(g.shape, jnp.float32),
            dma, dma, dma, dma,
        ],
        compiler_params=pltpu.CompilerParams(collective_id=1, has_side_effects=True),
        name="project",
    )(w, g, factors)


def region_kernel(index_ref, p_ref, vecs_ref, refl_ref, out_ref, vecs, refl, sems):
    count = vecs.shape[0]

    def copies(b):
        at = index_ref[b]
        return (
            pltpu.make_async_copy(vecs_ref.at[at], vecs.at[b], sems.at[b, 0]),
            pltpu.make_async_copy(refl_ref.at[0, at], refl.at[0, b], sems.at[b, 1]),
            pltpu.make_async_copy(refl_ref.at[1, at], refl.at[1, b], sems.at[b, 2]),
        )

    for b in range(count):
        for copy in copies(b):
            copy.start()
    for b in range(count):
        for copy in copies(b):
            copy.wait()
        value = vecs[b].astype(jnp.float32)
        value = value - jnp.dot(refl[1, b], p_ref[1], preferred_element_type=jnp.float32)
        value = value - jnp.dot(refl[0, b], p_ref[0], preferred_element_type=jnp.float32)
        out_ref[b] = value.astype(out_ref.dtype)


def region_rows(index, applied, vecs, refl):
    count = index.shape[0]
    columns, width = vecs.shape[2], refl.shape[3]
    vmem = pl.BlockSpec(memory_space=pltpu.VMEM)
    hbm = pl.BlockSpec(memory_space=pl.ANY)
    return pl.pallas_call(
        region_kernel,
        out_shape=jax.ShapeDtypeStruct((count, BLOCK, columns), vecs.dtype),
        in_specs=[pl.BlockSpec(memory_space=pltpu.SMEM), vmem, hbm, hbm],
        out_specs=vmem,
        scratch_shapes=[
            pltpu.VMEM((count, BLOCK, columns), vecs.dtype),
            pltpu.VMEM((2, count, BLOCK, width), refl.dtype),
            pltpu.SemaphoreType.DMA((count, 3)),
        ],
        name="region",
    )(index, applied, vecs, refl)


def per_device(n_row, eigvecs, reflectors, factors, frequencies, region_blocks):
    columns = eigvecs.shape[1]
    width = reflectors.shape[2]
    local = lax.dot_general(
        reflectors, eigvecs, (((1,), (0,)), ((), ())), preferred_element_type=jnp.float32
    ).reshape(2 * width, columns)
    cross_local = contract_rows(reflectors[0], reflectors[1])
    applied = project(local, cross_local, jnp.triu(factors), n_row)
    local_blocks = eigvecs.shape[0] // BLOCK
    local_index = region_blocks - lax.axis_index("row") * local_blocks
    region = region_rows(
        local_index,
        applied,
        eigvecs.reshape(local_blocks, BLOCK, columns),
        reflectors.reshape(2, local_blocks, BLOCK, width),
    ).reshape(-1, columns)
    weight = 1.0 / jnp.tanh(frequencies / 2.0) / (2.0 * frequencies)
    mine, partner = exchange(region, n_row)
    scaled = (mine.astype(jnp.float32) * weight[None, :]).astype(jnp.bfloat16)
    return contract_cols(scaled, partner)


BF = jnp.bfloat16
F32 = jnp.float32
HIGH = lax.Precision.HIGHEST


def dot_nt(left, right, **kw):
    return lax.dot_general(left, right, (((1,), (1,)), ((), ())), preferred_element_type=F32, **kw)


def dot_tn(left, right):
    return lax.dot_general(left, right, (((0,), (0,)), ((), ())), preferred_element_type=F32)


def spread_kernel(
    chunks, index_ref, vecs_ref, refl_ref, factor_ref, freq_ref, acc_ref, sa_ref, last_ref,
    index, vecs, refl, w_sum, g_sum, w_ref, t_ref, f_ref, small_sem, vec_sem, refl_sem, buf, tbuf, rbuf, w_in, g_in, g_full, p_full, weight,
    w_send, w_recv, g_send, g_recv, h_send, h_recv, p_send, p_recv,
    own_send, relay_send, zrel_send, zsrc_send, detz_send, deti_send, rr_send,
    ax, ay, ad, asib, zb, det, tz, rr,
):
    r = lax.axis_index("row")
    c = lax.axis_index("col")
    k = c // 2
    h = lax.rem(c, 2)
    o = 1 - h
    count = index.shape[0]
    half = count // 2
    columns = vecs.shape[2]
    width = refl.shape[3]
    blocks = vecs.shape[0] // chunks
    quarter = columns // 4
    last_row = 3

    def col(chip, core):
        return 2 * chip + core

    barrier = pltpu.get_barrier_semaphore()

    def greet(row, column):
        pl.semaphore_signal(barrier, inc=1, device_id=(row, column), device_id_type=MESH)

    for d in range(1, 4):
        greet(lax.rem(r + d, 4), c)
    for e in range(1, 8):
        greet(r, c ^ e)

    def load_vecs(i):
        part = pl.ds(i * blocks, blocks)
        return pltpu.make_async_copy(vecs_ref.at[part], vecs.at[part], vec_sem.at[i])

    def load_refl(i):
        part = pl.ds(i * blocks, blocks)
        return pltpu.make_async_copy(refl_ref.at[:, part], refl.at[:, part], refl_sem.at[i])

    def rows_of(array, i):
        return array[pl.ds(i * blocks, blocks)].reshape(blocks * BLOCK, array.shape[2])

    for i in range(chunks):
        load_refl(i).start()
    load_vecs(0).start()
    small = [
        pltpu.make_async_copy(src, dst, small_sem.at[i])
        for i, (src, dst) in enumerate(((index_ref, index), (factor_ref, t_ref), (freq_ref, f_ref)))
    ]
    for copy in small:
        copy.start()
    for i in range(chunks):
        if i + 1 < chunks:
            load_vecs(i + 1).start()
        load_refl(i).wait()
        g = dot_tn(rows_of(refl.at[0], i), rows_of(refl.at[1], i))
        if i:
            g = g + g_sum[...]
        g_sum[...] = g
    for copy in small:
        copy.wait()

    pl.semaphore_wait(barrier, 10)

    def remote(src, dst, send, recv, row, column):
        return pltpu.make_async_remote_copy(
            src_ref=src, dst_ref=dst, send_sem=send, recv_sem=recv,
            device_id=(row, column), device_id_type=MESH,
        )

    far = [jnp.where(r < 2, 3, 0), jnp.where(r < 2, 2, 1), jnp.where(r < 2, 1 - r, 5 - r)]

    def w_copy(q, part):
        d = lax.rem(q - r + 4, 4)
        rows = pl.ds(pl.multiple_of(q * quarter, quarter), quarter)
        lanes = pl.ds(part * width, width)
        return remote(
            w_ref.at[rows, lanes], w_in.at[d, :, lanes], w_send.at[d, part], w_recv.at[d, part], q, c
        )

    g_rows = width // 8
    g_part = pl.ds(pl.multiple_of(c * g_rows, g_rows), g_rows)

    def g_copy(q):
        d = lax.rem(q - r + 4, 4)
        return remote(g_sum.at[g_part], g_in.at[d], g_send.at[d], g_recv.at[d], q, c)

    for q in far:
        g_copy(q).start()
    for i in range(chunks):
        load_vecs(i).wait()
        y = jnp.concatenate([rows_of(refl.at[0], i), rows_of(refl.at[1], i)], axis=1)
        w = dot_tn(rows_of(vecs, i), y)
        if i:
            w = w + w_sum[...]
        w_sum[...] = w
    w_ref[...] = w.astype(BF)
    for part in (1, 0):
        for q in far:
            w_copy(q, part).start()
    for q in far:
        g_copy(q).wait_recv()
    value = g_sum[g_part, :]
    for d in (1, 2, 3):
        value = value + g_in[d]
    g_full[c] = value

    def h_copy(e):
        return remote(g_full.at[c], g_full.at[c], h_send.at[e], h_recv.at[e], r, c ^ e)

    def h_arrival(e):
        return remote(g_full.at[c ^ e], g_full.at[c ^ e], h_send.at[e], h_recv.at[e], r, c ^ e)

    for e in range(1, 8):
        h_copy(e).start()

    f = f_ref[...]
    weight[...] = 1.0 / jnp.tanh(f / 2.0) / (2.0 * f)
    row_at = lax.broadcasted_iota(jnp.int32, (width, width), 0)
    col_at = lax.broadcasted_iota(jnp.int32, (width, width), 1)
    upper = row_at <= col_at
    zero = jnp.zeros((width, width), F32)
    t0 = jnp.where(upper, t_ref[0], zero)
    t1 = jnp.where(upper, t_ref[1], zero)

    mine = pl.ds(pl.multiple_of(r * quarter, quarter), quarter)

    def w_total(part):
        lanes = pl.ds(part * width, width)
        for q in far:
            w_copy(q, part).wait_recv()
        w = w_sum[mine, lanes]
        for d in (1, 2, 3):
            w = w + w_in[d, :, lanes].astype(F32)
        return w

    def p_copy(q, part):
        d = lax.rem(q - r + 4, 4)
        at = p_full.at[r, :, pl.ds(part * width, width)]
        return remote(at, at, p_send.at[d, part], p_recv.at[d, part], q, c)

    def p_arrival(q, part):
        d = lax.rem(r - q + 4, 4)
        at = p_full.at[q, :, pl.ds(part * width, width)]
        return remote(at, at, p_send.at[d, part], p_recv.at[d, part], q, c)

    second = dot_nt(w_total(1), t1, precision=HIGH).astype(BF)
    p_full[r, :, width:] = second
    for q in far:
        p_copy(q, 1).start()
    first = w_total(0)
    for e in range(1, 8):
        h_arrival(e).wait_recv()
    g = g_full[...].reshape(width, width)
    first = first - dot_nt(second.astype(F32), g, precision=HIGH)
    p_full[r, :, :width] = dot_nt(first, t0, precision=HIGH).astype(BF)
    for q in far:
        p_copy(q, 0).start()
    for part in (1, 0):
        for q in far:
            p_arrival(q, part).wait_recv()

    def block_of(n):
        return lax.rem(n, 2) * half + n // 2

    def a_copy(way, n):
        b = block_of(n)
        src = buf.at[c, b]
        if way == 2:
            return remote(src, buf.at[c, b], own_send.at[2], asib.at[0, n], r, col(k, o))
        sem = ax if way == 0 else ay
        return remote(src, buf.at[c, b], own_send.at[way], sem.at[n], r, col(k ^ (way + 1), h))

    corner = (k == 0) | (k == 3)
    is_low = k == 0
    rank = jnp.where(is_low, r, 3 - r)
    away = jnp.where(is_low, -1, 1)
    slot = jnp.where(is_low, 0, 1)
    early = 4

    extra = 2
    near = count - extra

    def det_more(hops, i):
        b = half - 1 + i * half
        return remote(
            buf.at[col(k ^ 1, h), b], tbuf.at[rank - 1, count + i], detz_send.at[hops - 1],
            tz.at[rank - 1, count + i], r + away * hops, c,
        )

    def slot_of(n):
        return jnp.where(n < count, block_of(n), n)

    def det_own(hops, n):
        b = block_of(n)
        return remote(
            buf.at[c, b], tbuf.at[rank - 1, b], detz_send.at[hops - 1], tz.at[rank - 1, n],
            r + away * hops, c,
        )

    down = r < k
    at_source = r == k
    step = jnp.where(down, -1, 1)
    depth = jnp.where(down, k, 3 - k)

    def z_piece(t, depth, is_down):
        third = t // (2 * half)
        n = jnp.where(third == 0, lax.rem(t, half), lax.rem(t, 2 * half) // 2)
        e = jnp.where(third == 0, t // half, lax.rem(t, 2))
        j1 = jnp.where(depth == 3, 2, 3)
        j2 = 6 - depth - j1
        j = jnp.where(third == 0, depth, jnp.where(third == 1, j1, j2))
        j = jnp.where(is_down, j, 3 - j)
        return col(j, lax.rem(h + e, 2)), n

    steps = 3 * 2 * half

    def z_relay(t):
        src, n = z_piece(t, depth, down)
        at = buf.at[src, count + n]
        return remote(at, at, zrel_send, zb.at[t], r + step, c)

    def z_source(t, is_down):
        src, n = z_piece(t, k if is_down else 3 - k, jnp.bool_(is_down))
        return remote(
            buf.at[src, h * half + n], buf.at[src, count + n],
            zsrc_send.at[0 if is_down else 1], zb.at[t], r + (-1 if is_down else 1), c,
        )

    def z_source_step(t):
        @pl.when(at_source)
        def _():
            @pl.when((r > 0) & ((k < 3) | (t < steps - extra)))
            def _():
                z_source(t, True).start()

            @pl.when((r < last_row) & ((k > 0) | (t < steps - extra)))
            def _():
                z_source(t, False).start()

    applied = p_full[...].reshape(columns, 2 * width)

    base = r * vecs.shape[0]

    def make_region(n, _):
        b = block_of(n)
        at = jnp.clip(index[b] - base, 0, vecs.shape[0] - 1)
        y = jnp.concatenate([refl[0, at], refl[1, at]], axis=1)
        buf[c, b] = (vecs[at].astype(F32) - dot_nt(y, applied)).astype(BF)
        for way in (0, 1, 2):
            a_copy(way, n).start()

        @pl.when(corner & ((rank > 1) | ((rank == 1) & (n < early))))
        def _():
            @pl.when(rank == 3)
            def _():
                det_own(2, n).start()

            det_own(1, n).start()

        @pl.when(lax.rem(n, 2) == h)
        def _():
            z_source_step(n // 2)

        return 0

    lax.fori_loop(0, count, make_region, 0)

    def a_arrival(way, n):
        src = col(k ^ (way + 1), h)
        b = block_of(n)
        at = buf.at[src, b]
        sem = (ax, ay, ad)[way]
        return remote(at, at, own_send.at[2], sem.at[n], r, col(k, o))

    def sib_copy(j, n):
        src = col(k ^ j, h)
        b = block_of(n)
        at = buf.at[src, b]
        return remote(at, at, own_send.at[2], asib.at[j, n], r, col(k, o))

    def sib_arrival(j, n):
        src = col(k ^ j, o)
        b = block_of(n)
        at = buf.at[src, b]
        return remote(at, at, own_send.at[2], asib.at[j, n], r, col(k, o))

    def relay(way, n):
        src = col(k ^ (way + 1), h)
        at = buf.at[src, block_of(n)]
        to = k ^ (2 - way)
        return remote(at, at, relay_send.at[way], ad.at[n], r, col(to, h))

    def det_z(p, n):
        at = tbuf.at[p - 1, slot_of(n)]
        return remote(at, at, detz_send.at[p], tz.at[p - 1, n], r + away, c)

    def det_plane(p, n):
        src = tbuf.at[p - 1, slot_of(n)]
        core = lax.rem(n, 2)
        if p < 3:
            return remote(
                src, buf.at[c, count + n // 2], deti_send.at[p], det.at[h, n // 2],
                r, col(k ^ p, core),
            )
        return remote(
            src, rbuf.at[slot, n // 2], deti_send.at[p], rr.at[slot, n // 2],
            r, col(k ^ (1 + h), core),
        )

    between = (k == 1) | (k == 2)

    def rr_copy(way, n):
        low = k - 1 if way == 0 else 2 - k
        more = (n == half).astype(jnp.int32)
        src = low + 2 * more if way == 0 else low + 6 - 2 * more
        return remote(
            rbuf.at[way, n], buf.at[src, count + n - more], rr_send.at[way], det.at[low, n],
            r, col(3 if way == 0 else 0, h),
        )

    def det_arrival(low, n, more=0):
        src = jnp.where(down, low + 2 * more, low + 6 - 2 * more)
        at = buf.at[src, count + n - more]
        return remote(at, at, own_send.at[2], det.at[low, n], r, col(k, o))

    mine_at = jnp.where(at_source, h * half, count)

    from_low = jnp.logical_not(down | (at_source & (k >= 2)))
    deep = jnp.where(from_low, 3 - k, k)
    mid = jnp.where(deep == 3, 2, 3)
    order = []
    for j in (deep, mid, 6 - deep - mid, 0):
        j = jnp.where(from_low, 3 - j, j)
        order += [col(j, 0), col(j, 1)]

    def at_place(s):
        src = order[0]
        for i in range(1, 8):
            src = jnp.where(s == i, order[i], src)
        return src

    def scale(s, part):
        src = at_place(s)
        wt = jnp.concatenate([weight[pl.ds(2 * src, 1), :], weight[pl.ds(2 * src + 1, 1), :]], axis=1)

        def one(i, _):
            b = part * half + i
            rows = pl.ds(pl.multiple_of(b * BLOCK, BLOCK), BLOCK)
            sa_ref[s, rows, :] = (buf[src, b].astype(F32) * wt).astype(BF)
            return 0

        lax.fori_loop(0, half, one, 0)

    tile = 2 * BLOCK
    row_tile = acc_ref.shape[0] // 3

    def product(block, lane, size, third, places, add):
        at = mine_at + block
        lanes = pl.ds(pl.multiple_of(lane, BLOCK), size * BLOCK)
        rows = pl.ds(pl.multiple_of(third * row_tile, row_tile), row_tile)
        total = jnp.zeros((row_tile, size * BLOCK), F32)
        for s in places:
            right = buf[order[s], pl.ds(at, size)].reshape(size * BLOCK, columns)
            total = total + dot_nt(sa_ref[s, rows, :], right)
        if add:
            total = total + acc_ref[rows, lanes]
        acc_ref[rows, lanes] = total

    def pair(q, third, places, add):
        product(2 * q, q * tile, 2, third, places, add)

    def straight(e):
        core = lax.rem(h + e, 2)
        src = col(k ^ 1, core)
        return remote(
            buf.at[src, h * half + half - 1], buf.at[src, count + half - 1], detz_send.at[e],
            det.at[core, half - 1], r + jnp.where(k == 1, -1, 1), c,
        )

    def wait_more():
        @pl.when(jnp.logical_not(at_source) & (depth == 3))
        def _():
            for low in (0, 1):
                det_arrival(low, half, 1).wait_recv()

    def wait_detours(n):
        @pl.when(jnp.logical_not(at_source))
        def _():
            for low in (0, 1):
                det_arrival(low, n).wait_recv()

    hops = jnp.where(down, k - r, r - k)
    lag = 2

    def z_relay_step(u):
        t = u - lag * hops

        @pl.when(jnp.logical_not(at_source) & (t >= 0) & (t < jnp.where(depth == 3, steps - extra, steps)))
        def _():
            z_relay(t).wait_recv()

            @pl.when((down & (r > 0)) | (jnp.logical_not(down) & (r < last_row)))
            def _():
                z_relay(t).start()

    def first_third(n, _):
        sib_arrival(0, 2 * n).wait_recv()
        sib_arrival(0, 2 * n + 1).wait_recv()
        z_source_step(half + n)
        return 0

    lax.fori_loop(0, half, first_third, 0)


    def beat(u, _):
        def span(first, length):
            return (u >= first) & (u < first + length)

        z_relay_step(u)

        @pl.when(span(2, count))
        def _():
            n = u - 2
            for way in (0, 1):
                a_arrival(way, n).wait_recv()
                sib_copy(way + 1, n).start()
            even = lax.rem(n, 2) == 0

            @pl.when(even)
            def _():
                relay(0, n).start()

            @pl.when(jnp.logical_not(even))
            def _():
                relay(1, n).start()

        @pl.when(span(4, count))
        def _():
            n = u - 4
            sib_arrival(1, n).wait_recv()
            sib_arrival(2, n).wait_recv()

        @pl.when(span(6, count))
        def _():
            z_source_step(u + count - 6)

        @pl.when(corner)
        def _():
            n5 = (u - 3) // 2

            @pl.when((rank == 1) & span(3, 2 * (count + extra)) & (lax.rem(u - 3, 2) == 0))
            def _():
                det_z(3, n5).wait_recv()
                det_z(3, n5).start()

                @pl.when(n5 < count)
                def _():
                    det_z(2, n5).wait_recv()
                    det_z(2, n5).start()

            @pl.when((rank == 3) & span(20, extra))
            def _():
                det_more(2, u - 20).start()
                det_more(1, u - 20).start()

            @pl.when((rank == 1) & span(36, near - early))
            def _():
                det_own(1, u - 36 + early).start()

            v = u - 22
            n3 = (4 * v + 4) // 5

            @pl.when((rank < 3) & span(22, 24) & (lax.rem(v, 5) != 4))
            def _():
                @pl.when(rank != 1)
                def _():
                    det_z(3, n3).wait_recv()

                det_plane(3, n3).start()

            v2 = u - 28
            n2 = (2 * v2) // 3

            @pl.when((rank < 2) & span(28, 27) & (lax.rem(v2, 3) != 1))
            def _():
                @pl.when(rank != 1)
                def _():
                    det_z(2, n2).wait_recv()

                det_plane(2, n2).start()

            @pl.when((rank == 0) & (span(22, early) | span(39 + early, near - early)))
            def _():
                n = jnp.where(u < 40, u - 22, u - 39)
                det_z(1, n).wait_recv()
                det_plane(1, n).start()

        w = u - 30
        item = (4 * w + 4) // 5

        @pl.when(between & span(30, 24) & (lax.rem(w, 5) != 4) & (lax.rem(item, 2) == h))
        def _():
            n = item // 2
            for way in (0, 1):
                @pl.when(r < last_row if way == 0 else r > 0)
                def _():
                    at = rbuf.at[way, n]
                    remote(at, at, rr_send.at[way], rr.at[way, n], r, col(k, o)).wait_recv()
                    rr_copy(way, n).start()

        @pl.when(span(23, half))
        def _():
            for i in range(2):
                n = 2 * (u - 23) + i
                a_arrival(2, n).wait_recv()
                sib_copy(3, n).start()

        @pl.when(span(25, half))
        def _():
            for i in range(2):
                sib_arrival(3, 2 * (u - 25) + i).wait_recv()

        @pl.when(span(27, count))
        def _():
            z_source_step(u + 2 * count - 27)

        @pl.when(at_source & (u == 36) & ((k == 1) | (k == 2)))
        def _():
            for e in (0, 1):
                straight(e).start()

        for first, length, place in ((6, 4, 0), (22, 4, 2), (34, 8, 4)):
            @pl.when(span(first, length))
            def _():
                scale(place + (u - first) // 2, lax.rem(u - first, 2))

        for first, q in ((27, 0), (31, 1), (42, 2)):
            @pl.when(span(first, 3))
            def _():
                pair(q, u - first, range(4), False)

        q = (u - 46) // 4
        i = lax.rem(u - 46, 4)

        @pl.when((u == 45) | (u == 49) | (u == 53))
        def _():
            pair(3, (u - 45) // 4, range(4), False)

        @pl.when(span(46, 12) & (i == 0))
        def _():
            wait_detours(2 * q)
            wait_detours(2 * q + 1)

        @pl.when(span(46, 12) & (i < 3))
        def _():
            pair(q, i, range(4, 8), True)

        @pl.when((u == 47) | (u == 51) | (u == 55))
        def _():
            product(8, 4 * tile, 1, (u - 47) // 4, range(4), False)

        return 0

    lax.fori_loop(0, steps + 2 * lag, beat, 0)
    wait_detours(6)
    wait_detours(7)
    wait_detours(8)
    wait_more()
    for s in range(4):
        last_ref[s] = buf[order[4 + s], pl.ds(mine_at + 6, 3)]

    def drain(ref, sem):
        pltpu.make_async_copy(ref, ref, sem).wait()

    for q in far:
        g_copy(q).wait_send()
        for part in (0, 1):
            w_copy(q, part).wait_send()
            p_copy(q, part).wait_send()
    for e in range(1, 8):
        h_copy(e).wait_send()
    shard = buf.at[0, pl.ds(0, count)]
    for way in (0, 1):
        drain(shard, own_send.at[way])
        drain(buf.at[0, pl.ds(0, half)], relay_send.at[way])
    drain(buf.at[:, pl.ds(0, half)], own_send.at[2])

    whole = buf.at[pl.ds(0, 2)]
    short = buf.at[pl.ds(0, 2), pl.ds(0, count + half - extra // 2)]
    longer = buf.at[0, pl.ds(0, count + extra)]
    brief = buf.at[0, pl.ds(0, near)]

    @pl.when(at_source & ((k == 1) | (k == 2)))
    def _():
        for e in (0, 1):
            straight(e).wait_send()

    def drain_either(is_short, sem):
        @pl.when(is_short)
        def _():
            drain(short, sem)

        @pl.when(jnp.logical_not(is_short))
        def _():
            drain(whole, sem)

    @pl.when(at_source)
    def _():
        @pl.when(r > 0)
        def _():
            drain_either(k == 3, zsrc_send.at[0])

        @pl.when(r < last_row)
        def _():
            drain_either(k == 0, zsrc_send.at[1])

    @pl.when((down & (r > 0)) | ((r > k) & (r < last_row)))
    def _():
        drain_either(depth == 3, zrel_send)

    @pl.when(corner)
    def _():
        for p in (3, 2, 1):
            @pl.when(p > rank)
            def _():
                drain({1: brief, 2: shard, 3: longer}[p], deti_send.at[p])

        @pl.when(rank == 1)
        def _():
            drain(longer, detz_send.at[3])
            drain(shard, detz_send.at[2])

            drain(brief, detz_send.at[0])

        @pl.when(rank == 2)
        def _():
            drain(shard, detz_send.at[0])

        @pl.when(rank == 3)
        def _():
            drain(longer, detz_send.at[0])
            drain(longer, detz_send.at[1])

    @pl.when(between)
    def _():
        for way in (0, 1):
            @pl.when(r < last_row if way == 0 else r > 0)
            def _():
                drain(rbuf.at[0], rr_send.at[way])


def spread(index, vecs, refl, factors, frequencies):
    count = index.shape[0]
    columns, width = vecs.shape[2], refl.shape[3]
    chunks = 5
    half = count // 2
    dma = pltpu.SemaphoreType.DMA
    vmem = pl.BlockSpec(memory_space=pltpu.VMEM)
    hbm = pl.BlockSpec(memory_space=pltpu.HBM)
    return pl.pallas_call(
        functools.partial(spread_kernel, chunks),
        out_shape=(
            pltpu.VMEM((count * BLOCK, half * BLOCK), F32),
            pltpu.VMEM((8, count * BLOCK, columns), BF),
            pltpu.VMEM((4, 3, BLOCK, columns), BF),
        ),
        in_specs=[hbm] * 5,
        out_specs=(vmem,) * 3,
        scratch_shapes=[
            pltpu.SMEM((count,), jnp.int32),
            pltpu.VMEM(vecs.shape, BF),
            pltpu.VMEM(refl.shape, BF),
            pltpu.VMEM((columns, 2 * width), F32),
            pltpu.VMEM((width, width), F32),
            pltpu.VMEM((columns, 2 * width), BF),
            pltpu.VMEM(factors.shape, F32),
            pltpu.VMEM(frequencies.shape, F32),
            dma((3,)), dma((chunks,)), dma((chunks,)),
            pltpu.VMEM((8, count + half, BLOCK, columns), BF),
            pltpu.VMEM((3, count + 2, BLOCK, columns), BF),
            pltpu.VMEM((2, half + 1, BLOCK, columns), BF),
            pltpu.VMEM((4, columns // 4, 2 * width), BF),
            pltpu.VMEM((4, width // 8, width), F32),
            pltpu.VMEM((8, width // 8, width), F32),
            pltpu.VMEM((4, columns // 4, 2 * width), BF),
            pltpu.VMEM(frequencies.shape, F32),
            dma((4, 2)), dma((4, 2)), dma((4,)), dma((4,)), dma((8,)), dma((8,)), dma((4, 2)), dma((4, 2)),
            dma((3,)), dma((2,)), dma, dma((2,)), dma((4,)), dma((4,)), dma((2,)),
            dma((count,)), dma((count,)), dma((count,)), dma((4, count)),
            dma((3 * count,)), dma((2, half + 1)), dma((3, count + 2)), dma((2, half + 1)),
        ],
        compiler_params=pltpu.CompilerParams(
            collective_id=2, has_side_effects=True, vmem_limit_bytes=36 << 20
        ),
        name="spread",
    )(index, vecs, refl, factors, frequencies)


def finish_kernel(acc_ref, sa_ref, last_ref, out_ref, tail, sem, pair_sem, single_sem):
    rows, columns = acc_ref.shape
    held, blocks, lane, depth = last_ref.shape
    parts = 4
    size = rows // parts
    done = columns - blocks * lane

    def at(i):
        return pl.ds(i * size, size)

    def main_copy(i):
        lanes = pl.ds(0, done)
        return pltpu.make_async_copy(acc_ref.at[at(i), lanes], out_ref.at[at(i), lanes], sem.at[i])

    def pair_copy(i):
        return pltpu.make_async_copy(
            tail.at[at(i), pl.ds(0, 2 * lane)], out_ref.at[at(i), pl.ds(done, 2 * lane)], pair_sem.at[i]
        )

    def single_copy(i):
        return pltpu.make_async_copy(
            tail.at[at(i), pl.ds(2 * lane, lane)],
            out_ref.at[at(i), pl.ds(columns - lane, lane)], single_sem.at[i],
        )

    for i in range(parts):
        main_copy(i).start()
    for first, count, copy in ((0, 2, pair_copy), (2, 1, single_copy)):
        lanes = pl.ds(first * lane, count * lane)
        for i in range(parts):
            total = acc_ref[at(i), pl.ds(done + first * lane, count * lane)]
            for s in range(held):
                right = last_ref[s, first:first + count].reshape(count * lane, depth)
                total = total + dot_nt(sa_ref[held + s, at(i), :], right)
            tail[at(i), lanes] = total
            copy(i).start()
    for i in range(parts):
        main_copy(i).wait()
        pair_copy(i).wait()
        single_copy(i).wait()


def finish(acc, sa, last):
    vmem = pl.BlockSpec(memory_space=pltpu.VMEM)
    dma = pltpu.SemaphoreType.DMA
    return pl.pallas_call(
        finish_kernel,
        out_shape=jax.ShapeDtypeStruct(acc.shape, F32),
        in_specs=[vmem] * 3,
        out_specs=pl.BlockSpec(memory_space=pl.ANY),
        scratch_shapes=[pltpu.VMEM((acc.shape[0], last.shape[1] * last.shape[2]), F32), dma((4,)), dma((4,)), dma((4,))],
        compiler_params=pltpu.CompilerParams(vmem_limit_bytes=8 << 20),
        name="finish",
    )(acc, sa, last)


def per_device_square(eigvecs, reflectors, factors, frequencies, region_blocks):
    local_blocks = eigvecs.shape[0] // BLOCK
    in_hbm = functools.partial(pltpu.with_memory_space_constraint, memory_space=pltpu.HBM)
    acc, sa, last = spread(
        in_hbm(region_blocks),
        in_hbm(eigvecs.reshape(local_blocks, BLOCK, eigvecs.shape[1])),
        in_hbm(reflectors.reshape(2, local_blocks, BLOCK, reflectors.shape[2])),
        in_hbm(factors),
        in_hbm(frequencies.reshape(-1, 128)),
    )
    return finish(acc, sa, last)


def solution(mesh):
    shape = mesh.shape
    if shape["row"] == 4 and shape["col"] == 8:
        body = per_device_square
    else:
        body = functools.partial(per_device, shape["row"])
    return jax.shard_map(
        body,
        mesh=mesh,
        in_specs=(P("row", "col"), P(None, "row", None), P(), P(), P("row")),
        out_specs=P("row", "col"),
        check_vma=False,
    )
```

```python
import functools

import jax
import jax.numpy as jnp
from jax import lax
from jax.experimental import pallas as pl
from jax.experimental.pallas import tpu as pltpu
from jax.sharding import PartitionSpec as P

BLOCK = 128
MESH = pl.DeviceIdType.MESH
SUB = 12


def contract_rows(left, right):
    return lax.dot_general(
        left, right, (((0,), (0,)), ((), ())), preferred_element_type=jnp.float32
    )


def contract_cols(left, right):
    return lax.dot_general(
        left, right, (((1,), (1,)), ((), ())), preferred_element_type=jnp.float32
    )


def exchange_kernel(
    n_row, sub, x_ref, a_ref, b_ref, half_buf,
    own_sem, send_plane, send_sib, recv_a, send_z, recv_b, fill_sem,
):
    r = lax.axis_index("row")
    c = lax.axis_index("col")
    k = c // 2
    h = lax.rem(c, 2)
    o = 1 - h
    sib = 2 * k + o
    rows, cols = x_ref.shape
    step = rows // sub
    hsub = sub // 2
    half = rows // 2
    has_up = (r < n_row - 1).astype(jnp.int32)
    has_dn = (r > 0).astype(jnp.int32)

    barrier = pltpu.get_barrier_semaphore()

    def greet(row, col):
        pl.semaphore_signal(barrier, inc=1, device_id=(row, col), device_id_type=MESH)

    greet(r, sib)
    for d in range(1, n_row):
        greet(r, 2 * (k ^ d) + h)

    @pl.when(r < n_row - 1)
    def _():
        greet(r + 1, c)

    @pl.when(r > 0)
    def _():
        greet(r - 1, c)

    pl.semaphore_wait(barrier, n_row + has_up + has_dn)

    def piece_cols(d, side):
        owner = 2 * (k ^ d) + (h if side == 0 else o)
        return pl.ds(pl.multiple_of(owner * cols, cols), cols)

    def a_at(d, side, s):
        return a_ref.at[pl.ds(s * step, step), piece_cols(d, side)]

    def plane_copy(d, s):
        return pltpu.make_async_remote_copy(
            src_ref=x_ref.at[pl.ds(s * step, step), :],
            dst_ref=a_ref.at[pl.ds(s * step, step), piece_cols(0, 0)],
            send_sem=send_plane.at[d, s], recv_sem=recv_a.at[d, 0, s],
            device_id=(r, 2 * (k ^ d) + h), device_id_type=MESH,
        )

    def sib_copy(d, s):
        src = x_ref.at[pl.ds(s * step, step), :] if d == 0 else a_at(d, 0, s)
        return pltpu.make_async_remote_copy(
            src_ref=src, dst_ref=a_at(d, 0, s),
            send_sem=send_sib.at[d, s], recv_sem=recv_a.at[d, 1, s],
            device_id=(r, sib), device_id_type=MESH,
        )

    def half_rows(t):
        return pl.ds(pl.multiple_of(h * half + t * step, step), step)

    def z_copy(src, way, target, d, side, t):
        return pltpu.make_async_remote_copy(
            src_ref=src,
            dst_ref=b_ref.at[pl.ds(t * step, step), piece_cols(d, side)],
            send_sem=send_z.at[way, d, side, t], recv_sem=recv_b.at[d, side, t],
            device_id=(target, c), device_id_type=MESH,
        )

    def from_source(way, target, d, side, t):
        if d == 0 and side == 0:
            src = x_ref.at[half_rows(t), :]
        else:
            src = a_ref.at[half_rows(t), piece_cols(d, side)]
        return z_copy(src, way, target, d, side, t)

    def relay(way, target, d, side, t):
        src = b_ref.at[pl.ds(t * step, step), piece_cols(d, side)]
        return z_copy(src, way, target, d, side, t)

    own = pltpu.make_async_copy(x_ref, a_ref.at[:, piece_cols(0, 0)], own_sem)
    own.start()
    for s in range(sub):
        sib_copy(0, s).start()
    for d in range(1, n_row):
        for s in range(sub):
            plane_copy(d, s).start()

    arrivals = [(d, s) for d in range(1, n_row) for s in range(sub)]
    parts = [(d, side, t) for d in range(n_row) for side in (0, 1) for t in range(hsub)]

    def take_a(d, s):
        plane_copy(d, s).wait_recv()
        sib_copy(d, s).start()

    at_source = r == k
    above = r > k
    below = r < k

    @pl.when(at_source)
    def _():
        def push(d, side, t):
            @pl.when(r < n_row - 1)
            def _():
                from_source(0, r + 1, d, side, t).start()

            @pl.when(r > 0)
            def _():
                from_source(1, r - 1, d, side, t).start()

        for d in range(n_row):
            if d:
                for s in range(sub):
                    take_a(d, s)
            else:
                for t in range(hsub):
                    push(d, 0, t)
            for s in range(sub):
                sib_copy(d, s).wait_recv()
            for side in (0, 1) if d else (1,):
                for t in range(hsub):
                    push(d, side, t)
        own.wait()
        fill = pltpu.make_async_copy(
            a_ref.at[pl.ds(pl.multiple_of(h * half, half), half), :], half_buf, fill_sem
        )
        fill.start()
        fill.wait()
        out = pltpu.make_async_copy(half_buf, b_ref, fill_sem)
        out.start()
        out.wait()

    @pl.when(jnp.logical_not(at_source))
    def _():
        for i, (d, side, t) in enumerate(parts):
            if i < len(arrivals):
                take_a(*arrivals[i])
            relay(0, r, d, side, t).wait_recv()

            @pl.when(above & (r < n_row - 1))
            def _():
                relay(0, r + 1, d, side, t).start()

            @pl.when(below & (r > 0))
            def _():
                relay(1, r - 1, d, side, t).start()

        for d, s in arrivals[len(parts):]:
            take_a(d, s)
        for d in range(n_row):
            for s in range(sub):
                sib_copy(d, s).wait_recv()
        own.wait()

    for d in range(n_row):
        for s in range(sub):
            sib_copy(d, s).wait_send()
            if d:
                plane_copy(d, s).wait_send()
    for d, side, t in parts:
        @pl.when((r >= k) & (r < n_row - 1))
        def _():
            relay(0, r, d, side, t).wait_send()

        @pl.when((r <= k) & (r > 0))
        def _():
            relay(1, r, d, side, t).wait_send()


def exchange(x, n_row):
    rows, cols = x.shape
    n_col = 2 * n_row
    sub = SUB if n_row <= 4 else SUB // 2
    hsub = sub // 2
    dma = pltpu.SemaphoreType.DMA
    return pl.pallas_call(
        functools.partial(exchange_kernel, n_row, sub),
        out_shape=(
            jax.ShapeDtypeStruct((rows, cols * n_col), x.dtype),
            jax.ShapeDtypeStruct((rows // 2, cols * n_col), x.dtype),
        ),
        in_specs=[pl.BlockSpec(memory_space=pltpu.VMEM)],
        out_specs=(pl.BlockSpec(memory_space=pl.ANY),) * 2,
        scratch_shapes=[
            pltpu.VMEM((rows // 2, cols * n_col), x.dtype),
            dma,
            dma((n_row, sub)),
            dma((n_row, sub)),
            dma((n_row, 2, sub)),
            dma((2, n_row, 2, hsub)),
            dma((n_row, 2, hsub)),
            dma,
        ],
        compiler_params=pltpu.CompilerParams(collective_id=0, has_side_effects=True),
        name="exchange",
    )(x)


def project_kernel(
    n_row, w_ref, g_ref, t_ref, p_ref,
    w_in, g_in, w_sum, g_sum, w_full, g_full, send_1, recv_1, send_2, recv_2,
):
    r = lax.axis_index("row")
    c = lax.axis_index("col")
    barrier = pltpu.get_barrier_semaphore()
    for d in range(1, n_row):
        pl.semaphore_signal(barrier, inc=1, device_id=(r ^ d, c), device_id_type=MESH)
    pl.semaphore_wait(barrier, n_row - 1)
    pairs = ((w_ref, w_in, w_sum, w_full), (g_ref, g_in, g_sum, g_full))

    def part(array, owner):
        size = array.shape[0] // n_row
        return pl.ds(pl.multiple_of(owner * size, size), size)

    def scatter(d, i):
        array, landing, _, _ = pairs[i]
        return pltpu.make_async_remote_copy(
            src_ref=array.at[part(array, r ^ d), :], dst_ref=landing.at[d],
            send_sem=send_1.at[d, i], recv_sem=recv_1.at[d, i],
            device_id=(r ^ d, c), device_id_type=MESH,
        )

    def spread(d, i):
        array, _, total, full = pairs[i]
        return pltpu.make_async_remote_copy(
            src_ref=total, dst_ref=full.at[part(array, r), :],
            send_sem=send_2.at[d, i], recv_sem=recv_2.at[d, i],
            device_id=(r ^ d, c), device_id_type=MESH,
        )

    every = [(d, i) for d in range(1, n_row) for i in (1, 0)]
    for d, i in every:
        scatter(d, i).start()
    for d, i in every:
        scatter(d, i).wait_recv()
    for i in (1, 0):
        array, landing, total, full = pairs[i]
        value = array[part(array, r), :]
        for d in range(1, n_row):
            value = value + landing[d]
        total[...] = value
    for i in (1, 0):
        array, _, total, full = pairs[i]
        full[part(array, r), :] = total[...]
    for d, i in every:
        spread(d, i).start()
    for d, i in every:
        spread(d, i).wait_recv()
    highest = lax.Precision.HIGHEST
    width = g_ref.shape[0]
    second = jnp.dot(
        t_ref[1], w_full[width:, :], precision=highest, preferred_element_type=jnp.float32
    ).astype(jnp.bfloat16)
    first = w_full[:width, :] - jnp.dot(
        g_full[...], second.astype(jnp.float32),
        precision=highest, preferred_element_type=jnp.float32,
    )
    first = jnp.dot(t_ref[0], first, precision=highest, preferred_element_type=jnp.float32)
    p_ref[0] = first.astype(jnp.bfloat16)
    p_ref[1] = second
    for d, i in every:
        scatter(d, i).wait_send()
        spread(d, i).wait_send()


def project(w, g, factors, n_row):
    dma = pltpu.SemaphoreType.DMA((n_row, 2))
    width, columns = g.shape[0], w.shape[1]
    vmem = pl.BlockSpec(memory_space=pltpu.VMEM)

    def landing(array):
        return pltpu.VMEM((n_row, array.shape[0] // n_row, array.shape[1]), jnp.float32)

    def total(array):
        return pltpu.VMEM((array.shape[0] // n_row, array.shape[1]), jnp.float32)

    return pl.pallas_call(
        functools.partial(project_kernel, n_row),
        out_shape=jax.ShapeDtypeStruct((2, width, columns), jnp.bfloat16),
        in_specs=[vmem] * 3,
        out_specs=vmem,
        scratch_shapes=[
            landing(w), landing(g), total(w), total(g),
            pltpu.VMEM(w.shape, jnp.float32), pltpu.VMEM(g.shape, jnp.float32),
            dma, dma, dma, dma,
        ],
        compiler_params=pltpu.CompilerParams(collective_id=1, has_side_effects=True),
        name="project",
    )(w, g, factors)


def region_kernel(index_ref, p_ref, vecs_ref, refl_ref, out_ref, vecs, refl, sems):
    count = vecs.shape[0]

    def copies(b):
        at = index_ref[b]
        return (
            pltpu.make_async_copy(vecs_ref.at[at], vecs.at[b], sems.at[b, 0]),
            pltpu.make_async_copy(refl_ref.at[0, at], refl.at[0, b], sems.at[b, 1]),
            pltpu.make_async_copy(refl_ref.at[1, at], refl.at[1, b], sems.at[b, 2]),
        )

    for b in range(count):
        for copy in copies(b):
            copy.start()
    for b in range(count):
        for copy in copies(b):
            copy.wait()
        value = vecs[b].astype(jnp.float32)
        value = value - jnp.dot(refl[1, b], p_ref[1], preferred_element_type=jnp.float32)
        value = value - jnp.dot(refl[0, b], p_ref[0], preferred_element_type=jnp.float32)
        out_ref[b] = value.astype(out_ref.dtype)


def region_rows(index, applied, vecs, refl):
    count = index.shape[0]
    columns, width = vecs.shape[2], refl.shape[3]
    vmem = pl.BlockSpec(memory_space=pltpu.VMEM)
    hbm = pl.BlockSpec(memory_space=pl.ANY)
    return pl.pallas_call(
        region_kernel,
        out_shape=jax.ShapeDtypeStruct((count, BLOCK, columns), vecs.dtype),
        in_specs=[pl.BlockSpec(memory_space=pltpu.SMEM), vmem, hbm, hbm],
        out_specs=vmem,
        scratch_shapes=[
            pltpu.VMEM((count, BLOCK, columns), vecs.dtype),
            pltpu.VMEM((2, count, BLOCK, width), refl.dtype),
            pltpu.SemaphoreType.DMA((count, 3)),
        ],
        name="region",
    )(index, applied, vecs, refl)


def per_device(n_row, eigvecs, reflectors, factors, frequencies, region_blocks):
    columns = eigvecs.shape[1]
    width = reflectors.shape[2]
    local = lax.dot_general(
        reflectors, eigvecs, (((1,), (0,)), ((), ())), preferred_element_type=jnp.float32
    ).reshape(2 * width, columns)
    cross_local = contract_rows(reflectors[0], reflectors[1])
    applied = project(local, cross_local, jnp.triu(factors), n_row)
    local_blocks = eigvecs.shape[0] // BLOCK
    local_index = region_blocks - lax.axis_index("row") * local_blocks
    region = region_rows(
        local_index,
        applied,
        eigvecs.reshape(local_blocks, BLOCK, columns),
        reflectors.reshape(2, local_blocks, BLOCK, width),
    ).reshape(-1, columns)
    weight = 1.0 / jnp.tanh(frequencies / 2.0) / (2.0 * frequencies)
    mine, partner = exchange(region, n_row)
    scaled = (mine.astype(jnp.float32) * weight[None, :]).astype(jnp.bfloat16)
    return contract_cols(scaled, partner)


BF = jnp.bfloat16
F32 = jnp.float32
HIGH = lax.Precision.HIGHEST


def dot_nt(left, right, **kw):
    return lax.dot_general(left, right, (((1,), (1,)), ((), ())), preferred_element_type=F32, **kw)


def dot_tn(left, right):
    return lax.dot_general(left, right, (((0,), (0,)), ((), ())), preferred_element_type=F32)


def spread_kernel(
    chunks, index_ref, vecs_ref, refl_ref, factor_ref, freq_ref, acc_ref, sa_ref, last_ref,
    index, vecs, refl, w_sum, g_sum, w_ref, t_ref, f_ref, small_sem, vec_sem, refl_sem, buf, tbuf, rbuf, w_in, g_in, g_full, p_full, weight,
    w_send, w_recv, g_send, g_recv, h_send, h_recv, p_send, p_recv,
    own_send, relay_send, zrel_send, zsrc_send, detz_send, deti_send, rr_send,
    ax, ay, ad, asib, zb, det, tz, rr,
):
    r = lax.axis_index("row")
    c = lax.axis_index("col")
    k = c // 2
    h = lax.rem(c, 2)
    o = 1 - h
    count = index.shape[0]
    half = count // 2
    columns = vecs.shape[2]
    width = refl.shape[3]
    blocks = vecs.shape[0] // chunks
    quarter = columns // 4
    last_row = 3

    def col(chip, core):
        return 2 * chip + core

    barrier = pltpu.get_barrier_semaphore()

    def greet(row, column):
        pl.semaphore_signal(barrier, inc=1, device_id=(row, column), device_id_type=MESH)

    for d in range(1, 4):
        greet(lax.rem(r + d, 4), c)
    for e in range(1, 8):
        greet(r, c ^ e)

    def load_vecs(i):
        part = pl.ds(i * blocks, blocks)
        return pltpu.make_async_copy(vecs_ref.at[part], vecs.at[part], vec_sem.at[i])

    def load_refl(i):
        part = pl.ds(i * blocks, blocks)
        return pltpu.make_async_copy(refl_ref.at[:, part], refl.at[:, part], refl_sem.at[i])

    def rows_of(array, i):
        return array[pl.ds(i * blocks, blocks)].reshape(blocks * BLOCK, array.shape[2])

    for i in range(chunks):
        load_refl(i).start()
    load_vecs(0).start()
    small = [
        pltpu.make_async_copy(src, dst, small_sem.at[i])
        for i, (src, dst) in enumerate(((index_ref, index), (factor_ref, t_ref), (freq_ref, f_ref)))
    ]
    for copy in small:
        copy.start()
    for i in range(chunks):
        if i + 1 < chunks:
            load_vecs(i + 1).start()
        load_refl(i).wait()
        g = dot_tn(rows_of(refl.at[0], i), rows_of(refl.at[1], i))
        if i:
            g = g + g_sum[...]
        g_sum[...] = g
    for copy in small:
        copy.wait()

    pl.semaphore_wait(barrier, 10)

    def remote(src, dst, send, recv, row, column):
        return pltpu.make_async_remote_copy(
            src_ref=src, dst_ref=dst, send_sem=send, recv_sem=recv,
            device_id=(row, column), device_id_type=MESH,
        )

    far = [jnp.where(r < 2, 3, 0), jnp.where(r < 2, 2, 1), jnp.where(r < 2, 1 - r, 5 - r)]

    def w_copy(q, part):
        d = lax.rem(q - r + 4, 4)
        rows = pl.ds(pl.multiple_of(q * quarter, quarter), quarter)
        lanes = pl.ds(part * width, width)
        return remote(
            w_ref.at[rows, lanes], w_in.at[d, :, lanes], w_send.at[d, part], w_recv.at[d, part], q, c
        )

    g_rows = width // 8
    g_part = pl.ds(pl.multiple_of(c * g_rows, g_rows), g_rows)

    def g_copy(q):
        d = lax.rem(q - r + 4, 4)
        return remote(g_sum.at[g_part], g_in.at[d], g_send.at[d], g_recv.at[d], q, c)

    for q in far:
        g_copy(q).start()
    for i in range(chunks):
        load_vecs(i).wait()
        y = jnp.concatenate([rows_of(refl.at[0], i), rows_of(refl.at[1], i)], axis=1)
        w = dot_tn(rows_of(vecs, i), y)
        if i:
            w = w + w_sum[...]
        w_sum[...] = w
    w_ref[...] = w.astype(BF)
    for part in (1, 0):
        for q in far:
            w_copy(q, part).start()
    for q in far:
        g_copy(q).wait_recv()
    value = g_sum[g_part, :]
    for d in (1, 2, 3):
        value = value + g_in[d]
    g_full[c] = value

    def h_copy(e):
        return remote(g_full.at[c], g_full.at[c], h_send.at[e], h_recv.at[e], r, c ^ e)

    def h_arrival(e):
        return remote(g_full.at[c ^ e], g_full.at[c ^ e], h_send.at[e], h_recv.at[e], r, c ^ e)

    for e in range(1, 8):
        h_copy(e).start()

    f = f_ref[...]
    weight[...] = 1.0 / jnp.tanh(f / 2.0) / (2.0 * f)
    row_at = lax.broadcasted_iota(jnp.int32, (width, width), 0)
    col_at = lax.broadcasted_iota(jnp.int32, (width, width), 1)
    upper = row_at <= col_at
    zero = jnp.zeros((width, width), F32)
    t0 = jnp.where(upper, t_ref[0], zero)
    t1 = jnp.where(upper, t_ref[1], zero)

    mine = pl.ds(pl.multiple_of(r * quarter, quarter), quarter)

    def w_total(part):
        lanes = pl.ds(part * width, width)
        for q in far:
            w_copy(q, part).wait_recv()
        w = w_sum[mine, lanes]
        for d in (1, 2, 3):
            w = w + w_in[d, :, lanes].astype(F32)
        return w

    def p_copy(q, part):
        d = lax.rem(q - r + 4, 4)
        at = p_full.at[r, :, pl.ds(part * width, width)]
        return remote(at, at, p_send.at[d, part], p_recv.at[d, part], q, c)

    def p_arrival(q, part):
        d = lax.rem(r - q + 4, 4)
        at = p_full.at[q, :, pl.ds(part * width, width)]
        return remote(at, at, p_send.at[d, part], p_recv.at[d, part], q, c)

    second = dot_nt(w_total(1), t1, precision=HIGH).astype(BF)
    p_full[r, :, width:] = second
    for q in far:
        p_copy(q, 1).start()
    first = w_total(0)
    for e in range(1, 8):
        h_arrival(e).wait_recv()
    g = g_full[...].reshape(width, width)
    first = first - dot_nt(second.astype(F32), g, precision=HIGH)
    p_full[r, :, :width] = dot_nt(first, t0, precision=HIGH).astype(BF)
    for q in far:
        p_copy(q, 0).start()
    for part in (1, 0):
        for q in far:
            p_arrival(q, part).wait_recv()

    def block_of(n):
        return lax.rem(n, 2) * half + n // 2

    def a_copy(way, n):
        b = block_of(n)
        src = buf.at[c, b]
        if way == 2:
            return remote(src, buf.at[c, b], own_send.at[2], asib.at[0, n], r, col(k, o))
        sem = ax if way == 0 else ay
        return remote(src, buf.at[c, b], own_send.at[way], sem.at[n], r, col(k ^ (way + 1), h))

    corner = (k == 0) | (k == 3)
    is_low = k == 0
    rank = jnp.where(is_low, r, 3 - r)
    away = jnp.where(is_low, -1, 1)
    slot = jnp.where(is_low, 0, 1)
    early = 4

    extra = 2
    near = count - extra

    def det_more(hops, i):
        b = half - 1 + i * half
        return remote(
            buf.at[col(k ^ 1, h), b], tbuf.at[rank - 1, count + i], detz_send.at[hops - 1],
            tz.at[rank - 1, count + i], r + away * hops, c,
        )

    def slot_of(n):
        return jnp.where(n < count, block_of(n), n)

    def det_own(hops, n):
        b = block_of(n)
        return remote(
            buf.at[c, b], tbuf.at[rank - 1, b], detz_send.at[hops - 1], tz.at[rank - 1, n],
            r + away * hops, c,
        )

    down = r < k
    at_source = r == k
    step = jnp.where(down, -1, 1)
    depth = jnp.where(down, k, 3 - k)

    def z_piece(t, depth, is_down):
        third = t // (2 * half)
        n = jnp.where(third == 0, lax.rem(t, half), lax.rem(t, 2 * half) // 2)
        e = jnp.where(third == 0, t // half, lax.rem(t, 2))
        j1 = jnp.where(depth == 3, 2, 3)
        j2 = 6 - depth - j1
        j = jnp.where(third == 0, depth, jnp.where(third == 1, j1, j2))
        j = jnp.where(is_down, j, 3 - j)
        return col(j, lax.rem(h + e, 2)), n

    steps = 3 * 2 * half

    def z_relay(t):
        src, n = z_piece(t, depth, down)
        at = buf.at[src, count + n]
        return remote(at, at, zrel_send, zb.at[t], r + step, c)

    def z_source(t, is_down):
        src, n = z_piece(t, k if is_down else 3 - k, jnp.bool_(is_down))
        return remote(
            buf.at[src, h * half + n], buf.at[src, count + n],
            zsrc_send.at[0 if is_down else 1], zb.at[t], r + (-1 if is_down else 1), c,
        )

    def z_source_step(t):
        @pl.when(at_source)
        def _():
            @pl.when((r > 0) & ((k < 3) | (t < steps - extra)))
            def _():
                z_source(t, True).start()

            @pl.when((r < last_row) & ((k > 0) | (t < steps - extra)))
            def _():
                z_source(t, False).start()

    applied = p_full[...].reshape(columns, 2 * width)

    base = r * vecs.shape[0]

    def make_region(n, _):
        b = block_of(n)
        at = jnp.clip(index[b] - base, 0, vecs.shape[0] - 1)
        y = jnp.concatenate([refl[0, at], refl[1, at]], axis=1)
        buf[c, b] = (vecs[at].astype(F32) - dot_nt(y, applied)).astype(BF)
        for way in (0, 1, 2):
            a_copy(way, n).start()

        @pl.when(corner & ((rank > 1) | ((rank == 1) & (n < early))))
        def _():
            @pl.when(rank == 3)
            def _():
                det_own(2, n).start()

            det_own(1, n).start()

        @pl.when(lax.rem(n, 2) == h)
        def _():
            z_source_step(n // 2)

        return 0

    lax.fori_loop(0, count, make_region, 0)

    def a_arrival(way, n):
        src = col(k ^ (way + 1), h)
        b = block_of(n)
        at = buf.at[src, b]
        sem = (ax, ay, ad)[way]
        return remote(at, at, own_send.at[2], sem.at[n], r, col(k, o))

    def sib_copy(j, n):
        src = col(k ^ j, h)
        b = block_of(n)
        at = buf.at[src, b]
        return remote(at, at, own_send.at[2], asib.at[j, n], r, col(k, o))

    def sib_arrival(j, n):
        src = col(k ^ j, o)
        b = block_of(n)
        at = buf.at[src, b]
        return remote(at, at, own_send.at[2], asib.at[j, n], r, col(k, o))

    def relay(way, n):
        src = col(k ^ (way + 1), h)
        at = buf.at[src, block_of(n)]
        to = k ^ (2 - way)
        return remote(at, at, relay_send.at[way], ad.at[n], r, col(to, h))

    def det_z(p, n):
        at = tbuf.at[p - 1, slot_of(n)]
        return remote(at, at, detz_send.at[p], tz.at[p - 1, n], r + away, c)

    def det_plane(p, n):
        src = tbuf.at[p - 1, slot_of(n)]
        core = lax.rem(n, 2)
        if p < 3:
            return remote(
                src, buf.at[c, count + n // 2], deti_send.at[p], det.at[h, n // 2],
                r, col(k ^ p, core),
            )
        return remote(
            src, rbuf.at[slot, n // 2], deti_send.at[p], rr.at[slot, n // 2],
            r, col(k ^ (1 + h), core),
        )

    between = (k == 1) | (k == 2)

    def rr_copy(way, n):
        low = k - 1 if way == 0 else 2 - k
        more = (n == half).astype(jnp.int32)
        src = low + 2 * more if way == 0 else low + 6 - 2 * more
        return remote(
            rbuf.at[way, n], buf.at[src, count + n - more], rr_send.at[way], det.at[low, n],
            r, col(3 if way == 0 else 0, h),
        )

    def det_arrival(low, n, more=0):
        src = jnp.where(down, low + 2 * more, low + 6 - 2 * more)
        at = buf.at[src, count + n - more]
        return remote(at, at, own_send.at[2], det.at[low, n], r, col(k, o))

    mine_at = jnp.where(at_source, h * half, count)

    from_low = jnp.logical_not(down | (at_source & (k >= 2)))
    deep = jnp.where(from_low, 3 - k, k)
    mid = jnp.where(deep == 3, 2, 3)
    order = []
    for j in (deep, mid, 6 - deep - mid, 0):
        j = jnp.where(from_low, 3 - j, j)
        order += [col(j, 0), col(j, 1)]

    def at_place(s):
        src = order[0]
        for i in range(1, 8):
            src = jnp.where(s == i, order[i], src)
        return src

    def scale(s, part):
        src = at_place(s)
        wt = jnp.concatenate([weight[pl.ds(2 * src, 1), :], weight[pl.ds(2 * src + 1, 1), :]], axis=1)

        def one(i, _):
            b = part * half + i
            rows = pl.ds(pl.multiple_of(b * BLOCK, BLOCK), BLOCK)
            sa_ref[s, rows, :] = (buf[src, b].astype(F32) * wt).astype(BF)
            return 0

        lax.fori_loop(0, half, one, 0)

    tile = 2 * BLOCK
    row_tile = acc_ref.shape[0] // 3

    def product(block, lane, size, third, places, add):
        at = mine_at + block
        lanes = pl.ds(pl.multiple_of(lane, BLOCK), size * BLOCK)
        rows = pl.ds(pl.multiple_of(third * row_tile, row_tile), row_tile)
        total = jnp.zeros((row_tile, size * BLOCK), F32)
        for s in places:
            right = buf[order[s], pl.ds(at, size)].reshape(size * BLOCK, columns)
            total = total + dot_nt(sa_ref[s, rows, :], right)
        if add:
            total = total + acc_ref[rows, lanes]
        acc_ref[rows, lanes] = total

    def pair(q, third, places, add):
        product(2 * q, q * tile, 2, third, places, add)

    def straight(e):
        core = lax.rem(h + e, 2)
        src = col(k ^ 1, core)
        return remote(
            buf.at[src, h * half + half - 1], buf.at[src, count + half - 1], detz_send.at[e],
            det.at[core, half - 1], r + jnp.where(k == 1, -1, 1), c,
        )

    def wait_more():
        @pl.when(jnp.logical_not(at_source) & (depth == 3))
        def _():
            for low in (0, 1):
                det_arrival(low, half, 1).wait_recv()

    def wait_detours(n):
        @pl.when(jnp.logical_not(at_source))
        def _():
            for low in (0, 1):
                det_arrival(low, n).wait_recv()

    hops = jnp.where(down, k - r, r - k)
    lag = 2

    def z_relay_step(u):
        t = u - lag * hops

        @pl.when(jnp.logical_not(at_source) & (t >= 0) & (t < jnp.where(depth == 3, steps - extra, steps)))
        def _():
            z_relay(t).wait_recv()

            @pl.when((down & (r > 0)) | (jnp.logical_not(down) & (r < last_row)))
            def _():
                z_relay(t).start()

    def first_third(n, _):
        sib_arrival(0, 2 * n).wait_recv()
        sib_arrival(0, 2 * n + 1).wait_recv()
        z_source_step(half + n)
        return 0

    lax.fori_loop(0, half, first_third, 0)


    def beat(u, _):
        def span(first, length):
            return (u >= first) & (u < first + length)


        @pl.when(span(2, count))
        def _():
            n = u - 2
            for way in (0, 1):
                a_arrival(way, n).wait_recv()
                sib_copy(way + 1, n).start()
            even = lax.rem(n, 2) == 0

            @pl.when(even)
            def _():
                relay(0, n).start()

            @pl.when(jnp.logical_not(even))
            def _():
                relay(1, n).start()

        @pl.when(span(4, count))
        def _():
            n = u - 4
            sib_arrival(1, n).wait_recv()
            sib_arrival(2, n).wait_recv()

        @pl.when(span(6, count))
        def _():
            z_source_step(u + count - 6)

        @pl.when(corner)
        def _():
            n5 = (u - 3) // 2

            @pl.when((rank == 1) & span(3, 2 * (count + extra)) & (lax.rem(u - 3, 2) == 0))
            def _():
                det_z(3, n5).wait_recv()
                det_z(3, n5).start()

                @pl.when(n5 < count)
                def _():
                    det_z(2, n5).wait_recv()
                    det_z(2, n5).start()

            @pl.when((rank == 3) & span(20, extra))
            def _():
                det_more(2, u - 20).start()
                det_more(1, u - 20).start()

            @pl.when((rank == 1) & span(36, near - early))
            def _():
                det_own(1, u - 36 + early).start()

            v = u - 22
            n3 = (4 * v + 4) // 5

            @pl.when((rank < 3) & span(22, 24) & (lax.rem(v, 5) != 4))
            def _():
                @pl.when(rank != 1)
                def _():
                    det_z(3, n3).wait_recv()

                det_plane(3, n3).start()

            v2 = u - 28
            n2 = (2 * v2) // 3

            @pl.when((rank < 2) & span(28, 27) & (lax.rem(v2, 3) != 1))
            def _():
                @pl.when(rank != 1)
                def _():
                    det_z(2, n2).wait_recv()

                det_plane(2, n2).start()

            @pl.when((rank == 0) & (span(22, early) | span(39 + early, near - early)))
            def _():
                n = jnp.where(u < 40, u - 22, u - 39)
                det_z(1, n).wait_recv()
                det_plane(1, n).start()

        w = u - 30
        item = (4 * w + 4) // 5

        @pl.when(between & span(30, 24) & (lax.rem(w, 5) != 4) & (lax.rem(item, 2) == h))
        def _():
            n = item // 2
            for way in (0, 1):
                @pl.when(r < last_row if way == 0 else r > 0)
                def _():
                    at = rbuf.at[way, n]
                    remote(at, at, rr_send.at[way], rr.at[way, n], r, col(k, o)).wait_recv()
                    rr_copy(way, n).start()

        @pl.when(span(23, half))
        def _():
            for i in range(2):
                n = 2 * (u - 23) + i
                a_arrival(2, n).wait_recv()
                sib_copy(3, n).start()

        @pl.when(span(25, half))
        def _():
            for i in range(2):
                sib_arrival(3, 2 * (u - 25) + i).wait_recv()

        @pl.when(span(27, count))
        def _():
            z_source_step(u + 2 * count - 27)

        z_relay_step(u)

        @pl.when(at_source & (u == 36) & ((k == 1) | (k == 2)))
        def _():
            for e in (0, 1):
                straight(e).start()

        for first, length, place in ((6, 4, 0), (22, 4, 2), (34, 8, 4)):
            @pl.when(span(first, length))
            def _():
                scale(place + (u - first) // 2, lax.rem(u - first, 2))

        for first, q in ((27, 0), (31, 1), (42, 2)):
            @pl.when(span(first, 3))
            def _():
                pair(q, u - first, range(4), False)

        q = (u - 46) // 4
        i = lax.rem(u - 46, 4)

        @pl.when((u == 45) | (u == 49) | (u == 53))
        def _():
            pair(3, (u - 45) // 4, range(4), False)

        @pl.when(span(46, 12) & (i == 0))
        def _():
            wait_detours(2 * q)
            wait_detours(2 * q + 1)

        @pl.when(span(46, 12) & (i < 3))
        def _():
            pair(q, i, range(4, 8), True)

        @pl.when((u == 47) | (u == 51) | (u == 55))
        def _():
            product(8, 4 * tile, 1, (u - 47) // 4, range(4), False)

        return 0

    lax.fori_loop(0, steps + 2 * lag, beat, 0)
    wait_detours(6)
    wait_detours(7)
    wait_detours(8)
    wait_more()
    for s in range(4):
        last_ref[s] = buf[order[4 + s], pl.ds(mine_at + 6, 3)]

    def drain(ref, sem):
        pltpu.make_async_copy(ref, ref, sem).wait()

    for q in far:
        g_copy(q).wait_send()
        for part in (0, 1):
            w_copy(q, part).wait_send()
            p_copy(q, part).wait_send()
    for e in range(1, 8):
        h_copy(e).wait_send()
    shard = buf.at[0, pl.ds(0, count)]
    for way in (0, 1):
        drain(shard, own_send.at[way])
        drain(buf.at[0, pl.ds(0, half)], relay_send.at[way])
    drain(buf.at[:, pl.ds(0, half)], own_send.at[2])

    whole = buf.at[pl.ds(0, 2)]
    short = buf.at[pl.ds(0, 2), pl.ds(0, count + half - extra // 2)]
    longer = buf.at[0, pl.ds(0, count + extra)]
    brief = buf.at[0, pl.ds(0, near)]

    @pl.when(at_source & ((k == 1) | (k == 2)))
    def _():
        for e in (0, 1):
            straight(e).wait_send()

    def drain_either(is_short, sem):
        @pl.when(is_short)
        def _():
            drain(short, sem)

        @pl.when(jnp.logical_not(is_short))
        def _():
            drain(whole, sem)

    @pl.when(at_source)
    def _():
        @pl.when(r > 0)
        def _():
            drain_either(k == 3, zsrc_send.at[0])

        @pl.when(r < last_row)
        def _():
            drain_either(k == 0, zsrc_send.at[1])

    @pl.when((down & (r > 0)) | ((r > k) & (r < last_row)))
    def _():
        drain_either(depth == 3, zrel_send)

    @pl.when(corner)
    def _():
        for p in (3, 2, 1):
            @pl.when(p > rank)
            def _():
                drain({1: brief, 2: shard, 3: longer}[p], deti_send.at[p])

        @pl.when(rank == 1)
        def _():
            drain(longer, detz_send.at[3])
            drain(shard, detz_send.at[2])

            drain(brief, detz_send.at[0])

        @pl.when(rank == 2)
        def _():
            drain(shard, detz_send.at[0])

        @pl.when(rank == 3)
        def _():
            drain(longer, detz_send.at[0])
            drain(longer, detz_send.at[1])

    @pl.when(between)
    def _():
        for way in (0, 1):
            @pl.when(r < last_row if way == 0 else r > 0)
            def _():
                drain(rbuf.at[0], rr_send.at[way])


def spread(index, vecs, refl, factors, frequencies):
    count = index.shape[0]
    columns, width = vecs.shape[2], refl.shape[3]
    chunks = 5
    half = count // 2
    dma = pltpu.SemaphoreType.DMA
    vmem = pl.BlockSpec(memory_space=pltpu.VMEM)
    hbm = pl.BlockSpec(memory_space=pltpu.HBM)
    return pl.pallas_call(
        functools.partial(spread_kernel, chunks),
        out_shape=(
            pltpu.VMEM((count * BLOCK, half * BLOCK), F32),
            pltpu.VMEM((8, count * BLOCK, columns), BF),
            pltpu.VMEM((4, 3, BLOCK, columns), BF),
        ),
        in_specs=[hbm] * 5,
        out_specs=(vmem,) * 3,
        scratch_shapes=[
            pltpu.SMEM((count,), jnp.int32),
            pltpu.VMEM(vecs.shape, BF),
            pltpu.VMEM(refl.shape, BF),
            pltpu.VMEM((columns, 2 * width), F32),
            pltpu.VMEM((width, width), F32),
            pltpu.VMEM((columns, 2 * width), BF),
            pltpu.VMEM(factors.shape, F32),
            pltpu.VMEM(frequencies.shape, F32),
            dma((3,)), dma((chunks,)), dma((chunks,)),
            pltpu.VMEM((8, count + half, BLOCK, columns), BF),
            pltpu.VMEM((3, count + 2, BLOCK, columns), BF),
            pltpu.VMEM((2, half + 1, BLOCK, columns), BF),
            pltpu.VMEM((4, columns // 4, 2 * width), BF),
            pltpu.VMEM((4, width // 8, width), F32),
            pltpu.VMEM((8, width // 8, width), F32),
            pltpu.VMEM((4, columns // 4, 2 * width), BF),
            pltpu.VMEM(frequencies.shape, F32),
            dma((4, 2)), dma((4, 2)), dma((4,)), dma((4,)), dma((8,)), dma((8,)), dma((4, 2)), dma((4, 2)),
            dma((3,)), dma((2,)), dma, dma((2,)), dma((4,)), dma((4,)), dma((2,)),
            dma((count,)), dma((count,)), dma((count,)), dma((4, count)),
            dma((3 * count,)), dma((2, half + 1)), dma((3, count + 2)), dma((2, half + 1)),
        ],
        compiler_params=pltpu.CompilerParams(
            collective_id=2, has_side_effects=True, vmem_limit_bytes=36 << 20
        ),
        name="spread",
    )(index, vecs, refl, factors, frequencies)


def finish_kernel(acc_ref, sa_ref, last_ref, out_ref, tail, sem, pair_sem, single_sem):
    rows, columns = acc_ref.shape
    held, blocks, lane, depth = last_ref.shape
    parts = 4
    size = rows // parts
    done = columns - blocks * lane

    def at(i):
        return pl.ds(i * size, size)

    def main_copy(i):
        lanes = pl.ds(0, done)
        return pltpu.make_async_copy(acc_ref.at[at(i), lanes], out_ref.at[at(i), lanes], sem.at[i])

    def pair_copy(i):
        return pltpu.make_async_copy(
            tail.at[at(i), pl.ds(0, 2 * lane)], out_ref.at[at(i), pl.ds(done, 2 * lane)], pair_sem.at[i]
        )

    def single_copy(i):
        return pltpu.make_async_copy(
            tail.at[at(i), pl.ds(2 * lane, lane)],
            out_ref.at[at(i), pl.ds(columns - lane, lane)], single_sem.at[i],
        )

    for i in range(parts):
        main_copy(i).start()
    for first, count, copy in ((0, 2, pair_copy), (2, 1, single_copy)):
        lanes = pl.ds(first * lane, count * lane)
        for i in range(parts):
            total = acc_ref[at(i), pl.ds(done + first * lane, count * lane)]
            for s in range(held):
                right = last_ref[s, first:first + count].reshape(count * lane, depth)
                total = total + dot_nt(sa_ref[held + s, at(i), :], right)
            tail[at(i), lanes] = total
            copy(i).start()
    for i in range(parts):
        main_copy(i).wait()
        pair_copy(i).wait()
        single_copy(i).wait()


def finish(acc, sa, last):
    vmem = pl.BlockSpec(memory_space=pltpu.VMEM)
    dma = pltpu.SemaphoreType.DMA
    return pl.pallas_call(
        finish_kernel,
        out_shape=jax.ShapeDtypeStruct(acc.shape, F32),
        in_specs=[vmem] * 3,
        out_specs=pl.BlockSpec(memory_space=pl.ANY),
        scratch_shapes=[pltpu.VMEM((acc.shape[0], last.shape[1] * last.shape[2]), F32), dma((4,)), dma((4,)), dma((4,))],
        compiler_params=pltpu.CompilerParams(vmem_limit_bytes=8 << 20),
        name="finish",
    )(acc, sa, last)


def per_device_square(eigvecs, reflectors, factors, frequencies, region_blocks):
    local_blocks = eigvecs.shape[0] // BLOCK
    in_hbm = functools.partial(pltpu.with_memory_space_constraint, memory_space=pltpu.HBM)
    acc, sa, last = spread(
        in_hbm(region_blocks),
        in_hbm(eigvecs.reshape(local_blocks, BLOCK, eigvecs.shape[1])),
        in_hbm(reflectors.reshape(2, local_blocks, BLOCK, reflectors.shape[2])),
        in_hbm(factors),
        in_hbm(frequencies.reshape(-1, 128)),
    )
    return finish(acc, sa, last)


def solution(mesh):
    shape = mesh.shape
    if shape["row"] == 4 and shape["col"] == 8:
        body = per_device_square
    else:
        body = functools.partial(per_device, shape["row"])
    return jax.shard_map(
        body,
        mesh=mesh,
        in_specs=(P("row", "col"), P(None, "row", None), P(), P(), P("row")),
        out_specs=P("row", "col"),
        check_vma=False,
    )
```

```python
import functools

import jax
import jax.numpy as jnp
from jax import lax
from jax.experimental import pallas as pl
from jax.experimental.pallas import tpu as pltpu
from jax.sharding import PartitionSpec as P

BLOCK = 128
MESH = pl.DeviceIdType.MESH
SUB = 12


def contract_rows(left, right):
    return lax.dot_general(
        left, right, (((0,), (0,)), ((), ())), preferred_element_type=jnp.float32
    )


def contract_cols(left, right):
    return lax.dot_general(
        left, right, (((1,), (1,)), ((), ())), preferred_element_type=jnp.float32
    )


def exchange_kernel(
    n_row, sub, x_ref, a_ref, b_ref, half_buf,
    own_sem, send_plane, send_sib, recv_a, send_z, recv_b, fill_sem,
):
    r = lax.axis_index("row")
    c = lax.axis_index("col")
    k = c // 2
    h = lax.rem(c, 2)
    o = 1 - h
    sib = 2 * k + o
    rows, cols = x_ref.shape
    step = rows // sub
    hsub = sub // 2
    half = rows // 2
    has_up = (r < n_row - 1).astype(jnp.int32)
    has_dn = (r > 0).astype(jnp.int32)

    barrier = pltpu.get_barrier_semaphore()

    def greet(row, col):
        pl.semaphore_signal(barrier, inc=1, device_id=(row, col), device_id_type=MESH)

    greet(r, sib)
    for d in range(1, n_row):
        greet(r, 2 * (k ^ d) + h)

    @pl.when(r < n_row - 1)
    def _():
        greet(r + 1, c)

    @pl.when(r > 0)
    def _():
        greet(r - 1, c)

    pl.semaphore_wait(barrier, n_row + has_up + has_dn)

    def piece_cols(d, side):
        owner = 2 * (k ^ d) + (h if side == 0 else o)
        return pl.ds(pl.multiple_of(owner * cols, cols), cols)

    def a_at(d, side, s):
        return a_ref.at[pl.ds(s * step, step), piece_cols(d, side)]

    def plane_copy(d, s):
        return pltpu.make_async_remote_copy(
            src_ref=x_ref.at[pl.ds(s * step, step), :],
            dst_ref=a_ref.at[pl.ds(s * step, step), piece_cols(0, 0)],
            send_sem=send_plane.at[d, s], recv_sem=recv_a.at[d, 0, s],
            device_id=(r, 2 * (k ^ d) + h), device_id_type=MESH,
        )

    def sib_copy(d, s):
        src = x_ref.at[pl.ds(s * step, step), :] if d == 0 else a_at(d, 0, s)
        return pltpu.make_async_remote_copy(
            src_ref=src, dst_ref=a_at(d, 0, s),
            send_sem=send_sib.at[d, s], recv_sem=recv_a.at[d, 1, s],
            device_id=(r, sib), device_id_type=MESH,
        )

    def half_rows(t):
        return pl.ds(pl.multiple_of(h * half + t * step, step), step)

    def z_copy(src, way, target, d, side, t):
        return pltpu.make_async_remote_copy(
            src_ref=src,
            dst_ref=b_ref.at[pl.ds(t * step, step), piece_cols(d, side)],
            send_sem=send_z.at[way, d, side, t], recv_sem=recv_b.at[d, side, t],
            device_id=(target, c), device_id_type=MESH,
        )

    def from_source(way, target, d, side, t):
        if d == 0 and side == 0:
            src = x_ref.at[half_rows(t), :]
        else:
            src = a_ref.at[half_rows(t), piece_cols(d, side)]
        return z_copy(src, way, target, d, side, t)

    def relay(way, target, d, side, t):
        src = b_ref.at[pl.ds(t * step, step), piece_cols(d, side)]
        return z_copy(src, way, target, d, side, t)

    own = pltpu.make_async_copy(x_ref, a_ref.at[:, piece_cols(0, 0)], own_sem)
    own.start()
    for s in range(sub):
        sib_copy(0, s).start()
    for d in range(1, n_row):
        for s in range(sub):
            plane_copy(d, s).start()

    arrivals = [(d, s) for d in range(1, n_row) for s in range(sub)]
    parts = [(d, side, t) for d in range(n_row) for side in (0, 1) for t in range(hsub)]

    def take_a(d, s):
        plane_copy(d, s).wait_recv()
        sib_copy(d, s).start()

    at_source = r == k
    above = r > k
    below = r < k

    @pl.when(at_source)
    def _():
        def push(d, side, t):
            @pl.when(r < n_row - 1)
            def _():
                from_source(0, r + 1, d, side, t).start()

            @pl.when(r > 0)
            def _():
                from_source(1, r - 1, d, side, t).start()

        for d in range(n_row):
            if d:
                for s in range(sub):
                    take_a(d, s)
            else:
                for t in range(hsub):
                    push(d, 0, t)
            for s in range(sub):
                sib_copy(d, s).wait_recv()
            for side in (0, 1) if d else (1,):
                for t in range(hsub):
                    push(d, side, t)
        own.wait()
        fill = pltpu.make_async_copy(
            a_ref.at[pl.ds(pl.multiple_of(h * half, half), half), :], half_buf, fill_sem
        )
        fill.start()
        fill.wait()
        out = pltpu.make_async_copy(half_buf, b_ref, fill_sem)
        out.start()
        out.wait()

    @pl.when(jnp.logical_not(at_source))
    def _():
        for i, (d, side, t) in enumerate(parts):
            if i < len(arrivals):
                take_a(*arrivals[i])
            relay(0, r, d, side, t).wait_recv()

            @pl.when(above & (r < n_row - 1))
            def _():
                relay(0, r + 1, d, side, t).start()

            @pl.when(below & (r > 0))
            def _():
                relay(1, r - 1, d, side, t).start()

        for d, s in arrivals[len(parts):]:
            take_a(d, s)
        for d in range(n_row):
            for s in range(sub):
                sib_copy(d, s).wait_recv()
        own.wait()

    for d in range(n_row):
        for s in range(sub):
            sib_copy(d, s).wait_send()
            if d:
                plane_copy(d, s).wait_send()
    for d, side, t in parts:
        @pl.when((r >= k) & (r < n_row - 1))
        def _():
            relay(0, r, d, side, t).wait_send()

        @pl.when((r <= k) & (r > 0))
        def _():
            relay(1, r, d, side, t).wait_send()


def exchange(x, n_row):
    rows, cols = x.shape
    n_col = 2 * n_row
    sub = SUB if n_row <= 4 else SUB // 2
    hsub = sub // 2
    dma = pltpu.SemaphoreType.DMA
    return pl.pallas_call(
        functools.partial(exchange_kernel, n_row, sub),
        out_shape=(
            jax.ShapeDtypeStruct((rows, cols * n_col), x.dtype),
            jax.ShapeDtypeStruct((rows // 2, cols * n_col), x.dtype),
        ),
        in_specs=[pl.BlockSpec(memory_space=pltpu.VMEM)],
        out_specs=(pl.BlockSpec(memory_space=pl.ANY),) * 2,
        scratch_shapes=[
            pltpu.VMEM((rows // 2, cols * n_col), x.dtype),
            dma,
            dma((n_row, sub)),
            dma((n_row, sub)),
            dma((n_row, 2, sub)),
            dma((2, n_row, 2, hsub)),
            dma((n_row, 2, hsub)),
            dma,
        ],
        compiler_params=pltpu.CompilerParams(collective_id=0, has_side_effects=True),
        name="exchange",
    )(x)


def project_kernel(
    n_row, w_ref, g_ref, t_ref, p_ref,
    w_in, g_in, w_sum, g_sum, w_full, g_full, send_1, recv_1, send_2, recv_2,
):
    r = lax.axis_index("row")
    c = lax.axis_index("col")
    barrier = pltpu.get_barrier_semaphore()
    for d in range(1, n_row):
        pl.semaphore_signal(barrier, inc=1, device_id=(r ^ d, c), device_id_type=MESH)
    pl.semaphore_wait(barrier, n_row - 1)
    pairs = ((w_ref, w_in, w_sum, w_full), (g_ref, g_in, g_sum, g_full))

    def part(array, owner):
        size = array.shape[0] // n_row
        return pl.ds(pl.multiple_of(owner * size, size), size)

    def scatter(d, i):
        array, landing, _, _ = pairs[i]
        return pltpu.make_async_remote_copy(
            src_ref=array.at[part(array, r ^ d), :], dst_ref=landing.at[d],
            send_sem=send_1.at[d, i], recv_sem=recv_1.at[d, i],
            device_id=(r ^ d, c), device_id_type=MESH,
        )

    def spread(d, i):
        array, _, total, full = pairs[i]
        return pltpu.make_async_remote_copy(
            src_ref=total, dst_ref=full.at[part(array, r), :],
            send_sem=send_2.at[d, i], recv_sem=recv_2.at[d, i],
            device_id=(r ^ d, c), device_id_type=MESH,
        )

    every = [(d, i) for d in range(1, n_row) for i in (1, 0)]
    for d, i in every:
        scatter(d, i).start()
    for d, i in every:
        scatter(d, i).wait_recv()
    for i in (1, 0):
        array, landing, total, full = pairs[i]
        value = array[part(array, r), :]
        for d in range(1, n_row):
            value = value + landing[d]
        total[...] = value
    for i in (1, 0):
        array, _, total, full = pairs[i]
        full[part(array, r), :] = total[...]
    for d, i in every:
        spread(d, i).start()
    for d, i in every:
        spread(d, i).wait_recv()
    highest = lax.Precision.HIGHEST
    width = g_ref.shape[0]
    second = jnp.dot(
        t_ref[1], w_full[width:, :], precision=highest, preferred_element_type=jnp.float32
    ).astype(jnp.bfloat16)
    first = w_full[:width, :] - jnp.dot(
        g_full[...], second.astype(jnp.float32),
        precision=highest, preferred_element_type=jnp.float32,
    )
    first = jnp.dot(t_ref[0], first, precision=highest, preferred_element_type=jnp.float32)
    p_ref[0] = first.astype(jnp.bfloat16)
    p_ref[1] = second
    for d, i in every:
        scatter(d, i).wait_send()
        spread(d, i).wait_send()


def project(w, g, factors, n_row):
    dma = pltpu.SemaphoreType.DMA((n_row, 2))
    width, columns = g.shape[0], w.shape[1]
    vmem = pl.BlockSpec(memory_space=pltpu.VMEM)

    def landing(array):
        return pltpu.VMEM((n_row, array.shape[0] // n_row, array.shape[1]), jnp.float32)

    def total(array):
        return pltpu.VMEM((array.shape[0] // n_row, array.shape[1]), jnp.float32)

    return pl.pallas_call(
        functools.partial(project_kernel, n_row),
        out_shape=jax.ShapeDtypeStruct((2, width, columns), jnp.bfloat16),
        in_specs=[vmem] * 3,
        out_specs=vmem,
        scratch_shapes=[
            landing(w), landing(g), total(w), total(g),
            pltpu.VMEM(w.shape, jnp.float32), pltpu.VMEM(g.shape, jnp.float32),
            dma, dma, dma, dma,
        ],
        compiler_params=pltpu.CompilerParams(collective_id=1, has_side_effects=True),
        name="project",
    )(w, g, factors)


def region_kernel(index_ref, p_ref, vecs_ref, refl_ref, out_ref, vecs, refl, sems):
    count = vecs.shape[0]

    def copies(b):
        at = index_ref[b]
        return (
            pltpu.make_async_copy(vecs_ref.at[at], vecs.at[b], sems.at[b, 0]),
            pltpu.make_async_copy(refl_ref.at[0, at], refl.at[0, b], sems.at[b, 1]),
            pltpu.make_async_copy(refl_ref.at[1, at], refl.at[1, b], sems.at[b, 2]),
        )

    for b in range(count):
        for copy in copies(b):
            copy.start()
    for b in range(count):
        for copy in copies(b):
            copy.wait()
        value = vecs[b].astype(jnp.float32)
        value = value - jnp.dot(refl[1, b], p_ref[1], preferred_element_type=jnp.float32)
        value = value - jnp.dot(refl[0, b], p_ref[0], preferred_element_type=jnp.float32)
        out_ref[b] = value.astype(out_ref.dtype)


def region_rows(index, applied, vecs, refl):
    count = index.shape[0]
    columns, width = vecs.shape[2], refl.shape[3]
    vmem = pl.BlockSpec(memory_space=pltpu.VMEM)
    hbm = pl.BlockSpec(memory_space=pl.ANY)
    return pl.pallas_call(
        region_kernel,
        out_shape=jax.ShapeDtypeStruct((count, BLOCK, columns), vecs.dtype),
        in_specs=[pl.BlockSpec(memory_space=pltpu.SMEM), vmem, hbm, hbm],
        out_specs=vmem,
        scratch_shapes=[
            pltpu.VMEM((count, BLOCK, columns), vecs.dtype),
            pltpu.VMEM((2, count, BLOCK, width), refl.dtype),
            pltpu.SemaphoreType.DMA((count, 3)),
        ],
        name="region",
    )(index, applied, vecs, refl)


def per_device(n_row, eigvecs, reflectors, factors, frequencies, region_blocks):
    columns = eigvecs.shape[1]
    width = reflectors.shape[2]
    local = lax.dot_general(
        reflectors, eigvecs, (((1,), (0,)), ((), ())), preferred_element_type=jnp.float32
    ).reshape(2 * width, columns)
    cross_local = contract_rows(reflectors[0], reflectors[1])
    applied = project(local, cross_local, jnp.triu(factors), n_row)
    local_blocks = eigvecs.shape[0] // BLOCK
    local_index = region_blocks - lax.axis_index("row") * local_blocks
    region = region_rows(
        local_index,
        applied,
        eigvecs.reshape(local_blocks, BLOCK, columns),
        reflectors.reshape(2, local_blocks, BLOCK, width),
    ).reshape(-1, columns)
    weight = 1.0 / jnp.tanh(frequencies / 2.0) / (2.0 * frequencies)
    mine, partner = exchange(region, n_row)
    scaled = (mine.astype(jnp.float32) * weight[None, :]).astype(jnp.bfloat16)
    return contract_cols(scaled, partner)


BF = jnp.bfloat16
F32 = jnp.float32
HIGH = lax.Precision.HIGHEST


def dot_nt(left, right, **kw):
    return lax.dot_general(left, right, (((1,), (1,)), ((), ())), preferred_element_type=F32, **kw)


def dot_tn(left, right):
    return lax.dot_general(left, right, (((0,), (0,)), ((), ())), preferred_element_type=F32)


def spread_kernel(
    chunks, index_ref, vecs_ref, refl_ref, factor_ref, freq_ref, acc_ref, sa_ref, last_ref,
    index, vecs, refl, w_sum, g_sum, w_ref, t_ref, f_ref, small_sem, vec_sem, refl_sem, buf, tbuf, rbuf, w_in, g_in, g_full, p_full, weight,
    w_send, w_recv, g_send, g_recv, h_send, h_recv, p_send, p_recv,
    own_send, relay_send, zrel_send, zsrc_send, detz_send, deti_send, rr_send,
    ax, ay, ad, asib, zb, det, tz, rr,
):
    r = lax.axis_index("row")
    c = lax.axis_index("col")
    k = c // 2
    h = lax.rem(c, 2)
    o = 1 - h
    count = index.shape[0]
    half = count // 2
    columns = vecs.shape[2]
    width = refl.shape[3]
    blocks = vecs.shape[0] // chunks
    quarter = columns // 4
    last_row = 3

    def col(chip, core):
        return 2 * chip + core

    barrier = pltpu.get_barrier_semaphore()

    def greet(row, column):
        pl.semaphore_signal(barrier, inc=1, device_id=(row, column), device_id_type=MESH)

    for d in range(1, 4):
        greet(lax.rem(r + d, 4), c)
    for e in range(1, 8):
        greet(r, c ^ e)

    def load_vecs(i):
        part = pl.ds(i * blocks, blocks)
        return pltpu.make_async_copy(vecs_ref.at[part], vecs.at[part], vec_sem.at[i])

    def load_refl(i):
        part = pl.ds(i * blocks, blocks)
        return pltpu.make_async_copy(refl_ref.at[:, part], refl.at[:, part], refl_sem.at[i])

    def rows_of(array, i):
        return array[pl.ds(i * blocks, blocks)].reshape(blocks * BLOCK, array.shape[2])

    for i in range(chunks):
        load_refl(i).start()
    load_vecs(0).start()
    small = [
        pltpu.make_async_copy(src, dst, small_sem.at[i])
        for i, (src, dst) in enumerate(((index_ref, index), (factor_ref, t_ref), (freq_ref, f_ref)))
    ]
    for copy in small:
        copy.start()
    for i in range(chunks):
        if i + 1 < chunks:
            load_vecs(i + 1).start()
        load_refl(i).wait()
        g = dot_tn(rows_of(refl.at[0], i), rows_of(refl.at[1], i))
        if i:
            g = g + g_sum[...]
        g_sum[...] = g
    for copy in small:
        copy.wait()

    pl.semaphore_wait(barrier, 10)

    def remote(src, dst, send, recv, row, column):
        return pltpu.make_async_remote_copy(
            src_ref=src, dst_ref=dst, send_sem=send, recv_sem=recv,
            device_id=(row, column), device_id_type=MESH,
        )

    far = [jnp.where(r < 2, 3, 0), jnp.where(r < 2, 2, 1), jnp.where(r < 2, 1 - r, 5 - r)]

    def w_copy(q, part):
        d = lax.rem(q - r + 4, 4)
        rows = pl.ds(pl.multiple_of(q * quarter, quarter), quarter)
        lanes = pl.ds(part * width, width)
        return remote(
            w_ref.at[rows, lanes], w_in.at[d, :, lanes], w_send.at[d, part], w_recv.at[d, part], q, c
        )

    g_rows = width // 8
    g_part = pl.ds(pl.multiple_of(c * g_rows, g_rows), g_rows)

    def g_copy(q):
        d = lax.rem(q - r + 4, 4)
        return remote(g_sum.at[g_part], g_in.at[d], g_send.at[d], g_recv.at[d], q, c)

    for q in far:
        g_copy(q).start()
    for i in range(chunks):
        load_vecs(i).wait()
        y = jnp.concatenate([rows_of(refl.at[0], i), rows_of(refl.at[1], i)], axis=1)
        w = dot_tn(rows_of(vecs, i), y)
        if i:
            w = w + w_sum[...]
        w_sum[...] = w
    w_ref[...] = w.astype(BF)
    for part in (1, 0):
        for q in far:
            w_copy(q, part).start()
    for q in far:
        g_copy(q).wait_recv()
    value = g_sum[g_part, :]
    for d in (1, 2, 3):
        value = value + g_in[d]
    g_full[c] = value

    def h_copy(e):
        return remote(g_full.at[c], g_full.at[c], h_send.at[e], h_recv.at[e], r, c ^ e)

    def h_arrival(e):
        return remote(g_full.at[c ^ e], g_full.at[c ^ e], h_send.at[e], h_recv.at[e], r, c ^ e)

    for e in range(1, 8):
        h_copy(e).start()

    f = f_ref[...]
    weight[...] = 1.0 / jnp.tanh(f / 2.0) / (2.0 * f)
    row_at = lax.broadcasted_iota(jnp.int32, (width, width), 0)
    col_at = lax.broadcasted_iota(jnp.int32, (width, width), 1)
    upper = row_at <= col_at
    zero = jnp.zeros((width, width), F32)
    t0 = jnp.where(upper, t_ref[0], zero)
    t1 = jnp.where(upper, t_ref[1], zero)

    mine = pl.ds(pl.multiple_of(r * quarter, quarter), quarter)

    def w_total(part):
        lanes = pl.ds(part * width, width)
        for q in far:
            w_copy(q, part).wait_recv()
        w = w_sum[mine, lanes]
        for d in (1, 2, 3):
            w = w + w_in[d, :, lanes].astype(F32)
        return w

    def p_copy(q, part):
        d = lax.rem(q - r + 4, 4)
        at = p_full.at[r, :, pl.ds(part * width, width)]
        return remote(at, at, p_send.at[d, part], p_recv.at[d, part], q, c)

    def p_arrival(q, part):
        d = lax.rem(r - q + 4, 4)
        at = p_full.at[q, :, pl.ds(part * width, width)]
        return remote(at, at, p_send.at[d, part], p_recv.at[d, part], q, c)

    second = dot_nt(w_total(1), t1, precision=HIGH).astype(BF)
    p_full[r, :, width:] = second
    for q in far:
        p_copy(q, 1).start()
    first = w_total(0)
    for e in range(1, 8):
        h_arrival(e).wait_recv()
    g = g_full[...].reshape(width, width)
    first = first - dot_nt(second.astype(F32), g, precision=HIGH)
    p_full[r, :, :width] = dot_nt(first, t0, precision=HIGH).astype(BF)
    for q in far:
        p_copy(q, 0).start()
    for part in (1, 0):
        for q in far:
            p_arrival(q, part).wait_recv()

    def block_of(n):
        return lax.rem(n, 2) * half + n // 2

    def a_copy(way, n):
        b = block_of(n)
        src = buf.at[c, b]
        if way == 2:
            return remote(src, buf.at[c, b], own_send.at[2], asib.at[0, n], r, col(k, o))
        sem = ax if way == 0 else ay
        return remote(src, buf.at[c, b], own_send.at[way], sem.at[n], r, col(k ^ (way + 1), h))

    corner = (k == 0) | (k == 3)
    is_low = k == 0
    rank = jnp.where(is_low, r, 3 - r)
    away = jnp.where(is_low, -1, 1)
    slot = jnp.where(is_low, 0, 1)
    early = 4

    extra = 2
    near = count - extra

    def det_more(hops, i):
        b = half - 1 + i * half
        return remote(
            buf.at[col(k ^ 1, h), b], tbuf.at[rank - 1, count + i], detz_send.at[hops - 1],
            tz.at[rank - 1, count + i], r + away * hops, c,
        )

    def slot_of(n):
        return jnp.where(n < count, block_of(n), n)

    def det_own(hops, n):
        b = block_of(n)
        return remote(
            buf.at[c, b], tbuf.at[rank - 1, b], detz_send.at[hops - 1], tz.at[rank - 1, n],
            r + away * hops, c,
        )

    down = r < k
    at_source = r == k
    step = jnp.where(down, -1, 1)
    depth = jnp.where(down, k, 3 - k)

    def z_piece(t, depth, is_down):
        third = t // (2 * half)
        n = jnp.where(third == 0, lax.rem(t, half), lax.rem(t, 2 * half) // 2)
        e = jnp.where(third == 0, t // half, lax.rem(t, 2))
        j1 = jnp.where(depth == 3, 2, 3)
        j2 = 6 - depth - j1
        j = jnp.where(third == 0, depth, jnp.where(third == 1, j1, j2))
        j = jnp.where(is_down, j, 3 - j)
        return col(j, lax.rem(h + e, 2)), n

    steps = 3 * 2 * half

    def z_relay(t):
        src, n = z_piece(t, depth, down)
        at = buf.at[src, count + n]
        return remote(at, at, zrel_send, zb.at[t], r + step, c)

    def z_source(t, is_down):
        src, n = z_piece(t, k if is_down else 3 - k, jnp.bool_(is_down))
        return remote(
            buf.at[src, h * half + n], buf.at[src, count + n],
            zsrc_send.at[0 if is_down else 1], zb.at[t], r + (-1 if is_down else 1), c,
        )

    def z_source_step(t):
        @pl.when(at_source)
        def _():
            @pl.when((r > 0) & ((k < 3) | (t < steps - extra)))
            def _():
                z_source(t, True).start()

            @pl.when((r < last_row) & ((k > 0) | (t < steps - extra)))
            def _():
                z_source(t, False).start()

    applied = p_full[...].reshape(columns, 2 * width)

    base = r * vecs.shape[0]

    def make_region(n, _):
        b = block_of(n)
        at = jnp.clip(index[b] - base, 0, vecs.shape[0] - 1)
        y = jnp.concatenate([refl[0, at], refl[1, at]], axis=1)
        buf[c, b] = (vecs[at].astype(F32) - dot_nt(y, applied)).astype(BF)
        for way in (0, 1, 2):
            a_copy(way, n).start()

        @pl.when(corner & ((rank > 1) | ((rank == 1) & (n < early))))
        def _():
            @pl.when(rank == 3)
            def _():
                det_own(2, n).start()

            det_own(1, n).start()

        @pl.when(lax.rem(n, 2) == h)
        def _():
            z_source_step(n // 2)

        return 0

    lax.fori_loop(0, count, make_region, 0)

    def a_arrival(way, n):
        src = col(k ^ (way + 1), h)
        b = block_of(n)
        at = buf.at[src, b]
        sem = (ax, ay, ad)[way]
        return remote(at, at, own_send.at[2], sem.at[n], r, col(k, o))

    def sib_copy(j, n):
        src = col(k ^ j, h)
        b = block_of(n)
        at = buf.at[src, b]
        return remote(at, at, own_send.at[2], asib.at[j, n], r, col(k, o))

    def sib_arrival(j, n):
        src = col(k ^ j, o)
        b = block_of(n)
        at = buf.at[src, b]
        return remote(at, at, own_send.at[2], asib.at[j, n], r, col(k, o))

    def relay(way, n):
        src = col(k ^ (way + 1), h)
        at = buf.at[src, block_of(n)]
        to = k ^ (2 - way)
        return remote(at, at, relay_send.at[way], ad.at[n], r, col(to, h))

    def det_z(p, n):
        at = tbuf.at[p - 1, slot_of(n)]
        return remote(at, at, detz_send.at[p], tz.at[p - 1, n], r + away, c)

    def det_plane(p, n):
        src = tbuf.at[p - 1, slot_of(n)]
        core = lax.rem(n, 2)
        if p < 3:
            return remote(
                src, buf.at[c, count + n // 2], deti_send.at[p], det.at[h, n // 2],
                r, col(k ^ p, core),
            )
        return remote(
            src, rbuf.at[slot, n // 2], deti_send.at[p], rr.at[slot, n // 2],
            r, col(k ^ (1 + h), core),
        )

    between = (k == 1) | (k == 2)

    def rr_copy(way, n):
        low = k - 1 if way == 0 else 2 - k
        more = (n == half).astype(jnp.int32)
        src = low + 2 * more if way == 0 else low + 6 - 2 * more
        return remote(
            rbuf.at[way, n], buf.at[src, count + n - more], rr_send.at[way], det.at[low, n],
            r, col(3 if way == 0 else 0, h),
        )

    def det_arrival(low, n, more=0):
        src = jnp.where(down, low + 2 * more, low + 6 - 2 * more)
        at = buf.at[src, count + n - more]
        return remote(at, at, own_send.at[2], det.at[low, n], r, col(k, o))

    mine_at = jnp.where(at_source, h * half, count)

    from_low = jnp.logical_not(down | (at_source & (k >= 2)))
    deep = jnp.where(from_low, 3 - k, k)
    mid = jnp.where(deep == 3, 2, 3)
    order = []
    for j in (deep, mid, 6 - deep - mid, 0):
        j = jnp.where(from_low, 3 - j, j)
        order += [col(j, 0), col(j, 1)]

    def at_place(s):
        src = order[0]
        for i in range(1, 8):
            src = jnp.where(s == i, order[i], src)
        return src

    def scale(s, part):
        src = at_place(s)
        wt = jnp.concatenate([weight[pl.ds(2 * src, 1), :], weight[pl.ds(2 * src + 1, 1), :]], axis=1)

        def one(i, _):
            b = part * half + i
            rows = pl.ds(pl.multiple_of(b * BLOCK, BLOCK), BLOCK)
            sa_ref[s, rows, :] = (buf[src, b].astype(F32) * wt).astype(BF)
            return 0

        lax.fori_loop(0, half, one, 0)

    tile = 2 * BLOCK
    row_tile = acc_ref.shape[0] // 3

    def product(block, lane, size, third, places, add):
        at = mine_at + block
        lanes = pl.ds(pl.multiple_of(lane, BLOCK), size * BLOCK)
        rows = pl.ds(pl.multiple_of(third * row_tile, row_tile), row_tile)
        total = jnp.zeros((row_tile, size * BLOCK), F32)
        for s in places:
            right = buf[order[s], pl.ds(at, size)].reshape(size * BLOCK, columns)
            total = total + dot_nt(sa_ref[s, rows, :], right)
        if add:
            total = total + acc_ref[rows, lanes]
        acc_ref[rows, lanes] = total

    def pair(q, third, places, add):
        product(2 * q, q * tile, 2, third, places, add)

    def straight(e):
        core = lax.rem(h + e, 2)
        src = col(k ^ 1, core)
        return remote(
            buf.at[src, h * half + half - 1], buf.at[src, count + half - 1], detz_send.at[e],
            det.at[core, half - 1], r + jnp.where(k == 1, -1, 1), c,
        )

    def wait_more():
        @pl.when(jnp.logical_not(at_source) & (depth == 3))
        def _():
            for low in (0, 1):
                det_arrival(low, half, 1).wait_recv()

    def wait_detours(n):
        @pl.when(jnp.logical_not(at_source))
        def _():
            for low in (0, 1):
                det_arrival(low, n).wait_recv()

    hops = jnp.where(down, k - r, r - k)
    lag = 2

    def z_relay_step(u):
        t = u - lag * hops

        @pl.when(jnp.logical_not(at_source) & (t >= 0) & (t < jnp.where(depth == 3, steps - extra, steps)))
        def _():
            z_relay(t).wait_recv()

            @pl.when((down & (r > 0)) | (jnp.logical_not(down) & (r < last_row)))
            def _():
                z_relay(t).start()

    def first_third(n, _):
        sib_arrival(0, 2 * n).wait_recv()
        sib_arrival(0, 2 * n + 1).wait_recv()
        z_source_step(half + n)
        return 0

    lax.fori_loop(0, half, first_third, 0)


    def beat(u, _):
        def span(first, length):
            return (u >= first) & (u < first + length)


        @pl.when(span(2, count))
        def _():
            n = u - 2
            for way in (0, 1):
                a_arrival(way, n).wait_recv()
                sib_copy(way + 1, n).start()
            even = lax.rem(n, 2) == 0

            @pl.when(even)
            def _():
                relay(0, n).start()

            @pl.when(jnp.logical_not(even))
            def _():
                relay(1, n).start()

        @pl.when(span(4, count))
        def _():
            n = u - 4
            sib_arrival(1, n).wait_recv()
            sib_arrival(2, n).wait_recv()

        @pl.when(span(6, count))
        def _():
            z_source_step(u + count - 6)

        @pl.when(corner)
        def _():
            n5 = (u - 3) // 2

            @pl.when((rank == 1) & span(3, 2 * (count + extra)) & (lax.rem(u - 3, 2) == 0))
            def _():
                det_z(3, n5).wait_recv()
                det_z(3, n5).start()

                @pl.when(n5 < count)
                def _():
                    det_z(2, n5).wait_recv()
                    det_z(2, n5).start()

            @pl.when((rank == 3) & span(20, extra))
            def _():
                det_more(2, u - 20).start()
                det_more(1, u - 20).start()

            @pl.when((rank == 1) & span(36, near - early))
            def _():
                det_own(1, u - 36 + early).start()

            v = u - 22
            n3 = (4 * v + 4) // 5

            @pl.when((rank < 3) & span(22, 24) & (lax.rem(v, 5) != 4))
            def _():
                @pl.when(rank != 1)
                def _():
                    det_z(3, n3).wait_recv()

                det_plane(3, n3).start()

            v2 = u - 28
            n2 = (2 * v2) // 3

            @pl.when((rank < 2) & span(28, 27) & (lax.rem(v2, 3) != 1))
            def _():
                @pl.when(rank != 1)
                def _():
                    det_z(2, n2).wait_recv()

                det_plane(2, n2).start()

            @pl.when((rank == 0) & (span(22, early) | span(39 + early, near - early)))
            def _():
                n = jnp.where(u < 40, u - 22, u - 39)
                det_z(1, n).wait_recv()
                det_plane(1, n).start()

        w = u - 30
        item = (4 * w + 4) // 5

        @pl.when(between & span(30, 24) & (lax.rem(w, 5) != 4) & (lax.rem(item, 2) == h))
        def _():
            n = item // 2
            for way in (0, 1):
                @pl.when(r < last_row if way == 0 else r > 0)
                def _():
                    at = rbuf.at[way, n]
                    remote(at, at, rr_send.at[way], rr.at[way, n], r, col(k, o)).wait_recv()
                    rr_copy(way, n).start()

        @pl.when(span(23, half))
        def _():
            for i in range(2):
                n = 2 * (u - 23) + i
                a_arrival(2, n).wait_recv()
                sib_copy(3, n).start()

        @pl.when(span(25, half))
        def _():
            for i in range(2):
                sib_arrival(3, 2 * (u - 25) + i).wait_recv()

        @pl.when(span(27, count))
        def _():
            z_source_step(u + 2 * count - 27)

        z_relay_step(u)

        @pl.when(at_source & (u == 36) & ((k == 1) | (k == 2)))
        def _():
            for e in (0, 1):
                straight(e).start()

        for first, length, place in ((6, 4, 0), (22, 4, 2), (34, 8, 4)):
            @pl.when(span(first, length))
            def _():
                scale(place + (u - first) // 2, lax.rem(u - first, 2))

        for first, q in ((27, 0), (31, 1), (42, 2)):
            @pl.when(span(first, 3))
            def _():
                pair(q, u - first, range(4), False)

        q = (u - 46) // 4
        i = lax.rem(u - 46, 4)

        @pl.when((u == 45) | (u == 49) | (u == 53))
        def _():
            pair(3, (u - 45) // 4, range(4), False)

        @pl.when(span(46, 12) & (i == 0))
        def _():
            wait_detours(2 * q)
            wait_detours(2 * q + 1)

        @pl.when(span(46, 12) & (i < 3))
        def _():
            pair(q, i, range(4, 8), True)

        @pl.when((u == 47) | (u == 51) | (u == 55))
        def _():
            product(8, 4 * tile, 1, (u - 47) // 4, range(4), False)

        return 0

    lax.fori_loop(0, steps + 2 * lag, beat, 0)
    wait_detours(6)
    wait_detours(7)
    wait_detours(8)
    wait_more()
    for s in range(4):
        last_ref[s] = buf[order[4 + s], pl.ds(mine_at + 6, 3)]

    def drain(ref, sem):
        pltpu.make_async_copy(ref, ref, sem).wait()

    for q in far:
        g_copy(q).wait_send()
        for part in (0, 1):
            w_copy(q, part).wait_send()
            p_copy(q, part).wait_send()
    for e in range(1, 8):
        h_copy(e).wait_send()
    shard = buf.at[0, pl.ds(0, count)]
    for way in (0, 1):
        drain(shard, own_send.at[way])
        drain(buf.at[0, pl.ds(0, half)], relay_send.at[way])
    drain(buf.at[:, pl.ds(0, half)], own_send.at[2])

    whole = buf.at[pl.ds(0, 2)]
    short = buf.at[pl.ds(0, 2), pl.ds(0, count + half - extra // 2)]
    longer = buf.at[0, pl.ds(0, count + extra)]
    brief = buf.at[0, pl.ds(0, near)]

    @pl.when(at_source & ((k == 1) | (k == 2)))
    def _():
        for e in (0, 1):
            straight(e).wait_send()

    def drain_either(is_short, sem):
        @pl.when(is_short)
        def _():
            drain(short, sem)

        @pl.when(jnp.logical_not(is_short))
        def _():
            drain(whole, sem)

    @pl.when(at_source)
    def _():
        @pl.when(r > 0)
        def _():
            drain_either(k == 3, zsrc_send.at[0])

        @pl.when(r < last_row)
        def _():
            drain_either(k == 0, zsrc_send.at[1])

    @pl.when((down & (r > 0)) | ((r > k) & (r < last_row)))
    def _():
        drain_either(depth == 3, zrel_send)

    @pl.when(corner)
    def _():
        for p in (3, 2, 1):
            @pl.when(p > rank)
            def _():
                drain({1: brief, 2: shard, 3: longer}[p], deti_send.at[p])

        @pl.when(rank == 1)
        def _():
            drain(longer, detz_send.at[3])
            drain(shard, detz_send.at[2])

            drain(brief, detz_send.at[0])

        @pl.when(rank == 2)
        def _():
            drain(shard, detz_send.at[0])

        @pl.when(rank == 3)
        def _():
            drain(longer, detz_send.at[0])
            drain(longer, detz_send.at[1])

    @pl.when(between)
    def _():
        for way in (0, 1):
            @pl.when(r < last_row if way == 0 else r > 0)
            def _():
                drain(rbuf.at[0], rr_send.at[way])


def spread(index, vecs, refl, factors, frequencies):
    count = index.shape[0]
    columns, width = vecs.shape[2], refl.shape[3]
    chunks = 5
    half = count // 2
    dma = pltpu.SemaphoreType.DMA
    vmem = pl.BlockSpec(memory_space=pltpu.VMEM)
    hbm = pl.BlockSpec(memory_space=pltpu.HBM)
    return pl.pallas_call(
        functools.partial(spread_kernel, chunks),
        out_shape=(
            pltpu.VMEM((count * BLOCK, half * BLOCK), F32),
            pltpu.VMEM((8, count * BLOCK, columns), BF),
            pltpu.VMEM((4, 3, BLOCK, columns), BF),
        ),
        in_specs=[hbm] * 5,
        out_specs=(vmem,) * 3,
        scratch_shapes=[
            pltpu.SMEM((count,), jnp.int32),
            pltpu.VMEM(vecs.shape, BF),
            pltpu.VMEM(refl.shape, BF),
            pltpu.VMEM((columns, 2 * width), F32),
            pltpu.VMEM((width, width), F32),
            pltpu.VMEM((columns, 2 * width), BF),
            pltpu.VMEM(factors.shape, F32),
            pltpu.VMEM(frequencies.shape, F32),
            dma((3,)), dma((chunks,)), dma((chunks,)),
            pltpu.VMEM((8, count + half, BLOCK, columns), BF),
            pltpu.VMEM((3, count + 2, BLOCK, columns), BF),
            pltpu.VMEM((2, half + 1, BLOCK, columns), BF),
            pltpu.VMEM((4, columns // 4, 2 * width), BF),
            pltpu.VMEM((4, width // 8, width), F32),
            pltpu.VMEM((8, width // 8, width), F32),
            pltpu.VMEM((4, columns // 4, 2 * width), BF),
            pltpu.VMEM(frequencies.shape, F32),
            dma((4, 2)), dma((4, 2)), dma((4,)), dma((4,)), dma((8,)), dma((8,)), dma((4, 2)), dma((4, 2)),
            dma((3,)), dma((2,)), dma, dma((2,)), dma((4,)), dma((4,)), dma((2,)),
            dma((count,)), dma((count,)), dma((count,)), dma((4, count)),
            dma((3 * count,)), dma((2, half + 1)), dma((3, count + 2)), dma((2, half + 1)),
        ],
        compiler_params=pltpu.CompilerParams(
            collective_id=2, has_side_effects=True, vmem_limit_bytes=36 << 20
        ),
        name="spread",
    )(index, vecs, refl, factors, frequencies)


def finish_kernel(acc_ref, sa_ref, last_ref, out_ref, tail, sem, pair_sem, single_sem):
    rows, columns = acc_ref.shape
    held, blocks, lane, depth = last_ref.shape
    parts = 2
    size = rows // parts
    done = columns - blocks * lane

    def at(i):
        return pl.ds(i * size, size)

    def main_copy(i):
        lanes = pl.ds(0, done)
        return pltpu.make_async_copy(acc_ref.at[at(i), lanes], out_ref.at[at(i), lanes], sem.at[i])

    def pair_copy(i):
        return pltpu.make_async_copy(
            tail.at[at(i), pl.ds(0, 2 * lane)], out_ref.at[at(i), pl.ds(done, 2 * lane)], pair_sem.at[i]
        )

    def single_copy(i):
        return pltpu.make_async_copy(
            tail.at[at(i), pl.ds(2 * lane, lane)],
            out_ref.at[at(i), pl.ds(columns - lane, lane)], single_sem.at[i],
        )

    for i in range(parts):
        main_copy(i).start()
    for first, count, copy in ((0, 2, pair_copy), (2, 1, single_copy)):
        lanes = pl.ds(first * lane, count * lane)
        for i in range(parts):
            total = acc_ref[at(i), pl.ds(done + first * lane, count * lane)]
            for s in range(held):
                right = last_ref[s, first:first + count].reshape(count * lane, depth)
                total = total + dot_nt(sa_ref[held + s, at(i), :], right)
            tail[at(i), lanes] = total
            copy(i).start()
    for i in range(parts):
        main_copy(i).wait()
        pair_copy(i).wait()
        single_copy(i).wait()


def finish(acc, sa, last):
    vmem = pl.BlockSpec(memory_space=pltpu.VMEM)
    dma = pltpu.SemaphoreType.DMA
    return pl.pallas_call(
        finish_kernel,
        out_shape=jax.ShapeDtypeStruct(acc.shape, F32),
        in_specs=[vmem] * 3,
        out_specs=pl.BlockSpec(memory_space=pl.ANY),
        scratch_shapes=[pltpu.VMEM((acc.shape[0], last.shape[1] * last.shape[2]), F32), dma((4,)), dma((4,)), dma((4,))],
        compiler_params=pltpu.CompilerParams(vmem_limit_bytes=8 << 20),
        name="finish",
    )(acc, sa, last)


def per_device_square(eigvecs, reflectors, factors, frequencies, region_blocks):
    local_blocks = eigvecs.shape[0] // BLOCK
    in_hbm = functools.partial(pltpu.with_memory_space_constraint, memory_space=pltpu.HBM)
    acc, sa, last = spread(
        in_hbm(region_blocks),
        in_hbm(eigvecs.reshape(local_blocks, BLOCK, eigvecs.shape[1])),
        in_hbm(reflectors.reshape(2, local_blocks, BLOCK, reflectors.shape[2])),
        in_hbm(factors),
        in_hbm(frequencies.reshape(-1, 128)),
    )
    return finish(acc, sa, last)


def solution(mesh):
    shape = mesh.shape
    if shape["row"] == 4 and shape["col"] == 8:
        body = per_device_square
    else:
        body = functools.partial(per_device, shape["row"])
    return jax.shard_map(
        body,
        mesh=mesh,
        in_specs=(P("row", "col"), P(None, "row", None), P(), P(), P("row")),
        out_specs=P("row", "col"),
        check_vma=False,
    )
```
